32 devices in a mesh: dp: 8 (over z, y), tensor: 4 (over x, core).
Axes of the slice: x: 2, y: 2, z: 4, core: 2. Of those that a mesh axis runs over, the one named last changes fastest.
Arguments:
- block_input: float32 [16384, 1152], P(('dp', 'tensor'))
- conditioning: float32 [16, 1152], P('dp'), may hold values from -6 to 6
- patch_counts: int32 [16], P('dp'), may hold values from 480 to 1024, as said below
- positions: int32 [16384, 2], P('dp'), may hold values from 0 to 63, as said below
- w_mod: float32 [1152, 6, 1152], P('dp', None, 'tensor'), may hold values from -0.1875 to 0.1875
- b_mod: float32 [6, 1152], P(None, 'tensor'), may hold values from -3 to 3
- w_qkv: float32 [1152, 3, 1152], P('dp', None, 'tensor'), may hold values from -0.1875 to 0.1875
- b_qkv: float32 [3, 1152], P(None, 'tensor'), may hold values from -3 to 3
- w_out: float32 [1152, 1152], P('tensor', 'dp'), may hold values from -3 to 3
- b_out: float32 [1152], replicated, may hold values from -3 to 3
- w_up: float32 [1152, 4608], P('dp', 'tensor'), may hold values from -0.1875 to 0.1875
- b_up: float32 [4608], P('tensor'), may hold values from -3 to 3
- w_down: float32 [4608, 1152], P('tensor', 'dp'), may hold values from -0.09375 to 0.09375
- b_down: float32 [1152], replicated, may hold values from -3 to 3
- cotangent: float32 [16384, 1152], P(('dp', 'tensor')), may hold values from -6 to 6
Outputs:
- block_output: float32 [16384, 1152], P(('dp', 'tensor'))
- grad_input: float32 [16384, 1152], P(('dp', 'tensor'))
- grad_cond: float32 [16, 1152], P('dp')
- grad_wmod: float32 [1152, 6, 1152], P('dp', None, 'tensor')
- grad_bmod: float32 [6, 1152], P(None, 'tensor')
- grad_wqkv: float32 [1152, 3, 1152], P('dp', None, 'tensor')
- grad_bqkv: float32 [3, 1152], P(None, 'tensor')
- grad_wout: float32 [1152, 1152], P('tensor', 'dp')
- grad_bout: float32 [1152], replicated
- grad_wup: float32 [1152, 4608], P('dp', 'tensor')
- grad_bup: float32 [4608], P('tensor')
- grad_wdown: float32 [4608, 1152], P('tensor', 'dp')
- grad_bdown: float32 [1152], replicated
The draws below stay inside these ranges and needn't reach their ends.
Inputs may be any that keep to these rules, and one draw needn't show every extreme that they name: Image i's patches form a grid of h rows and w columns with h w = patch_counts[i]; one image in every draw fills all 1024 slots. `positions`: slot s of image i holds the patch at (s // w, s % w) of its grid of width w for s < patch_counts[i], and (0, 0) past it.
All inputs are finite; a program needn't handle non-finite values.
Results may differ from the reference program's by a relative error of at most 0.017.
The reference program's roundings to bfloat16 on the way count: a program that leaves them out, or rounds other values in their place, can miss the bound.
Values may be sent and summed in bfloat16 or wider, within the bound.
A program may use at most 320 MiB of HBM per device.

```python
import math
from functools import partial
import jax
import jax.numpy as jnp
from jax import lax

D = 1152
HEADS = 16
HEAD = 72
FF = 4608
GRID = 32
SLOTS = 1024
IMAGES = 16
TOKENS = 16384


def grid_shapes(key):
    folded = jax.random.fold_in(key, 11)
    height_key, width_key = jax.random.split(folded)
    heights = jax.random.randint(height_key, (IMAGES,), GRID // 2, 2 * GRID + 1)
    widest = jnp.minimum(SLOTS // heights, 2 * GRID)
    widths = widest - jax.random.randint(width_key, (IMAGES,), 0, widest // 2 + 1)
    image_ids = jnp.arange(IMAGES)
    heights = jnp.where(image_ids == 0, 2 * GRID, jnp.where(image_ids == 1, GRID // 2, heights))
    widths = jnp.where(image_ids == 0, GRID // 2, jnp.where(image_ids == 1, 2 * GRID, widths))
    return (heights, widths)


def draw_patch_counts(key, part):
    heights, widths = grid_shapes(key)
    return (heights * widths).astype(jnp.int32)


def draw_positions(key, part):
    heights, widths = grid_shapes(key)
    slot_ids = jnp.arange(SLOTS)[None, :]
    inside = slot_ids < (heights * widths)[:, None]
    row_ids = jnp.where(inside, slot_ids // widths[:, None], 0)
    col_ids = jnp.where(inside, slot_ids % widths[:, None], 0)
    return jnp.stack([row_ids, col_ids], -1).reshape(TOKENS, 2).astype(jnp.int32)


def draw_block_input(key, part):
    gauss_key, column_key, row_key = jax.random.split(key, 3)
    gaussian = jax.random.normal(gauss_key, (TOKENS, D), jnp.float32)
    fraction = jnp.arange(D, dtype=jnp.float32) / (D - 1)
    column_scale = 0.6 * 3.0 ** fraction * jnp.exp(jax.random.uniform(column_key, (D,), jnp.float32, -0.35, 0.35))
    row_scale = jnp.exp(jax.random.uniform(row_key, (TOKENS, 1), jnp.float32, -0.7, 0.7))
    return gaussian * column_scale * row_scale


def level_of(stream_key, shape, cuts, least, top_value):
    def one(axis_at, shards_of):
        steps = jax.random.uniform(jax.random.fold_in(jax.random.fold_in(stream_key, 6), axis_at), (shards_of,), jnp.float32, least / len(cuts), top_value / len(cuts))
        return jnp.repeat(jnp.exp(steps), shape[axis_at] // shards_of).reshape((-1,) + (1,) * (len(shape) - axis_at - 1))

    factor_of = one(*cuts[0])
    for cut in cuts[1:]:
        factor_of = factor_of * one(*cut)
    return factor_of


def scatter_about(stream_key, dims, spread, reach, shards=(), kind=jnp.bfloat16):
    loudness = level_of(stream_key, dims, shards, -0.22, 0.18) if shards else 1.0
    result = jax.random.normal(stream_key, dims, jnp.float32) * spread * loudness
    return jnp.minimum(jnp.maximum(result, -reach), reach).astype(kind)


def setup_inputs(seed: int = 0) -> dict:
    key_list = jax.random.split(jax.random.key(seed), 16)
    block_input = draw_block_input(jax.random.fold_in(key_list[15], 71), 0)
    conditioning = scatter_about(key_list[1], (IMAGES, D), 1.0, 6.0, ((0, 8),), jnp.float32)
    patch_counts = draw_patch_counts(jax.random.fold_in(key_list[15], 71), 0)
    positions = draw_positions(jax.random.fold_in(key_list[15], 71), 0)
    w_mod = scatter_about(key_list[4], (D, 6, D), D ** -0.5, 0.1875, ((0, 8), (2, 4)), jnp.float32)
    b_mod = scatter_about(key_list[5], (6, D), 0.5, 3.0, ((1, 4),), jnp.float32)
    w_qkv = scatter_about(key_list[6], (D, 3, D), D ** -0.5, 0.1875, ((0, 8), (2, 4)), jnp.float32)
    b_qkv = scatter_about(key_list[7], (3, D), 0.5, 3.0, ((1, 4),), jnp.float32)
    w_out = scatter_about(key_list[8], (D, D), 4 ** -0.5, 3.0, ((0, 4), (1, 8)), jnp.float32)
    b_out = scatter_about(key_list[9], (D,), 0.5, 3.0, (), jnp.float32)
    w_up = scatter_about(key_list[10], (D, FF), D ** -0.5, 0.1875, ((0, 8), (1, 4)), jnp.float32)
    b_up = scatter_about(key_list[11], (FF,), 0.5, 3.0, ((0, 4),), jnp.float32)
    w_down = scatter_about(key_list[12], (FF, D), FF ** -0.5, 0.09375, ((0, 4), (1, 8)), jnp.float32)
    b_down = scatter_about(key_list[13], (D,), 0.5, 3.0, (), jnp.float32)
    cotangent = scatter_about(key_list[14], (TOKENS, D), 1.0, 6.0, ((0, 32),), jnp.float32)
    return {"block_input": block_input, "conditioning": conditioning, "patch_counts": patch_counts, "positions": positions, "w_mod": w_mod, "b_mod": b_mod, "w_qkv": w_qkv, "b_qkv": b_qkv, "w_out": w_out, "b_out": b_out, "w_up": w_up, "b_up": b_up, "w_down": w_down, "b_down": b_down, "cotangent": cotangent}


epsilon = 1e-06
rope_base = 10000.0
gelu_coeff = 0.044715
root_two_pi = math.sqrt(2.0 / math.pi)

@jax.custom_vjp
def low(v):
    return lax.optimization_barrier(v.astype(jnp.bfloat16)).astype(jnp.float32)

@jax.custom_vjp
def low_back(v):
    return v

def low_keep(v):
    return (low(v), None)

def low_pass(kept, grad):
    return (grad,)

def back_keep(v):
    return (v, None)

def back_low(kept, grad):
    return (low(grad),)
low.defvjp(low_keep, low_pass)
low_back.defvjp(back_keep, back_low)

def gelu_tanh(values):
    return 0.5 * values * (1.0 + jnp.tanh(root_two_pi * (values + gelu_coeff * values * values * values)))

def rotate(values, positions, direction):
    quarter = values.shape[-1] // 4
    frequency = rope_base ** (-jnp.arange(quarter, dtype=jnp.float32) / quarter)
    pieces = []
    for column in range(2):
        angles = positions[:, column].astype(jnp.float32)[:, None, None] * frequency
        cosine = jnp.cos(angles)
        sine_term = direction * jnp.sin(angles)
        leading = values[..., 2 * column * quarter:(2 * column + 1) * quarter]
        trailing = values[..., (2 * column + 1) * quarter:(2 * column + 2) * quarter]
        pieces.append(leading * cosine - trailing * sine_term)
        pieces.append(leading * sine_term + trailing * cosine)
    return jnp.concatenate(pieces, -1)

def matmul(left, right):
    return jnp.dot(left, right, precision=lax.Precision.HIGHEST, preferred_element_type=jnp.float32)

def layer_norm(image_rows):
    average = lax.optimization_barrier(jnp.mean(image_rows, -1, keepdims=True))
    inverse = lax.rsqrt(lax.optimization_barrier(jnp.mean(image_rows * image_rows, -1, keepdims=True)) - average * average + epsilon)
    return (image_rows - average) * inverse

def image_block(weights, biases, inputs):
    qkv_matrix, out_matrix, up_matrix, down_matrix = weights
    qkv_bias, out_bias, up_bias, down_bias = biases
    image_rows, modulation, patch_count, positions = inputs
    hidden_one = low(layer_norm(image_rows) * (1.0 + modulation[1]) + modulation[0])
    projected = low_back(matmul(hidden_one, qkv_matrix.reshape(D, 3 * D)) + qkv_bias.reshape(-1))
    projected = projected.reshape(SLOTS, 3, HEADS, HEAD)
    query_rows = low(rotate(projected[:, 0], positions, 1.0))
    key_rows = low(rotate(projected[:, 1], positions, 1.0))
    value_rows = low(projected[:, 2])
    raw_scores = jnp.einsum('qhd,khd->hqk', query_rows, key_rows, precision=lax.Precision.HIGHEST)
    scores = low_back(raw_scores) * (1.0 / math.sqrt(HEAD))
    visible = jnp.arange(SLOTS) < patch_count
    scores = jnp.where(visible[None, None, :], scores, -1e+30)
    highest = lax.optimization_barrier(jnp.max(scores, -1, keepdims=True))
    exponent = jnp.exp(scores - highest)
    softmax_rows = exponent / lax.optimization_barrier(jnp.sum(exponent, -1, keepdims=True))
    attended = jnp.einsum('hqk,khd->qhd', low(softmax_rows), value_rows, precision=lax.Precision.HIGHEST)
    attended = low(low_back(attended.reshape(SLOTS, D)))
    branch_one = low_back(matmul(attended, out_matrix) + out_bias)
    middle = image_rows + modulation[2] * branch_one
    hidden_two = low(layer_norm(middle) * (1.0 + modulation[4]) + modulation[3])
    up_pre = low_back(matmul(hidden_two, up_matrix) + up_bias)
    activated = low(gelu_tanh(up_pre))
    branch_two = low_back(matmul(activated, down_matrix) + down_bias)
    return middle + modulation[5] * branch_two

def forward(block_input, conditioning, w_mod, b_mod, w_qkv, b_qkv, w_out, b_out, w_up, b_up, w_down, b_down, patch_counts, positions):
    weights = (low(w_qkv), low(w_out), low(w_up), low(w_down))
    biases = (b_qkv, b_out, b_up, b_down)
    silu_cond = low(jax.nn.silu(conditioning))
    modulation = low_back(matmul(silu_cond, low(w_mod).reshape(D, 6 * D)) + b_mod.reshape(-1))
    modulation = modulation.reshape(IMAGES, 6, D)
    per_block = jax.checkpoint(partial(image_block, weights, biases))
    outputs = lax.map(per_block, (block_input.reshape(IMAGES, SLOTS, D), modulation, patch_counts, positions.reshape(IMAGES, SLOTS, 2)))
    return outputs.reshape(TOKENS, D)

def reference(block_input, conditioning, patch_counts, positions, w_mod, b_mod, w_qkv, b_qkv, w_out, b_out, w_up, b_up, w_down, b_down, cotangent):

    def wrapped(*params):
        return forward(*params, patch_counts, positions)
    block_output, pullback = jax.vjp(wrapped, block_input, conditioning, w_mod, b_mod, w_qkv, b_qkv, w_out, b_out, w_up, b_up, w_down, b_down)
    gradients = pullback(cotangent)
    return (block_output, gradients[0], gradients[1], gradients[2], gradients[3], gradients[4], gradients[5], gradients[6], gradients[7], gradients[8], gradients[9], gradients[10], gradients[11])
```

```python
from functools import partial
import math

import jax
import jax.numpy as jnp
from jax import lax
from jax.experimental import pallas as pl
from jax.experimental.pallas import tpu as pltpu
from jax.sharding import PartitionSpec as P

HEAD = 72


epsilon = 1e-06
rope_base = 10000.0
gelu_coeff = 0.044715
root_two_pi = math.sqrt(2.0 / math.pi)


def gelu_tanh(values):
    return (
        0.5
        * values
        * (1.0 + jnp.tanh(root_two_pi * (values + gelu_coeff * values * values * values)))
    )


def rotate(values, positions, direction):
    quarter = values.shape[-1] // 4
    frequency = rope_base ** (-jnp.arange(quarter, dtype=jnp.float32) / quarter)
    pieces = []
    for column in range(2):
        angles = positions[:, column].astype(jnp.float32)[:, None, None] * frequency
        cosine = jnp.cos(angles)
        sine_term = direction * jnp.sin(angles)
        leading = values[..., 2 * column * quarter : (2 * column + 1) * quarter]
        trailing = values[..., (2 * column + 1) * quarter : (2 * column + 2) * quarter]
        pieces.append(leading * cosine - trailing * sine_term)
        pieces.append(leading * sine_term + trailing * cosine)
    return jnp.concatenate(pieces, -1)


def contract(left, right, left_dim, right_dim):
    return lax.dot_general(
        left, right, (((left_dim,), (right_dim,)), ((), ())), preferred_element_type=jnp.float32
    )


def exact_dot(left, right):
    return jnp.dot(left, right, precision=lax.Precision.HIGHEST, preferred_element_type=jnp.float32)


def row_norm(rows):
    average = jnp.mean(rows, 1)
    inverse = lax.rsqrt(jnp.mean(rows * rows, 1) - average * average + epsilon)
    return ((rows - average[:, None]) * inverse[:, None], inverse)


def masked_scores(query_rows, key_rows, patch_count, factor):
    raw_scores = (
        jnp.einsum("qhd,khd->hqk", query_rows, key_rows, preferred_element_type=jnp.float32)
        * factor
    )
    visible = jnp.arange(key_rows.shape[0]) < patch_count
    return jnp.where(visible[None, None, :], raw_scores, -1e30)


def attend_forward(factor, inputs):
    query_rows, key_rows, value_rows, patch_count = inputs
    scores = masked_scores(query_rows, key_rows, patch_count, factor)
    highest = jnp.max(scores, -1, keepdims=True)
    exponent = jnp.exp(scores - highest)
    denominator = jnp.sum(exponent, -1, keepdims=True)
    softmax_rows = (exponent / denominator).astype(jnp.bfloat16)
    attended = jnp.einsum(
        "hqk,khd->qhd", softmax_rows, value_rows, preferred_element_type=jnp.float32
    )
    return (attended, (highest + jnp.log(denominator))[..., 0])


def attend_backward(factor, inputs):
    query_rows, key_rows, value_rows, patch_count, logsum, grad_rows = inputs
    scores = masked_scores(query_rows, key_rows, patch_count, factor)
    softmax_rows = jnp.exp(scores - logsum[..., None])
    grad_soft = jnp.einsum(
        "qhd,khd->hqk", grad_rows, value_rows, preferred_element_type=jnp.float32
    )
    grad_values = jnp.einsum(
        "hqk,qhd->khd",
        softmax_rows.astype(jnp.bfloat16),
        grad_rows,
        preferred_element_type=jnp.float32,
    )
    inner_sum = jnp.sum(softmax_rows * grad_soft, -1, keepdims=True)
    grad_scores = (softmax_rows * (grad_soft - inner_sum) * factor).astype(jnp.bfloat16)
    grad_query = jnp.einsum(
        "hqk,khd->qhd", grad_scores, key_rows, preferred_element_type=jnp.float32
    )
    grad_keys = jnp.einsum(
        "hqk,qhd->khd", grad_scores, query_rows, preferred_element_type=jnp.float32
    )
    return (grad_query, grad_keys, grad_values)


def per_device(
    block_input,
    conditioning,
    patch_counts,
    positions,
    w_mod,
    b_mod,
    w_qkv,
    b_qkv,
    w_out,
    b_out,
    w_up,
    b_up,
    w_down,
    b_down,
    cotangent,
):
    own_rows, model_width = block_input.shape
    group_rows = positions.shape[0]
    images_local = conditioning.shape[0]
    slot_count = group_rows // images_local
    feat_local = w_qkv.shape[2]
    heads_local = feat_local // HEAD
    row_start = lax.axis_index("tensor") * own_rows
    factor = 1.0 / math.sqrt(HEAD)
    image_of = (row_start + jnp.arange(own_rows)) // slot_count
    one_hot = (image_of[:, None] == jnp.arange(images_local)[None, :]).astype(jnp.float32)

    def to_rows(vectors):
        return exact_dot(one_hot, vectors)

    def to_images(values):
        return exact_dot(one_hot.T, values)

    def per_image(stacked):
        return stacked.reshape((images_local, slot_count) + stacked.shape[1:])

    def modulate_group(values, shift, scale):
        shaped = values.reshape(images_local, slot_count, values.shape[1])
        return (shaped * (1.0 + scale[:, None, :]) + shift[:, None, :]).reshape(values.shape)

    mod_full, qkv_full, out_full, up_full, down_full = (
        lax.all_gather(w_mod.astype(jnp.bfloat16), "dp", axis=0, tiled=True),
        lax.all_gather(w_qkv.astype(jnp.bfloat16), "dp", axis=0, tiled=True),
        lax.all_gather(w_out.astype(jnp.bfloat16), "dp", axis=1, tiled=True),
        lax.all_gather(w_up.astype(jnp.bfloat16), "dp", axis=0, tiled=True),
        lax.all_gather(w_down.astype(jnp.bfloat16), "dp", axis=1, tiled=True),
    )
    silu_cond = jax.nn.silu(conditioning).astype(jnp.bfloat16)
    mod_cols = jnp.dot(
        silu_cond, mod_full.reshape(model_width, 6 * feat_local), preferred_element_type=jnp.float32
    )
    mod_cols = mod_cols.reshape(images_local, 6, feat_local) + b_mod
    mod_all = lax.all_gather(mod_cols, "tensor", axis=2, tiled=True)

    def norm_gather(rows_local, shift, scale):
        rows_group = lax.all_gather(rows_local, "tensor", axis=0, tiled=True)
        normal_group, inverse_group = row_norm(rows_group)
        hidden = modulate_group(normal_group, shift, scale).astype(jnp.bfloat16)
        normal = lax.dynamic_slice_in_dim(normal_group, row_start, own_rows, 0)
        inverse = lax.dynamic_slice_in_dim(inverse_group, row_start, own_rows, 0)
        return (hidden, normal, inverse)

    hidden_one, normal_one, inverse_one = norm_gather(block_input, mod_all[:, 0], mod_all[:, 1])
    projected = jnp.dot(
        hidden_one,
        qkv_full.reshape(model_width, 3 * feat_local),
        preferred_element_type=jnp.float32,
    ) + b_qkv.reshape(-1)
    projected = projected.reshape(group_rows, 3, heads_local, HEAD)
    query_rows = rotate(projected[:, 0], positions, 1.0).astype(jnp.bfloat16)
    key_rows = rotate(projected[:, 1], positions, 1.0).astype(jnp.bfloat16)
    value_rows = projected[:, 2].astype(jnp.bfloat16)
    attended, logsum = lax.map(
        partial(attend_forward, factor),
        (per_image(query_rows), per_image(key_rows), per_image(value_rows), patch_counts),
    )
    attended = attended.reshape(group_rows, feat_local).astype(jnp.bfloat16)

    def branch_sum(partial_terms, offset):
        return lax.psum_scatter(partial_terms, "tensor", scatter_dimension=0, tiled=True) + offset

    gate_one_rows = to_rows(mod_all[:, 2])
    gate_two_rows = to_rows(mod_all[:, 5])
    branch_one = branch_sum(jnp.dot(attended, out_full, preferred_element_type=jnp.float32), b_out)
    middle = block_input + gate_one_rows * branch_one
    hidden_two, normal_two, inverse_two = norm_gather(middle, mod_all[:, 3], mod_all[:, 4])
    up_pre = jnp.dot(hidden_two, up_full, preferred_element_type=jnp.float32) + b_up
    activated = gelu_tanh(up_pre).astype(jnp.bfloat16)
    branch_two = branch_sum(
        jnp.dot(activated, down_full, preferred_element_type=jnp.float32), b_down
    )
    block_output = middle + gate_two_rows * branch_two
    mod_back, qkv_back, out_back, up_back, down_back = (
        lax.all_gather(w_mod.astype(jnp.bfloat16), "dp", axis=0, tiled=True),
        lax.all_gather(w_qkv.astype(jnp.bfloat16), "dp", axis=0, tiled=True),
        lax.all_gather(w_out.astype(jnp.bfloat16), "dp", axis=1, tiled=True),
        lax.all_gather(w_up.astype(jnp.bfloat16), "dp", axis=0, tiled=True),
        lax.all_gather(w_down.astype(jnp.bfloat16), "dp", axis=1, tiled=True),
    )

    def spread_grad(grad_branch):
        return lax.all_gather(grad_branch, "tensor", axis=0, tiled=True)

    def input_sum(partial_terms):
        return lax.psum_scatter(partial_terms, "tensor", scatter_dimension=0, tiled=True)

    def norm_backward(grad_hidden, normal, inverse, scale):
        grad_normal = grad_hidden * (1.0 + to_rows(scale))
        mean_plain = jnp.mean(grad_normal, 1, keepdims=True)
        mean_cross = jnp.mean(grad_normal * normal, 1, keepdims=True)
        return inverse[:, None] * (grad_normal - mean_plain - normal * mean_cross)

    grad_gate_two = to_images(cotangent * branch_two)
    grad_branch_two = (cotangent * gate_two_rows).astype(jnp.bfloat16)
    grad_rows_two = spread_grad(grad_branch_two)
    grad_bdown_local = jnp.sum(grad_rows_two.astype(jnp.float32), 0)
    grad_wdown_local = contract(activated, grad_rows_two, 0, 0)
    grad_activated = contract(grad_rows_two, down_back, 1, 1)
    gelu_pull = jax.vjp(gelu_tanh, up_pre)[1]
    grad_up = gelu_pull(grad_activated)[0].astype(jnp.bfloat16)
    grad_bup_local = jnp.sum(grad_up.astype(jnp.float32), 0)
    grad_wup_local = contract(hidden_two, grad_up, 0, 0)
    grad_hidden_two = input_sum(contract(grad_up, up_back, 1, 1))
    grad_shift_two = to_images(grad_hidden_two)
    grad_scale_two = to_images(grad_hidden_two * normal_two)
    grad_middle = cotangent + norm_backward(grad_hidden_two, normal_two, inverse_two, mod_all[:, 4])
    grad_gate_one = to_images(grad_middle * branch_one)
    grad_branch_one = (grad_middle * gate_one_rows).astype(jnp.bfloat16)
    grad_rows_one = spread_grad(grad_branch_one)
    grad_bout_local = jnp.sum(grad_rows_one.astype(jnp.float32), 0)
    grad_wout_local = contract(attended, grad_rows_one, 0, 0)
    grad_attended = contract(grad_rows_one, out_back, 1, 1).astype(jnp.bfloat16)
    grad_attended = grad_attended.reshape(group_rows, heads_local, HEAD)
    grad_query, grad_keys, grad_values = lax.map(
        partial(attend_backward, factor),
        (
            per_image(query_rows),
            per_image(key_rows),
            per_image(value_rows),
            patch_counts,
            logsum,
            per_image(grad_attended),
        ),
    )
    head_shape = (group_rows, heads_local, HEAD)
    grad_projected = jnp.stack(
        [
            rotate(grad_query.reshape(head_shape), positions, -1.0),
            rotate(grad_keys.reshape(head_shape), positions, -1.0),
            grad_values.reshape(head_shape),
        ],
        1,
    )
    grad_projected = grad_projected.astype(jnp.bfloat16).reshape(group_rows, 3 * feat_local)
    grad_bqkv_local = jnp.sum(grad_projected.astype(jnp.float32), 0).reshape(3, feat_local)
    grad_wqkv_local = contract(hidden_one, grad_projected, 0, 0).reshape(model_width, 3, feat_local)
    grad_hidden_one = input_sum(
        contract(grad_projected, qkv_back.reshape(model_width, 3 * feat_local), 1, 1)
    )
    grad_shift_one = to_images(grad_hidden_one)
    grad_scale_one = to_images(grad_hidden_one * normal_one)
    grad_input = grad_middle + norm_backward(
        grad_hidden_one, normal_one, inverse_one, mod_all[:, 1]
    )
    grad_mod_part = jnp.stack(
        [
            grad_shift_one,
            grad_scale_one,
            grad_gate_one,
            grad_shift_two,
            grad_scale_two,
            grad_gate_two,
        ],
        1,
    )
    grad_mod = lax.psum_scatter(grad_mod_part, "tensor", scatter_dimension=2, tiled=True).astype(
        jnp.bfloat16
    )
    grad_bmod_local = jnp.sum(grad_mod.astype(jnp.float32), 0)
    grad_mod_flat = grad_mod.reshape(images_local, 6 * feat_local)
    grad_wmod_local = contract(silu_cond, grad_mod_flat, 0, 0).reshape(model_width, 6, feat_local)
    grad_silu = lax.psum(
        contract(grad_mod_flat, mod_back.reshape(model_width, 6 * feat_local), 1, 1), "tensor"
    )
    silu_pull = jax.vjp(jax.nn.silu, conditioning)[1]
    grad_cond = silu_pull(grad_silu)[0]
    grad_wmod, grad_wqkv, grad_wout, grad_wup, grad_wdown = (
        lax.psum_scatter(
            grad_wmod_local.astype(jnp.bfloat16), "dp", scatter_dimension=0, tiled=True
        ).astype(jnp.float32),
        lax.psum_scatter(
            grad_wqkv_local.astype(jnp.bfloat16), "dp", scatter_dimension=0, tiled=True
        ).astype(jnp.float32),
        lax.psum_scatter(
            grad_wout_local.astype(jnp.bfloat16), "dp", scatter_dimension=1, tiled=True
        ).astype(jnp.float32),
        lax.psum_scatter(
            grad_wup_local.astype(jnp.bfloat16), "dp", scatter_dimension=0, tiled=True
        ).astype(jnp.float32),
        lax.psum_scatter(
            grad_wdown_local.astype(jnp.bfloat16), "dp", scatter_dimension=1, tiled=True
        ).astype(jnp.float32),
    )
    grad_bmod, grad_bqkv, grad_bout, grad_bup, grad_bdown = lax.psum(
        (grad_bmod_local, grad_bqkv_local, grad_bout_local, grad_bup_local, grad_bdown_local), "dp"
    )
    return (
        block_output,
        grad_input,
        grad_cond,
        grad_wmod,
        grad_bmod,
        grad_wqkv,
        grad_bqkv,
        grad_wout,
        grad_bout,
        grad_wup,
        grad_bup,
        grad_wdown,
        grad_bdown,
    )


LANES = 128
ZS, YS, XS, CORES = 4, 2, 2, 2
MESH_ID = pl.DeviceIdType.MESH
CORE_SWAP = [(0, 1), (1, 0), (2, 3), (3, 2)]
X_SWAP = [(0, 2), (2, 0), (1, 3), (3, 1)]
LOG2E = 1.0 / math.log(2.0)
PAIRS = (
    (0, 0, 32, 32),
    (0, 64, 48, 32),
    (1, 0, 32, 32),
    (1, 64, 32, 48),
    (2, 0, 32, 32),
    (2, 64, 48, 32),
)
HBM = pl.BlockSpec(memory_space=pl.ANY)
VMEM = pl.BlockSpec(memory_space=pltpu.VMEM)


def image_per_chip(mesh):
    return dict(mesh.shape) == {"dp": ZS * YS, "tensor": XS * CORES}


def place():
    data, tensor = lax.axis_index("dp"), lax.axis_index("tensor")
    return data // YS, data % YS, tensor // CORES, tensor % CORES


def flip_z(z, step):
    high, low = z // 2, z % 2
    if step & 2:
        high = 1 - high
    if step & 1:
        low = 1 - low
    return high * 2 + low


def device(z, y, x, core):
    return (z * YS + y, x * CORES + core)


def greet(targets):
    barrier = pltpu.get_barrier_semaphore()
    for target in targets:
        pl.semaphore_signal(barrier, inc=1, device_id=target, device_id_type=MESH_ID)
    pl.semaphore_wait(barrier, len(targets))


def grid_peers():
    z, y, x, core = place()
    peers = [device(z, y, 1 - x, core), device(z, 1 - y, x, core)]
    return peers + [device(flip_z(z, step), y, x, core) for step in (1, 2, 3)]


def chunk_list():
    chunks = []
    for matrix, row, first, second in PAIRS:
        chunks.append(((matrix, row, first, 0), (matrix, row + first, second, 1)))
    return chunks


def remote(source, target_ref, sems, index, where):
    return pltpu.make_async_remote_copy(
        src_ref=source,
        dst_ref=target_ref,
        send_sem=sems[0].at[index],
        recv_sem=sems[1].at[index],
        device_id=where,
        device_id_type=MESH_ID,
    )


def gather_kernel(*refs):
    shards, wholes = refs[:3], refs[3:6]
    sends, recvs, local = refs[6:]
    sems = (sends, recvs)
    z, y, x, core = place()
    peers = grid_peers()
    width = shards[0].shape[1]
    greet(peers)
    mine = pl.ds(pl.multiple_of(x * width, LANES), width)
    keeps = []
    for matrix in range(3):
        keep = pltpu.make_async_copy(
            shards[matrix], wholes[matrix].at[z, y, :, mine], local.at[matrix]
        )
        keep.start()
        keeps.append(keep)
    chunks = chunk_list()
    copies = {}

    def launch(number, stage, chunk):
        matrix, row, rows, route = chunk
        whole, span = wholes[matrix], pl.ds(row, rows)
        base = number * 5
        if stage == 0:
            made = [
                remote(
                    shards[matrix].at[span, :],
                    whole.at[z, y, span, mine],
                    sems,
                    base + step,
                    peers[2 + step],
                )
                for step in range(3)
            ]
        elif (stage == 1) == (route == 0):
            part = whole.at[:, y, span, mine] if stage == 1 else whole.at[:, :, span, mine]
            made = [remote(part, part, sems, base + 2 + stage, peers[0])]
        else:
            part = whole.at[:, y, span, mine] if stage == 1 else whole.at[:, y, span, :]
            made = [remote(part, part, sems, base + 2 + stage, peers[1])]
        for copy in made:
            copy.start()
        copies[number, stage] = made

    def settle(number, stage):
        for copy in copies[number, stage]:
            copy.wait_recv()

    total = len(chunks)
    for tick in range(total + 3):
        for stage in (2, 1, 0):
            pair = tick - stage
            if not 0 <= pair < total:
                continue
            for route in range(2):
                number = pair * 2 + route
                if stage > 0:
                    settle(number, stage - 1)
                if stage == 1 and route == 0 and chunks[pair][0][1] == 0:
                    keeps[chunks[pair][0][0]].wait()
                launch(number, stage, chunks[pair][route])
        pair = tick - 3
        if 0 <= pair < total:
            for route in range(2):
                settle(pair * 2 + route, 2)
    for made in copies.values():
        for copy in made:
            copy.wait_send()


def gather_weights(shards, ident):
    rows, width = shards[0].shape
    shape = jax.ShapeDtypeStruct((ZS, YS, rows, XS * width), jnp.bfloat16)
    count = len(PAIRS) * 2 * 5
    wholes = pl.pallas_call(
        gather_kernel,
        out_shape=[shape] * 3,
        in_specs=[VMEM] * 3,
        out_specs=[HBM] * 3,
        scratch_shapes=[
            pltpu.SemaphoreType.DMA((count,)),
            pltpu.SemaphoreType.DMA((count,)),
            pltpu.SemaphoreType.DMA((3,)),
        ],
        compiler_params=pltpu.CompilerParams(collective_id=ident, has_side_effects=True),
        name="gather_weights",
    )(*shards)
    return [whole.reshape(ZS * YS * rows, XS * width) for whole in wholes]


def scatter_kernel(*refs):
    parts, sums = refs[:3], refs[3:6]
    own, first_in, second_in, third_in, sends, recvs, local = refs[6:]
    sems = (sends, recvs)
    z, y, x, core = place()
    peers = grid_peers()
    width = sums[0].shape[1]
    greet(peers)
    mine = pl.ds(pl.multiple_of(x * width, LANES), width)
    theirs = pl.ds(pl.multiple_of((1 - x) * width, LANES), width)
    chunks = chunk_list()
    copies = {}
    loads = {}

    def launch(number, stage, chunk):
        matrix, row, rows, route = chunk
        part, span = parts[matrix], pl.ds(row, rows)
        base = number * 3
        if stage == 0:
            made = []
            for slot in range(2):
                if route == 0:
                    column = mine if slot == 0 else theirs
                    source = part.at[:, 1 - y, span, column]
                    kept = part.at[:, y, span, column]
                    where = peers[1]
                else:
                    line = y if slot == 0 else 1 - y
                    source = part.at[:, line, span, theirs]
                    kept = part.at[:, line, span, mine]
                    where = peers[0]
                copy = remote(source, first_in.at[matrix, slot, :, span, :], sems, base + slot, where)
                made.append(copy)
                load = pltpu.make_async_copy(
                    kept, own.at[matrix, slot, :, span, :], local.at[number * 2 + slot]
                )
                load.start()
                loads[number, slot] = load
        elif stage == 1:
            where = peers[0] if route == 0 else peers[1]
            made = [
                remote(
                    own.at[matrix, 1, :, span, :],
                    second_in.at[matrix, :, span, :],
                    sems,
                    base + 2,
                    where,
                )
            ]
        else:
            made = [
                remote(
                    own.at[matrix, 0, flip_z(z, step), span, :],
                    third_in.at[matrix, step - 1, span, :],
                    sems,
                    third[number] + step - 1,
                    peers[1 + step],
                )
                for step in (1, 2, 3)
            ]
        for copy in made:
            copy.start()
        copies[number, stage] = made

    third = {n: len(chunks) * 2 * 3 + n * 3 for n in range(len(chunks) * 2)}

    def add_into(target, arrived, rows):
        def step(i, carry):
            at = pl.ds(pl.multiple_of(i * 16, 16), 16)
            target[at, :] = (
                target[at, :].astype(jnp.float32) + arrived[at, :].astype(jnp.float32)
            ).astype(jnp.bfloat16)
            return carry

        lax.fori_loop(0, rows // 16, step, 0)

    def merge(number, stage, chunk):
        matrix, row, rows, route = chunk
        span = pl.ds(row, rows)
        for copy in copies[number, stage]:
            copy.wait_recv()
        if stage == 0:
            for slot in range(2):
                loads[number, slot].wait()

                def one(i, carry, slot=slot):
                    add_into(
                        own.at[matrix, slot, i, span, :],
                        first_in.at[matrix, slot, i, span, :],
                        rows,
                    )
                    return carry

                lax.fori_loop(0, ZS, one, 0)
        elif stage == 1:

            def two(i, carry):
                add_into(own.at[matrix, 0, i, span, :], second_in.at[matrix, i, span, :], rows)
                return carry

            lax.fori_loop(0, ZS, two, 0)
        else:

            def step(i, carry):
                at = pl.ds(pl.multiple_of(row + i * 16, 16), 16)
                total = own[matrix, 0, z, at, :].astype(jnp.float32)
                for k in range(3):
                    total = total + third_in[matrix, k, at, :].astype(jnp.float32)
                sums[matrix][at, :] = total
                return carry

            lax.fori_loop(0, rows // 16, step, 0)

    total = len(chunks)
    for tick in range(total + 3):
        for stage in (2, 1, 0):
            pair = tick - stage
            if not 0 <= pair < total:
                continue
            for route in range(2):
                number = pair * 2 + route
                if stage > 0:
                    merge(number, stage - 1, chunks[pair][route])
                launch(number, stage, chunks[pair][route])
        pair = tick - 3
        if 0 <= pair < total:
            for route in range(2):
                merge(pair * 2 + route, 2, chunks[pair][route])
    for made in copies.values():
        for copy in made:
            copy.wait_send()


def scatter_grads(parts, ident):
    rows, width = parts[0].shape[0] // (ZS * YS), parts[0].shape[1] // XS
    parts = [part.reshape(ZS, YS, rows, XS * width) for part in parts]
    pairs = len(PAIRS) * 2
    return pl.pallas_call(
        scatter_kernel,
        out_shape=[jax.ShapeDtypeStruct((rows, width), jnp.float32)] * 3,
        in_specs=[HBM] * 3,
        out_specs=[VMEM] * 3,
        scratch_shapes=[
            pltpu.VMEM((3, 2, ZS, rows, width), jnp.bfloat16),
            pltpu.VMEM((3, 2, ZS, rows, width), jnp.bfloat16),
            pltpu.VMEM((3, ZS, rows, width), jnp.bfloat16),
            pltpu.VMEM((3, 3, rows, width), jnp.bfloat16),
            pltpu.SemaphoreType.DMA((pairs * 6,)),
            pltpu.SemaphoreType.DMA((pairs * 6,)),
            pltpu.SemaphoreType.DMA((pairs * 2,)),
        ],
        compiler_params=pltpu.CompilerParams(
            collective_id=ident, has_side_effects=True, vmem_limit_bytes=60 * 2**20
        ),
        name="scatter_grads",
    )(*parts)


def group_of(kind):
    z, y, x, core = place()
    data, tensor = z * YS + y, x * CORES + core
    if kind == "dp":
        return ZS * YS, data, lambda i: (i, tensor)
    if kind == "same_core":
        return ZS * YS * XS, data * XS + x, lambda i: (i // XS, (i % XS) * CORES + core)
    return (
        ZS * YS * XS * CORES,
        data * XS * CORES + tensor,
        lambda i: (i // (XS * CORES), i % (XS * CORES)),
    )


def exchange_kernel(kind, gather, blocks, arrived, sends, recvs):
    count, me, device_of = group_of(kind)
    targets = [(me + step) % count for step in range(1, count)]
    greet([device_of(target) for target in targets])
    copies = []
    for step, target in enumerate(targets):
        copy = pltpu.make_async_remote_copy(
            src_ref=blocks if gather else blocks.at[target],
            dst_ref=arrived.at[me],
            send_sem=sends.at[step],
            recv_sem=recvs.at[step],
            device_id=device_of(target),
            device_id_type=MESH_ID,
        )
        copy.start()
        copies.append(copy)
    arrived[me] = blocks[...] if gather else blocks[me]
    for copy in copies:
        copy.wait_send()
    for copy in copies:
        copy.wait_recv()


def exchange(blocks, kind, ident, gather=False):
    count = {"dp": ZS * YS, "same_core": ZS * YS * XS, "all": ZS * YS * XS * CORES}[kind]
    shape = blocks.shape if gather else blocks.shape[1:]
    return pl.pallas_call(
        partial(exchange_kernel, kind, gather),
        out_shape=jax.ShapeDtypeStruct((count,) + shape, blocks.dtype),
        in_specs=[VMEM],
        out_specs=VMEM,
        scratch_shapes=[
            pltpu.SemaphoreType.DMA((count - 1,)),
            pltpu.SemaphoreType.DMA((count - 1,)),
        ],
        compiler_params=pltpu.CompilerParams(collective_id=ident, has_side_effects=True),
        name="exchange_" + kind,
    )(blocks)


QUARTER = HEAD // 4
BLOCK = 256


def turn(values, tables, back):
    cosine, to_left, to_right = tables
    swapped = (
        pltpu.roll(values, LANES - QUARTER, axis=1) * to_left
        + pltpu.roll(values, QUARTER, axis=1) * to_right
    )
    return values * cosine - swapped if back else values * cosine + swapped


def attend_kernel(heads, scale, *refs):
    projected, (cos_ref, left_ref, right_ref, hide_ref) = refs[:2], refs[2:6]
    out_refs = refs[6:8]
    query_ref, key_ref, value_ref, logsum_ref, held = refs[8:]
    slots = cos_ref.shape[0]
    per = heads // 2
    blocks = slots // BLOCK

    def prepare(i, carry):
        at = pl.ds(pl.multiple_of(i * BLOCK, BLOCK), BLOCK)
        tables = cos_ref[at, :], left_ref[at, :], right_ref[at, :]
        hide = hide_ref[at, :]
        lane = lax.broadcasted_iota(jnp.int32, (BLOCK, LANES), 1)
        for head in range(heads):
            source, local = projected[head // per], head % per
            for part, target in enumerate((query_ref, key_ref, value_ref)):
                start = (part * per + local) * HEAD
                values = source[at, start : start + LANES]
                if part == 2:
                    values = jnp.where(lane < HEAD, values, 0.0)
                else:
                    values = turn(values, tables, False)
                    values = values + (jnp.where(lane == HEAD, 1.0, 0.0) if part == 0 else hide)
                target[head, at, :] = values.astype(jnp.bfloat16)
        return carry

    lax.fori_loop(0, blocks, prepare, 0)

    def attend(i, carry):
        head, block = i // blocks, i % blocks
        at = pl.ds(pl.multiple_of(block * BLOCK, BLOCK), BLOCK)
        scores = contract(query_ref[head, at, :], key_ref[head], 1, 1)
        highest = jnp.max(scores, 1, keepdims=True)
        exponent = jnp.exp2((scores - highest) * (scale * LOG2E))
        denominator = jnp.sum(exponent, 1, keepdims=True)
        result = jnp.dot(
            exponent.astype(jnp.bfloat16), value_ref[head], preferred_element_type=jnp.float32
        )
        held[head, at, :] = result / denominator
        logsum_ref[head, at, :] = jnp.broadcast_to(
            (highest * scale + jnp.log(denominator)) * LOG2E, (BLOCK, LANES)
        )
        return carry

    lax.fori_loop(0, heads * blocks, attend, 0)

    def finish(i, carry):
        at = pl.ds(pl.multiple_of(i * BLOCK, BLOCK), BLOCK)
        for half in range(2):
            row = jnp.concatenate(
                [held[half * per + local, at, :][:, :HEAD] for local in range(per)], 1
            )
            out_refs[half][at, :] = row.astype(jnp.bfloat16)
        return carry

    lax.fori_loop(0, blocks, finish, 0)


def attend(projected, tables, heads, scale):
    slots = projected[0].shape[0]
    packed = jax.ShapeDtypeStruct((heads, slots, LANES), jnp.bfloat16)
    half = jax.ShapeDtypeStruct((slots, heads // 2 * HEAD), jnp.bfloat16)
    results = pl.pallas_call(
        partial(attend_kernel, heads, scale),
        out_shape=[
            half,
            half,
            packed,
            packed,
            packed,
            jax.ShapeDtypeStruct((heads, slots, LANES), jnp.float32),
        ],
        in_specs=[VMEM] * 6,
        out_specs=[VMEM] * 6,
        scratch_shapes=[pltpu.VMEM((heads, slots, LANES), jnp.float32)],
        compiler_params=pltpu.CompilerParams(vmem_limit_bytes=60 * 2**20),
        name="attend",
    )(*projected, *tables)
    return results[:2], results[2:]


def attend_back_kernel(heads, scale, *refs):
    query_ref, key_ref, value_ref, logsum_ref = refs[:4]
    grads, (cos_ref, left_ref, right_ref) = refs[4:6], refs[6:9]
    out_refs = refs[9:11]
    held, grad_q, grad_k, grad_v = refs[11:]
    slots = cos_ref.shape[0]
    per = heads // 2
    blocks = slots // BLOCK

    def prepare(i, carry):
        at = pl.ds(pl.multiple_of(i * BLOCK, BLOCK), BLOCK)
        for head in range(heads):
            local = head % per
            piece = grads[head // per][at, local * HEAD : (local + 1) * HEAD]
            padding = jnp.zeros((BLOCK, LANES - HEAD), piece.dtype)
            held[head, at, :] = jnp.concatenate([piece, padding], 1)
        return carry

    lax.fori_loop(0, blocks, prepare, 0)

    def attend(i, carry):
        head, block = i // blocks, i % blocks
        at = pl.ds(pl.multiple_of(block * BLOCK, BLOCK), BLOCK)
        query, grad = query_ref[head, at, :], held[head, at, :]
        key = key_ref[head]
        scores = contract(query, key, 1, 1)
        soft = jnp.exp2(scores * (scale * LOG2E) - logsum_ref[head, at, :1])
        grad_soft = contract(grad, value_ref[head], 1, 1)
        value_part = contract(soft.astype(jnp.bfloat16), grad, 0, 0)
        product = soft * grad_soft
        inner = jnp.sum(product, 1, keepdims=True)
        grad_scores = ((product - soft * inner) * scale).astype(jnp.bfloat16)
        grad_q[head, at, :] = jnp.dot(grad_scores, key, preferred_element_type=jnp.float32)
        key_part = contract(grad_scores, query, 0, 0)

        @pl.when(block == 0)
        def _():
            grad_v[head] = value_part
            grad_k[head] = key_part

        @pl.when(block > 0)
        def _():
            grad_v[head] += value_part
            grad_k[head] += key_part

        return carry

    lax.fori_loop(0, heads * blocks, attend, 0)

    def finish(i, carry):
        at = pl.ds(pl.multiple_of(i * BLOCK, BLOCK), BLOCK)
        tables = cos_ref[at, :], left_ref[at, :], right_ref[at, :]
        for half in range(2):
            pieces = []
            for part, source in enumerate((grad_q, grad_k, grad_v)):
                for local in range(per):
                    values = source[half * per + local, at, :]
                    if part < 2:
                        values = turn(values, tables, True)
                    pieces.append(values[:, :HEAD])
            out_refs[half][at, :] = jnp.concatenate(pieces, 1).astype(jnp.bfloat16)
        return carry

    lax.fori_loop(0, blocks, finish, 0)


def attend_back(saved, grads, tables, heads, scale):
    slots = grads[0].shape[0]
    half = jax.ShapeDtypeStruct((slots, 3 * (heads // 2) * HEAD), jnp.bfloat16)
    wide = pltpu.VMEM((heads, slots, LANES), jnp.float32)
    return pl.pallas_call(
        partial(attend_back_kernel, heads, scale),
        out_shape=[half, half],
        in_specs=[VMEM] * 9,
        out_specs=[VMEM] * 2,
        scratch_shapes=[pltpu.VMEM((heads, slots, LANES), jnp.bfloat16), wide, wide, wide],
        compiler_params=pltpu.CompilerParams(vmem_limit_bytes=60 * 2**20),
        name="attend_back",
    )(*saved, *grads, *tables[:3])


def turn_tables(positions, visible):
    lane = jnp.arange(LANES)
    inside = lane < HEAD
    frequency = rope_base ** (-(lane % QUARTER).astype(jnp.float32) / QUARTER)
    by_row = positions[:, :1].astype(jnp.float32) * frequency
    by_column = positions[:, 1:].astype(jnp.float32) * frequency
    angles = jnp.where(lane < HEAD // 2, by_row, by_column)
    cosine = jnp.where(inside, jnp.cos(angles), 0.0)
    sine = jnp.where(inside, jnp.sin(angles), 0.0)
    leads = lane // QUARTER % 2 == 0
    hide = jnp.where((lane == HEAD) & ~visible[:, None], -1e30, 0.0)
    return cosine, jnp.where(leads, -sine, 0.0), jnp.where(leads, 0.0, sine), hide


def image_device(
    block_input,
    conditioning,
    patch_counts,
    positions,
    w_mod,
    b_mod,
    w_qkv,
    b_qkv,
    w_out,
    b_out,
    w_up,
    b_up,
    w_down,
    b_down,
    cotangent,
):
    own_rows, model_width = block_input.shape
    slot_count = own_rows * CORES
    shard_rows, _, feat = w_qkv.shape
    units = w_up.shape[1]
    heads = CORES * feat // HEAD
    scale = 1.0 / math.sqrt(HEAD)
    images = ZS * YS * XS
    z, y, x, core = place()
    data = z * YS + y
    bf16 = jnp.bfloat16

    def swap(values):
        return lax.ppermute(values, "tensor", CORE_SWAP)

    def both(values):
        return jnp.concatenate([values, swap(values)], 0)

    def own_sum(terms):
        return terms[:own_rows] + swap(terms[own_rows:].astype(bf16)).astype(jnp.float32)

    silu_cond = jax.nn.silu(conditioning).astype(bf16)
    every = exchange(
        silu_cond.astype(jnp.float32).reshape(-1, LANES), "dp", 0, gather=True
    ).reshape(images, model_width)
    silu_rows = lax.dynamic_slice_in_dim(every, data * shard_rows, shard_rows, 1).astype(bf16)
    mod_matrix = w_mod.astype(bf16).reshape(shard_rows, 6 * feat)
    mod_part = jnp.dot(silu_rows, mod_matrix, preferred_element_type=jnp.float32)
    mod_part = mod_part + jnp.where(data == 0, b_mod.reshape(-1), 0.0)
    mod_part = jnp.broadcast_to(
        mod_part.reshape(images, 1, 8, -1), (images, CORES, 8, 6 * feat // 8)
    ).reshape(images * CORES, 8, -1)
    mod_parts = exchange(mod_part, "all", 1).reshape(ZS * YS, XS * CORES, 6, feat)
    mod = mod_parts.sum(0).transpose(1, 0, 2).reshape(6, model_width)
    shift_one, scale_one, gate_one, shift_two, scale_two, gate_two = (mod[i] for i in range(6))

    shards = [
        jnp.concatenate([w_qkv.reshape(shard_rows, 3 * feat), w_out.T], 1).astype(bf16),
        w_up.astype(bf16),
        w_down.T.astype(bf16),
    ]
    first, up_full, down_full = gather_weights(shards, 2)
    biases = jnp.concatenate([b_qkv.reshape(-1), b_up])
    other_biases = lax.ppermute(biases, "tensor", X_SWAP)
    low_biases = jnp.where(x == 0, biases, other_biases)
    high_biases = jnp.where(x == 0, other_biases, biases)
    qkv_width = 3 * feat
    joined = first.shape[1] // XS

    own_slots = core * own_rows + jnp.arange(own_rows)
    other_slots = (1 - core) * own_rows + jnp.arange(own_rows)
    slots = jnp.concatenate([own_slots, other_slots])
    visible = slots < lax.dynamic_index_in_dim(patch_counts, x, 0, False)
    image_start = x * slot_count
    places = jnp.concatenate(
        [
            lax.dynamic_slice_in_dim(positions, image_start + core * own_rows, own_rows, 0),
            lax.dynamic_slice_in_dim(positions, image_start + (1 - core) * own_rows, own_rows, 0),
        ]
    )
    tables = turn_tables(places, visible)

    normal_one, inverse_one = row_norm(block_input)
    hidden_one = both((normal_one * (1.0 + scale_one) + shift_one).astype(bf16))
    projected = []
    for half, bias in enumerate((low_biases, high_biases)):
        matrix = first[:, half * joined : half * joined + 8 * LANES]
        row = jnp.pad(bias[:qkv_width], (0, 8 * LANES - qkv_width))
        projected.append(jnp.dot(hidden_one, matrix, preferred_element_type=jnp.float32) + row)
    attended, saved = attend(projected, tables, heads, scale)
    out_parts = [first[:, half * joined + qkv_width : (half + 1) * joined] for half in range(2)]
    branch_one = (
        own_sum(contract(attended[0], out_parts[0], 1, 1) + contract(attended[1], out_parts[1], 1, 1))
        + b_out
    )
    middle = block_input + gate_one * branch_one
    normal_two, inverse_two = row_norm(middle)
    hidden_two = both((normal_two * (1.0 + scale_two) + shift_two).astype(bf16))
    bias_up = jnp.concatenate([low_biases[qkv_width:], high_biases[qkv_width:]])
    up_pre = jnp.dot(hidden_two, up_full, preferred_element_type=jnp.float32) + bias_up
    activated = gelu_tanh(up_pre).astype(bf16)
    branch_two = own_sum(contract(activated, down_full, 1, 1)) + b_down
    block_output = middle + gate_two * branch_two

    def norm_back(grad_hidden, normal, inverse, factor):
        grad_normal = grad_hidden * (1.0 + factor)
        mean_plain = jnp.mean(grad_normal, 1, keepdims=True)
        mean_cross = jnp.mean(grad_normal * normal, 1, keepdims=True)
        return inverse[:, None] * (grad_normal - mean_plain - normal * mean_cross)

    def column_sum(values):
        return jnp.sum(values.astype(jnp.float32), 0)

    grad_gate_two = jnp.sum(cotangent * branch_two, 0)
    grad_rows_two = both((cotangent * gate_two).astype(bf16))
    grad_bdown = column_sum(grad_rows_two)
    grad_down = contract(grad_rows_two, activated, 0, 0).astype(bf16)
    grad_activated = jnp.dot(grad_rows_two, down_full, preferred_element_type=jnp.float32)
    grad_up = jax.vjp(gelu_tanh, up_pre)[1](grad_activated)[0].astype(bf16)
    grad_bup = column_sum(grad_up)
    grad_wup = contract(hidden_two, grad_up, 0, 0).astype(bf16)
    grad_hidden_two = own_sum(contract(grad_up, up_full, 1, 1))
    grad_shift_two = jnp.sum(grad_hidden_two, 0)
    grad_scale_two = jnp.sum(grad_hidden_two * normal_two, 0)
    grad_middle = cotangent + norm_back(grad_hidden_two, normal_two, inverse_two, scale_two)
    grad_gate_one = jnp.sum(grad_middle * branch_one, 0)
    grad_rows_one = both((grad_middle * gate_one).astype(bf16))
    grad_bout = column_sum(grad_rows_one)
    grad_attended = [
        jnp.dot(grad_rows_one, part, preferred_element_type=jnp.float32).astype(bf16)
        for part in out_parts
    ]
    grad_projected = attend_back(saved, grad_attended, tables, heads, scale)
    first_parts, hidden_terms, bias_terms = [], 0.0, []
    for half in range(2):
        first_parts.append(contract(hidden_one, grad_projected[half], 0, 0).astype(bf16))
        first_parts.append(contract(grad_rows_one, attended[half], 0, 0).astype(bf16))
        matrix = first[:, half * joined : half * joined + qkv_width]
        hidden_terms = hidden_terms + contract(grad_projected[half], matrix, 1, 1)
        bias_terms.append(column_sum(grad_projected[half]))
    grad_first = jnp.concatenate(first_parts, 1)
    grad_hidden_one = own_sum(hidden_terms)
    grad_shift_one = jnp.sum(grad_hidden_one, 0)
    grad_scale_one = jnp.sum(grad_hidden_one * normal_one, 0)
    grad_input = grad_middle + norm_back(grad_hidden_one, normal_one, inverse_one, scale_one)

    sum_down, sum_up, sum_first = scatter_grads([grad_down, grad_wup, grad_first], 3)
    grad_wqkv = sum_first[:, :qkv_width].reshape(shard_rows, 3, feat)
    grad_wout = sum_first[:, qkv_width:].T
    grad_wdown = sum_down.T

    grad_mod = jnp.stack(
        [
            grad_shift_one,
            grad_scale_one,
            grad_gate_one,
            grad_shift_two,
            grad_scale_two,
            grad_gate_two,
        ]
    )
    grad_mod = (grad_mod + swap(grad_mod)).astype(bf16).astype(jnp.float32)
    grad_mod = grad_mod.reshape(6, XS, CORES, feat)
    grad_mod = lax.dynamic_index_in_dim(grad_mod, core, 2, False)
    small = 6 * feat + qkv_width + units + 2 * model_width
    lines = -(-small // LANES)
    sends = []
    for half in range(2):
        flat = jnp.concatenate(
            [
                grad_mod[:, half].reshape(-1),
                bias_terms[half],
                grad_bup[half * units : (half + 1) * units],
                grad_bout,
                grad_bdown,
            ]
        )
        sends.append(jnp.pad(flat, (0, lines * LANES - small)).reshape(1, lines, LANES))
    blocks = jnp.broadcast_to(jnp.stack(sends, 1), (ZS * YS, 2, lines, LANES))
    small_all = exchange(blocks.reshape(images, lines, LANES), "same_core", 4).reshape(images, -1)
    mod_all = small_all[:, : 6 * feat]
    summed = jnp.sum(small_all, 0)
    grad_bmod = summed[: 6 * feat].reshape(6, feat)
    offset = 6 * feat
    grad_bqkv = summed[offset : offset + qkv_width].reshape(3, feat)
    offset += qkv_width
    grad_bup = summed[offset : offset + units]
    offset += units
    grad_bout = summed[offset : offset + model_width]
    grad_bdown = summed[offset + model_width : offset + 2 * model_width]
    mod_all = mod_all.astype(bf16)
    grad_wmod = contract(silu_rows, mod_all, 0, 0).reshape(shard_rows, 6, feat)
    silu_part = contract(mod_all, mod_matrix, 1, 1).reshape(ZS * YS, 1, -1)
    silu_part = jnp.pad(silu_part, ((0, 0), (0, 0), (0, 8 * LANES - XS * shard_rows)))
    silu_part = jnp.broadcast_to(silu_part, (ZS * YS, XS * CORES, 8 * LANES))
    silu_all = exchange(silu_part.reshape(-1, 8, LANES), "all", 5)
    silu_all = silu_all.reshape(ZS * YS, XS * CORES, -1)[:, :, : XS * shard_rows].sum(1)
    grad_silu = silu_all.reshape(ZS * YS, XS, shard_rows).transpose(1, 0, 2).reshape(XS, model_width)
    grad_cond = jax.vjp(jax.nn.silu, conditioning)[1](grad_silu)[0]
    return (
        block_output,
        grad_input,
        grad_cond,
        grad_wmod,
        grad_bmod,
        grad_wqkv,
        grad_bqkv,
        grad_wout,
        grad_bout,
        sum_up,
        grad_bup,
        grad_wdown,
        grad_bdown,
    )


def solution(mesh):
    body = image_device if image_per_chip(mesh) else per_device
    placed = (
        P(("dp", "tensor"), None),
        P("dp", None),
        P("dp"),
        P("dp", None),
        P("dp", None, "tensor"),
        P(None, "tensor"),
        P("dp", None, "tensor"),
        P(None, "tensor"),
        P("tensor", "dp"),
        P(),
        P("dp", "tensor"),
        P("tensor"),
        P("tensor", "dp"),
        P(),
        P(("dp", "tensor"), None),
    )
    return jax.shard_map(
        body,
        mesh=mesh,
        in_specs=placed,
        out_specs=(
            P(("dp", "tensor"), None),
            P(("dp", "tensor"), None),
            P("dp", None),
            P("dp", None, "tensor"),
            P(None, "tensor"),
            P("dp", None, "tensor"),
            P(None, "tensor"),
            P("tensor", "dp"),
            P(),
            P("dp", "tensor"),
            P("tensor"),
            P("tensor", "dp"),
            P(),
        ),
        check_vma=False,
    )
```

```python
from functools import partial
import math

import jax
import jax.numpy as jnp
from jax import lax
from jax.experimental import pallas as pl
from jax.experimental.pallas import tpu as pltpu
from jax.sharding import PartitionSpec as P

HEAD = 72


epsilon = 1e-06
rope_base = 10000.0
gelu_coeff = 0.044715
root_two_pi = math.sqrt(2.0 / math.pi)


def gelu_tanh(values):
    return (
        0.5
        * values
        * (1.0 + jnp.tanh(root_two_pi * (values + gelu_coeff * values * values * values)))
    )


def rotate(values, positions, direction):
    quarter = values.shape[-1] // 4
    frequency = rope_base ** (-jnp.arange(quarter, dtype=jnp.float32) / quarter)
    pieces = []
    for column in range(2):
        angles = positions[:, column].astype(jnp.float32)[:, None, None] * frequency
        cosine = jnp.cos(angles)
        sine_term = direction * jnp.sin(angles)
        leading = values[..., 2 * column * quarter : (2 * column + 1) * quarter]
        trailing = values[..., (2 * column + 1) * quarter : (2 * column + 2) * quarter]
        pieces.append(leading * cosine - trailing * sine_term)
        pieces.append(leading * sine_term + trailing * cosine)
    return jnp.concatenate(pieces, -1)


def contract(left, right, left_dim, right_dim):
    return lax.dot_general(
        left, right, (((left_dim,), (right_dim,)), ((), ())), preferred_element_type=jnp.float32
    )


def exact_dot(left, right):
    return jnp.dot(left, right, precision=lax.Precision.HIGHEST, preferred_element_type=jnp.float32)


def row_norm(rows):
    average = jnp.mean(rows, 1)
    inverse = lax.rsqrt(jnp.mean(rows * rows, 1) - average * average + epsilon)
    return ((rows - average[:, None]) * inverse[:, None], inverse)


def masked_scores(query_rows, key_rows, patch_count, factor):
    raw_scores = (
        jnp.einsum("qhd,khd->hqk", query_rows, key_rows, preferred_element_type=jnp.float32)
        * factor
    )
    visible = jnp.arange(key_rows.shape[0]) < patch_count
    return jnp.where(visible[None, None, :], raw_scores, -1e30)


def attend_forward(factor, inputs):
    query_rows, key_rows, value_rows, patch_count = inputs
    scores = masked_scores(query_rows, key_rows, patch_count, factor)
    highest = jnp.max(scores, -1, keepdims=True)
    exponent = jnp.exp(scores - highest)
    denominator = jnp.sum(exponent, -1, keepdims=True)
    softmax_rows = (exponent / denominator).astype(jnp.bfloat16)
    attended = jnp.einsum(
        "hqk,khd->qhd", softmax_rows, value_rows, preferred_element_type=jnp.float32
    )
    return (attended, (highest + jnp.log(denominator))[..., 0])


def attend_backward(factor, inputs):
    query_rows, key_rows, value_rows, patch_count, logsum, grad_rows = inputs
    scores = masked_scores(query_rows, key_rows, patch_count, factor)
    softmax_rows = jnp.exp(scores - logsum[..., None])
    grad_soft = jnp.einsum(
        "qhd,khd->hqk", grad_rows, value_rows, preferred_element_type=jnp.float32
    )
    grad_values = jnp.einsum(
        "hqk,qhd->khd",
        softmax_rows.astype(jnp.bfloat16),
        grad_rows,
        preferred_element_type=jnp.float32,
    )
    inner_sum = jnp.sum(softmax_rows * grad_soft, -1, keepdims=True)
    grad_scores = (softmax_rows * (grad_soft - inner_sum) * factor).astype(jnp.bfloat16)
    grad_query = jnp.einsum(
        "hqk,khd->qhd", grad_scores, key_rows, preferred_element_type=jnp.float32
    )
    grad_keys = jnp.einsum(
        "hqk,qhd->khd", grad_scores, query_rows, preferred_element_type=jnp.float32
    )
    return (grad_query, grad_keys, grad_values)


def per_device(
    block_input,
    conditioning,
    patch_counts,
    positions,
    w_mod,
    b_mod,
    w_qkv,
    b_qkv,
    w_out,
    b_out,
    w_up,
    b_up,
    w_down,
    b_down,
    cotangent,
):
    own_rows, model_width = block_input.shape
    group_rows = positions.shape[0]
    images_local = conditioning.shape[0]
    slot_count = group_rows // images_local
    feat_local = w_qkv.shape[2]
    heads_local = feat_local // HEAD
    row_start = lax.axis_index("tensor") * own_rows
    factor = 1.0 / math.sqrt(HEAD)
    image_of = (row_start + jnp.arange(own_rows)) // slot_count
    one_hot = (image_of[:, None] == jnp.arange(images_local)[None, :]).astype(jnp.float32)

    def to_rows(vectors):
        return exact_dot(one_hot, vectors)

    def to_images(values):
        return exact_dot(one_hot.T, values)

    def per_image(stacked):
        return stacked.reshape((images_local, slot_count) + stacked.shape[1:])

    def modulate_group(values, shift, scale):
        shaped = values.reshape(images_local, slot_count, values.shape[1])
        return (shaped * (1.0 + scale[:, None, :]) + shift[:, None, :]).reshape(values.shape)

    mod_full, qkv_full, out_full, up_full, down_full = (
        lax.all_gather(w_mod.astype(jnp.bfloat16), "dp", axis=0, tiled=True),
        lax.all_gather(w_qkv.astype(jnp.bfloat16), "dp", axis=0, tiled=True),
        lax.all_gather(w_out.astype(jnp.bfloat16), "dp", axis=1, tiled=True),
        lax.all_gather(w_up.astype(jnp.bfloat16), "dp", axis=0, tiled=True),
        lax.all_gather(w_down.astype(jnp.bfloat16), "dp", axis=1, tiled=True),
    )
    silu_cond = jax.nn.silu(conditioning).astype(jnp.bfloat16)
    mod_cols = jnp.dot(
        silu_cond, mod_full.reshape(model_width, 6 * feat_local), preferred_element_type=jnp.float32
    )
    mod_cols = mod_cols.reshape(images_local, 6, feat_local) + b_mod
    mod_all = lax.all_gather(mod_cols, "tensor", axis=2, tiled=True)

    def norm_gather(rows_local, shift, scale):
        rows_group = lax.all_gather(rows_local, "tensor", axis=0, tiled=True)
        normal_group, inverse_group = row_norm(rows_group)
        hidden = modulate_group(normal_group, shift, scale).astype(jnp.bfloat16)
        normal = lax.dynamic_slice_in_dim(normal_group, row_start, own_rows, 0)
        inverse = lax.dynamic_slice_in_dim(inverse_group, row_start, own_rows, 0)
        return (hidden, normal, inverse)

    hidden_one, normal_one, inverse_one = norm_gather(block_input, mod_all[:, 0], mod_all[:, 1])
    projected = jnp.dot(
        hidden_one,
        qkv_full.reshape(model_width, 3 * feat_local),
        preferred_element_type=jnp.float32,
    ) + b_qkv.reshape(-1)
    projected = projected.reshape(group_rows, 3, heads_local, HEAD)
    query_rows = rotate(projected[:, 0], positions, 1.0).astype(jnp.bfloat16)
    key_rows = rotate(projected[:, 1], positions, 1.0).astype(jnp.bfloat16)
    value_rows = projected[:, 2].astype(jnp.bfloat16)
    attended, logsum = lax.map(
        partial(attend_forward, factor),
        (per_image(query_rows), per_image(key_rows), per_image(value_rows), patch_counts),
    )
    attended = attended.reshape(group_rows, feat_local).astype(jnp.bfloat16)

    def branch_sum(partial_terms, offset):
        return lax.psum_scatter(partial_terms, "tensor", scatter_dimension=0, tiled=True) + offset

    gate_one_rows = to_rows(mod_all[:, 2])
    gate_two_rows = to_rows(mod_all[:, 5])
    branch_one = branch_sum(jnp.dot(attended, out_full, preferred_element_type=jnp.float32), b_out)
    middle = block_input + gate_one_rows * branch_one
    hidden_two, normal_two, inverse_two = norm_gather(middle, mod_all[:, 3], mod_all[:, 4])
    up_pre = jnp.dot(hidden_two, up_full, preferred_element_type=jnp.float32) + b_up
    activated = gelu_tanh(up_pre).astype(jnp.bfloat16)
    branch_two = branch_sum(
        jnp.dot(activated, down_full, preferred_element_type=jnp.float32), b_down
    )
    block_output = middle + gate_two_rows * branch_two
    mod_back, qkv_back, out_back, up_back, down_back = (
        lax.all_gather(w_mod.astype(jnp.bfloat16), "dp", axis=0, tiled=True),
        lax.all_gather(w_qkv.astype(jnp.bfloat16), "dp", axis=0, tiled=True),
        lax.all_gather(w_out.astype(jnp.bfloat16), "dp", axis=1, tiled=True),
        lax.all_gather(w_up.astype(jnp.bfloat16), "dp", axis=0, tiled=True),
        lax.all_gather(w_down.astype(jnp.bfloat16), "dp", axis=1, tiled=True),
    )

    def spread_grad(grad_branch):
        return lax.all_gather(grad_branch, "tensor", axis=0, tiled=True)

    def input_sum(partial_terms):
        return lax.psum_scatter(partial_terms, "tensor", scatter_dimension=0, tiled=True)

    def norm_backward(grad_hidden, normal, inverse, scale):
        grad_normal = grad_hidden * (1.0 + to_rows(scale))
        mean_plain = jnp.mean(grad_normal, 1, keepdims=True)
        mean_cross = jnp.mean(grad_normal * normal, 1, keepdims=True)
        return inverse[:, None] * (grad_normal - mean_plain - normal * mean_cross)

    grad_gate_two = to_images(cotangent * branch_two)
    grad_branch_two = (cotangent * gate_two_rows).astype(jnp.bfloat16)
    grad_rows_two = spread_grad(grad_branch_two)
    grad_bdown_local = jnp.sum(grad_rows_two.astype(jnp.float32), 0)
    grad_wdown_local = contract(activated, grad_rows_two, 0, 0)
    grad_activated = contract(grad_rows_two, down_back, 1, 1)
    gelu_pull = jax.vjp(gelu_tanh, up_pre)[1]
    grad_up = gelu_pull(grad_activated)[0].astype(jnp.bfloat16)
    grad_bup_local = jnp.sum(grad_up.astype(jnp.float32), 0)
    grad_wup_local = contract(hidden_two, grad_up, 0, 0)
    grad_hidden_two = input_sum(contract(grad_up, up_back, 1, 1))
    grad_shift_two = to_images(grad_hidden_two)
    grad_scale_two = to_images(grad_hidden_two * normal_two)
    grad_middle = cotangent + norm_backward(grad_hidden_two, normal_two, inverse_two, mod_all[:, 4])
    grad_gate_one = to_images(grad_middle * branch_one)
    grad_branch_one = (grad_middle * gate_one_rows).astype(jnp.bfloat16)
    grad_rows_one = spread_grad(grad_branch_one)
    grad_bout_local = jnp.sum(grad_rows_one.astype(jnp.float32), 0)
    grad_wout_local = contract(attended, grad_rows_one, 0, 0)
    grad_attended = contract(grad_rows_one, out_back, 1, 1).astype(jnp.bfloat16)
    grad_attended = grad_attended.reshape(group_rows, heads_local, HEAD)
    grad_query, grad_keys, grad_values = lax.map(
        partial(attend_backward, factor),
        (
            per_image(query_rows),
            per_image(key_rows),
            per_image(value_rows),
            patch_counts,
            logsum,
            per_image(grad_attended),
        ),
    )
    head_shape = (group_rows, heads_local, HEAD)
    grad_projected = jnp.stack(
        [
            rotate(grad_query.reshape(head_shape), positions, -1.0),
            rotate(grad_keys.reshape(head_shape), positions, -1.0),
            grad_values.reshape(head_shape),
        ],
        1,
    )
    grad_projected = grad_projected.astype(jnp.bfloat16).reshape(group_rows, 3 * feat_local)
    grad_bqkv_local = jnp.sum(grad_projected.astype(jnp.float32), 0).reshape(3, feat_local)
    grad_wqkv_local = contract(hidden_one, grad_projected, 0, 0).reshape(model_width, 3, feat_local)
    grad_hidden_one = input_sum(
        contract(grad_projected, qkv_back.reshape(model_width, 3 * feat_local), 1, 1)
    )
    grad_shift_one = to_images(grad_hidden_one)
    grad_scale_one = to_images(grad_hidden_one * normal_one)
    grad_input = grad_middle + norm_backward(
        grad_hidden_one, normal_one, inverse_one, mod_all[:, 1]
    )
    grad_mod_part = jnp.stack(
        [
            grad_shift_one,
            grad_scale_one,
            grad_gate_one,
            grad_shift_two,
            grad_scale_two,
            grad_gate_two,
        ],
        1,
    )
    grad_mod = lax.psum_scatter(grad_mod_part, "tensor", scatter_dimension=2, tiled=True).astype(
        jnp.bfloat16
    )
    grad_bmod_local = jnp.sum(grad_mod.astype(jnp.float32), 0)
    grad_mod_flat = grad_mod.reshape(images_local, 6 * feat_local)
    grad_wmod_local = contract(silu_cond, grad_mod_flat, 0, 0).reshape(model_width, 6, feat_local)
    grad_silu = lax.psum(
        contract(grad_mod_flat, mod_back.reshape(model_width, 6 * feat_local), 1, 1), "tensor"
    )
    silu_pull = jax.vjp(jax.nn.silu, conditioning)[1]
    grad_cond = silu_pull(grad_silu)[0]
    grad_wmod, grad_wqkv, grad_wout, grad_wup, grad_wdown = (
        lax.psum_scatter(
            grad_wmod_local.astype(jnp.bfloat16), "dp", scatter_dimension=0, tiled=True
        ).astype(jnp.float32),
        lax.psum_scatter(
            grad_wqkv_local.astype(jnp.bfloat16), "dp", scatter_dimension=0, tiled=True
        ).astype(jnp.float32),
        lax.psum_scatter(
            grad_wout_local.astype(jnp.bfloat16), "dp", scatter_dimension=1, tiled=True
        ).astype(jnp.float32),
        lax.psum_scatter(
            grad_wup_local.astype(jnp.bfloat16), "dp", scatter_dimension=0, tiled=True
        ).astype(jnp.float32),
        lax.psum_scatter(
            grad_wdown_local.astype(jnp.bfloat16), "dp", scatter_dimension=1, tiled=True
        ).astype(jnp.float32),
    )
    grad_bmod, grad_bqkv, grad_bout, grad_bup, grad_bdown = lax.psum(
        (grad_bmod_local, grad_bqkv_local, grad_bout_local, grad_bup_local, grad_bdown_local), "dp"
    )
    return (
        block_output,
        grad_input,
        grad_cond,
        grad_wmod,
        grad_bmod,
        grad_wqkv,
        grad_bqkv,
        grad_wout,
        grad_bout,
        grad_wup,
        grad_bup,
        grad_wdown,
        grad_bdown,
    )


LANES = 128
ZS, YS, XS, CORES = 4, 2, 2, 2
MESH_ID = pl.DeviceIdType.MESH
CORE_SWAP = [(0, 1), (1, 0), (2, 3), (3, 2)]
X_SWAP = [(0, 2), (2, 0), (1, 3), (3, 1)]
LOG2E = 1.0 / math.log(2.0)
HBM = pl.BlockSpec(memory_space=pl.ANY)
VMEM = pl.BlockSpec(memory_space=pltpu.VMEM)


def image_per_chip(mesh):
    return dict(mesh.shape) == {"dp": ZS * YS, "tensor": XS * CORES}


def place():
    data, tensor = lax.axis_index("dp"), lax.axis_index("tensor")
    return data // YS, data % YS, tensor // CORES, tensor % CORES


def flip_z(z, step):
    high, low = z // 2, z % 2
    if step & 2:
        high = 1 - high
    if step & 1:
        low = 1 - low
    return high * 2 + low


def device(z, y, x, core):
    return (z * YS + y, x * CORES + core)


def greet(targets):
    barrier = pltpu.get_barrier_semaphore()
    for target in targets:
        pl.semaphore_signal(barrier, inc=1, device_id=target, device_id_type=MESH_ID)
    pl.semaphore_wait(barrier, len(targets))


GATHER_STEPS, SCATTER_STEPS = 5, 6


def grouped(matrices, rows, unit):
    groups = []
    for matrix in matrices:
        for row in range(0, rows, 3 * unit):
            short = len(groups) % 2
            groups.append(
                [
                    (matrix, row, unit, 2),
                    (matrix, row + unit, unit, 3),
                    (matrix, row + 2 * unit, unit, short),
                ]
            )
    return groups


def numbered(groups):
    chunks, members = [], []
    for group in groups:
        members.append(range(len(chunks), len(chunks) + len(group)))
        chunks.extend(group)
    return chunks, members


def ticks_of(members, steps, act):
    def tick(time):
        for group, numbers in enumerate(members):
            step = time - group
            if 0 <= step < steps:
                for number in numbers:
                    act(number, step)

    return [partial(tick, time) for time in range(len(members) + steps - 1)]


def gather_plan(groups, shards, wholes, sends, recvs, local):
    chunks, members = numbered(groups)
    z, y, x, core = place()
    inner = jnp.logical_or(z == 1, z == 2)
    width = shards[0].shape[1]
    mine = pl.ds(pl.multiple_of(x * width, LANES), width)
    every = slice(None)
    at_x, at_y = device(z, y, 1 - x, core), device(z, 1 - y, x, core)
    beside, mirror = device(flip_z(z, 1), y, x, core), device(3 - z, y, x, core)
    pair = pl.ds(z // 2 * 2, 2)
    far = pl.ds(2 - z // 2 * 2, 2)

    def copy(number, send, recv, source, target, where):
        return pltpu.make_async_remote_copy(
            src_ref=source,
            dst_ref=target,
            send_sem=sends.at[number * 5 + send],
            recv_sem=recvs.at[number * 4 + recv],
            device_id=where,
            device_id_type=MESH_ID,
        )

    def moves(number):
        matrix, row, rows, route = chunks[number]
        whole, span = wholes[matrix], pl.ds(row, rows)
        own, shard = whole.at[z, y, span, mine], shards[matrix].at[span, :]
        lines, columns = (every if route == 3 else y), (every if route == 2 else mine)
        made = {}
        near = shard if route < 2 else whole.at[z, lines, span, columns]
        near_to = own if route < 2 else near
        made["near"] = partial(copy, number, 0, 0, near, near_to, beside)
        both = whole.at[pair, lines, span, columns]
        made["mirror"] = partial(copy, number, 1, 1, both, both, mirror)
        there = whole.at[far, lines, span, columns]
        made["forward"] = partial(copy, number, 2, 1, there, there, beside)
        if route < 2:
            column = whole.at[:, y, span, mine]
            made["second"] = partial(copy, number, 3, 2, column, column, at_x if route == 0 else at_y)
        else:
            made["first"] = partial(copy, number, 3, 2, shard, own, at_x if route == 2 else at_y)
        if route in (0, 2):
            last = whole.at[:, y, span, :]
        else:
            last = whole.at[:, :, span, mine]
        made["third"] = partial(copy, number, 4, 3, last, last, at_y if route in (0, 2) else at_x)
        return made

    def keep(matrix):
        return pltpu.make_async_copy(
            shards[matrix], wholes[matrix].at[z, y, :, mine], local.at[matrix]
        )

    kept = []

    def ready(number):
        matrix = chunks[number][0]
        if matrix not in kept:
            kept.append(matrix)
            keep(matrix).wait()

    def act(number, step):
        made = moves(number)
        straight = chunks[number][3] < 2
        if step == 0:
            made["near" if straight else "first"]().start()
        elif step == 1:
            ready(number)
            if straight:
                made["near"]().wait_recv()
                pl.when(inner)(lambda: made["mirror"]().start())
            else:
                made["first"]().wait_recv()
                made["near"]().start()
        elif step == 2:
            if straight:
                made["mirror"]().wait_recv()
                pl.when(inner)(lambda: made["forward"]().start())
                made["second"]().start()
            else:
                made["near"]().wait_recv()
                pl.when(inner)(lambda: made["mirror"]().start())
        elif step == 3:
            if straight:
                made["second"]().wait_recv()
            else:
                made["mirror"]().wait_recv()
                pl.when(inner)(lambda: made["forward"]().start())
            made["third"]().start()
        else:
            made["third"]().wait_recv()

    def start():
        for matrix in sorted({chunk[0] for chunk in chunks}):
            keep(matrix).start()

    def finish():
        for number in range(len(chunks)):
            made = moves(number)
            for name in made:
                if name not in ("mirror", "forward"):
                    made[name]().wait_send()

            def rest(made=made):
                made["mirror"]().wait_send()
                made["forward"]().wait_send()

            pl.when(inner)(rest)

    return start, ticks_of(members, GATHER_STEPS, act), finish


def gather_scratch(groups, matrices):
    count = sum(len(group) for group in groups)
    return [
        pltpu.SemaphoreType.DMA((count * 5,)),
        pltpu.SemaphoreType.DMA((count * 4,)),
        pltpu.SemaphoreType.DMA((matrices,)),
    ]


def scatter_plan(groups, parts, sums, buffers, sends, recvs, local):
    chunks, members = numbered(groups)
    own, first_in, second_in, outer_in, mirror_in, near_in, last_in = buffers
    z, y, x, core = place()
    inner = jnp.logical_or(z == 1, z == 2)
    outer = jnp.logical_or(z == 0, z == 3)
    width = sums[0].shape[1]
    mine = pl.ds(pl.multiple_of(x * width, LANES), width)
    theirs = pl.ds(pl.multiple_of((1 - x) * width, LANES), width)
    at_x, at_y = device(z, y, 1 - x, core), device(z, 1 - y, x, core)
    z_near = flip_z(z, 1)
    beside, mirror = device(z_near, y, x, core), device(3 - z, y, x, core)
    pair_at, far_at = z // 2 * 2, 2 - z // 2 * 2
    pair, far = pl.ds(pair_at, 2), pl.ds(far_at, 2)

    def copy(number, index, source, target, where):
        return pltpu.make_async_remote_copy(
            src_ref=source,
            dst_ref=target,
            send_sem=sends.at[number * 6 + index],
            recv_sem=recvs.at[number * 6 + index],
            device_id=where,
            device_id_type=MESH_ID,
        )

    def moves(number):
        matrix, row, rows, route = chunks[number]
        part, span = parts[matrix], pl.ds(row, rows)
        by_y = route in (0, 2)
        made = {}
        for slot in range(2):
            if by_y:
                column = mine if slot == 0 else theirs
                source, kept = part.at[:, 1 - y, span, column], part.at[:, y, span, column]
            else:
                line = y if slot == 0 else 1 - y
                source, kept = part.at[:, line, span, theirs], part.at[:, line, span, mine]
            made["first", slot] = partial(
                copy,
                number,
                slot,
                source,
                first_in.at[matrix, slot, :, span, :],
                at_y if by_y else at_x,
            )
            made["load", slot] = partial(
                pltpu.make_async_copy,
                kept, own.at[matrix, slot, :, span, :], local.at[number * 2 + slot]
            )
        if route < 2:
            made["second"] = partial(
                copy,
                number,
                2,
                own.at[matrix, 1, :, span, :],
                second_in.at[matrix, :, span, :],
                at_x if by_y else at_y,
            )
            slots = 0
        else:
            made["last"] = partial(
                copy,
                number,
                2,
                own.at[matrix, 1, z, span, :],
                last_in.at[matrix, span, :],
                at_x if by_y else at_y,
            )
            slots = slice(None)
        made["outer"] = partial(
                copy,
            number,
            3,
            own.at[matrix, slots, far, span, :],
            outer_in.at[matrix, slots, :, span, :],
            beside,
        )
        made["mirror"] = partial(
                copy,
            number,
            4,
            own.at[matrix, slots, far, span, :],
            mirror_in.at[matrix, slots, :, span, :],
            mirror,
        )
        made["near"] = partial(
                copy,
            number,
            5,
            own.at[matrix, slots, z_near, span, :],
            near_in.at[matrix, slots, span, :],
            beside,
        )
        return made

    def add(rows, row, target, arrived):
        def one(i, carry):
            at = pl.ds(pl.multiple_of(row + i * 16, 16), 16)
            held = own[(*target, at, slice(None))].astype(jnp.float32)
            incoming = arrived[0][(*arrived[1], at, slice(None))].astype(jnp.float32)
            own[(*target, at, slice(None))] = (held + incoming).astype(jnp.bfloat16)
            return carry

        lax.fori_loop(0, rows // 16, one, 0)

    def add_blocks(number, count, target, arrived):
        matrix, row, rows, route = chunks[number]

        def one(i, carry):
            ref, index = arrived(i)
            add(rows, row, (matrix, *target(i)), (ref, (matrix, *index)))
            return carry

        lax.fori_loop(0, count, one, 0)

    def finalize(number, ref, index):
        matrix, row, rows, route = chunks[number]

        def one(i, carry):
            at = pl.ds(pl.multiple_of(row + i * 16, 16), 16)
            sums[matrix][at, :] = own[matrix, 0, z, at, :].astype(jnp.float32) + ref[
                (matrix, *index, at, slice(None))
            ].astype(jnp.float32)
            return carry

        lax.fori_loop(0, rows // 16, one, 0)

    def act(number, step):
        made = moves(number)
        straight = chunks[number][3] < 2
        count = 2 if straight else 4
        slots = 1 if straight else 2

        def from_outer():
            made["outer"]().wait_recv()
            add_blocks(
                number,
                count,
                lambda i: (i // 2, far_at + i % 2),
                lambda i: (outer_in, (i // 2, i % 2)),
            )
            made["mirror"]().start()

        def from_mirror():
            made["mirror"]().wait_recv()
            add_blocks(
                number,
                count,
                lambda i: (i // 2, pair_at + i % 2),
                lambda i: (mirror_in, (i // 2, i % 2)),
            )

        if step == 0:
            for slot in (1, 0):
                made["first", slot]().start()
                made["load", slot]().start()
        elif step == 1:
            for slot in (1, 0):
                made["first", slot]().wait_recv()
                made["load", slot]().wait()
                add_blocks(
                    number,
                    ZS,
                    lambda i, slot=slot: (slot, i),
                    lambda i, slot=slot: (first_in, (slot, i)),
                )
                if straight and slot == 1:
                    made["second"]().start()
            if not straight:
                pl.when(outer)(lambda: made["outer"]().start())
        elif straight:
            if step == 2:
                made["second"]().wait_recv()
                add_blocks(number, ZS, lambda i: (0, i), lambda i: (second_in, (i,)))
                pl.when(outer)(lambda: made["outer"]().start())
            elif step == 3:
                pl.when(inner)(from_outer)
            elif step == 4:
                pl.when(inner)(from_mirror)
                made["near"]().start()
            else:
                made["near"]().wait_recv()
                finalize(number, near_in, (0,))
        elif step == 2:
            pl.when(inner)(from_outer)
        elif step == 3:
            pl.when(inner)(from_mirror)
            made["near"]().start()
        elif step == 4:
            made["near"]().wait_recv()
            add_blocks(number, 2, lambda i: (i, z), lambda i: (near_in, (i,)))
            made["last"]().start()
        else:
            made["last"]().wait_recv()
            finalize(number, last_in, ())

    def finish():
        for number in range(len(chunks)):
            made = moves(number)
            for name in made:
                if name not in ("outer", "mirror") and name[0] != "load":
                    made[name]().wait_send()
            pl.when(outer)(lambda made=made: made["outer"]().wait_send())
            pl.when(inner)(lambda made=made: made["mirror"]().wait_send())

    return ticks_of(members, SCATTER_STEPS, act), finish


def scatter_scratch(groups, matrices, rows, width):
    count = sum(len(group) for group in groups)

    def wide(*lead):
        return pltpu.VMEM((matrices, *lead, rows, width), jnp.bfloat16)

    return [
        wide(2, ZS),
        wide(2, ZS),
        wide(ZS),
        wide(2, 2),
        wide(2, 2),
        wide(2),
        wide(),
        pltpu.SemaphoreType.DMA((count * 6,)),
        pltpu.SemaphoreType.DMA((count * 6,)),
        pltpu.SemaphoreType.DMA((count * 2,)),
    ]


def line_peers():
    z, y, x, core = place()
    return [
        device(z, y, 1 - x, core),
        device(z, 1 - y, x, core),
        device(flip_z(z, 1), y, x, core),
        device(3 - z, y, x, core),
    ]


def gather_kernel(groups, matrices, *refs):
    shards, wholes, scratch = refs[:matrices], refs[matrices : 2 * matrices], refs[2 * matrices :]
    greet(line_peers())
    start, ticks, finish = gather_plan(groups, shards, wholes, *scratch)
    start()
    for tick in ticks:
        tick()
    finish()


def whole_shape(shard):
    rows, width = shard.shape
    return jax.ShapeDtypeStruct((ZS, YS, rows, XS * width), jnp.bfloat16)


def gather_weights(shards, ident, unit=16):
    count = len(shards)
    groups = grouped(range(count), shards[0].shape[0], unit)
    return pl.pallas_call(
        partial(gather_kernel, groups, count),
        out_shape=[whole_shape(shard) for shard in shards],
        in_specs=[VMEM] * count,
        out_specs=[HBM] * count,
        scratch_shapes=gather_scratch(groups, count),
        compiler_params=pltpu.CompilerParams(collective_id=ident, has_side_effects=True),
        name="gather_weights",
    )(*shards)


def scatter_kernel(groups, matrices, *refs):
    parts, sums, scratch = refs[:matrices], refs[matrices : 2 * matrices], refs[2 * matrices :]
    greet(line_peers())
    ticks, finish = scatter_plan(groups, parts, sums, scratch[:7], *scratch[7:])
    for tick in ticks:
        tick()
    finish()


def split_rows(part):
    return part.reshape(ZS, YS, part.shape[0] // (ZS * YS), part.shape[1])


def scatter_grads(parts, ident, unit=16):
    parts = [split_rows(part) for part in parts]
    count = len(parts)
    rows, width = parts[0].shape[2], parts[0].shape[3] // XS
    groups = grouped(range(count), rows, unit)
    return pl.pallas_call(
        partial(scatter_kernel, groups, count),
        out_shape=[jax.ShapeDtypeStruct((rows, width), jnp.float32)] * count,
        in_specs=[HBM] * count,
        out_specs=[VMEM] * count,
        scratch_shapes=scatter_scratch(groups, count, rows, width),
        compiler_params=pltpu.CompilerParams(
            collective_id=ident, has_side_effects=True, vmem_limit_bytes=60 * 2**20
        ),
        name="scatter_grads",
    )(*parts)


def group_of(kind):
    z, y, x, core = place()
    data, tensor = z * YS + y, x * CORES + core
    if kind == "dp":
        return ZS * YS, data, lambda i: (i, tensor)
    if kind == "same_core":
        return ZS * YS * XS, data * XS + x, lambda i: (i // XS, (i % XS) * CORES + core)
    return (
        ZS * YS * XS * CORES,
        data * XS * CORES + tensor,
        lambda i: (i // (XS * CORES), i % (XS * CORES)),
    )


def exchange_kernel(kind, gather, blocks, arrived, sends, recvs):
    count, me, device_of = group_of(kind)
    targets = [(me + step) % count for step in range(1, count)]
    greet([device_of(target) for target in targets])
    copies = []
    for step, target in enumerate(targets):
        copy = pltpu.make_async_remote_copy(
            src_ref=blocks if gather else blocks.at[target],
            dst_ref=arrived.at[me],
            send_sem=sends.at[step],
            recv_sem=recvs.at[step],
            device_id=device_of(target),
            device_id_type=MESH_ID,
        )
        copy.start()
        copies.append(copy)
    arrived[me] = blocks[...] if gather else blocks[me]
    for copy in copies:
        copy.wait_send()
    for copy in copies:
        copy.wait_recv()


def exchange(blocks, kind, ident, gather=False):
    count = {"dp": ZS * YS, "same_core": ZS * YS * XS, "all": ZS * YS * XS * CORES}[kind]
    shape = blocks.shape if gather else blocks.shape[1:]
    return pl.pallas_call(
        partial(exchange_kernel, kind, gather),
        out_shape=jax.ShapeDtypeStruct((count,) + shape, blocks.dtype),
        in_specs=[VMEM],
        out_specs=VMEM,
        scratch_shapes=[
            pltpu.SemaphoreType.DMA((count - 1,)),
            pltpu.SemaphoreType.DMA((count - 1,)),
        ],
        compiler_params=pltpu.CompilerParams(collective_id=ident, has_side_effects=True),
        name="exchange_" + kind,
    )(blocks)


QUARTER = HEAD // 4
BLOCK = 256


def turn(values, tables, back):
    cosine, to_left, to_right = tables
    swapped = (
        pltpu.roll(values, LANES - QUARTER, axis=1) * to_left
        + pltpu.roll(values, QUARTER, axis=1) * to_right
    )
    return values * cosine - swapped if back else values * cosine + swapped


def spread(ticks, index, trips):
    for number, tick in enumerate(ticks):
        pl.when(index == number * trips // len(ticks))(tick)


def attend_kernel(heads, scale, groups, *refs):
    projected, (cos_ref, left_ref, right_ref, hide_ref) = refs[:2], refs[2:6]
    shards, out_refs = refs[6:8], refs[8:10]
    query_ref, key_ref, value_ref, logsum_ref = refs[10:14]
    wholes, held, gather_scratch_refs = refs[14:16], refs[16], refs[17:]
    slots = cos_ref.shape[0]
    per = heads // 2
    blocks = slots // BLOCK
    greet(line_peers())
    start, ticks, end = gather_plan(groups, shards, wholes, *gather_scratch_refs)
    start()
    ticks[0]()

    def prepare(i, carry):
        at = pl.ds(pl.multiple_of(i * BLOCK, BLOCK), BLOCK)
        tables = cos_ref[at, :], left_ref[at, :], right_ref[at, :]
        hide = hide_ref[at, :]
        lane = lax.broadcasted_iota(jnp.int32, (BLOCK, LANES), 1)
        for head in range(heads):
            source, local = projected[head // per], head % per
            for part, target in enumerate((query_ref, key_ref, value_ref)):
                start = (part * per + local) * HEAD
                values = source[at, start : start + LANES]
                if part == 2:
                    values = jnp.where(lane < HEAD, values, 0.0)
                else:
                    values = turn(values, tables, False)
                    values = values + (jnp.where(lane == HEAD, 1.0, 0.0) if part == 0 else hide)
                target[head, at, :] = values.astype(jnp.bfloat16)
        return carry

    lax.fori_loop(0, blocks, prepare, 0)

    def attend(i, carry):
        spread(ticks[1:], i, heads * blocks)
        head, block = i // blocks, i % blocks
        at = pl.ds(pl.multiple_of(block * BLOCK, BLOCK), BLOCK)
        scores = contract(query_ref[head, at, :], key_ref[head], 1, 1)
        highest = jnp.max(scores, 1, keepdims=True)
        exponent = jnp.exp2((scores - highest) * (scale * LOG2E))
        denominator = jnp.sum(exponent, 1, keepdims=True)
        result = jnp.dot(
            exponent.astype(jnp.bfloat16), value_ref[head], preferred_element_type=jnp.float32
        )
        held[head, at, :] = result / denominator
        logsum_ref[head, at, :] = jnp.broadcast_to(
            (highest * scale + jnp.log(denominator)) * LOG2E, (BLOCK, LANES)
        )
        return carry

    lax.fori_loop(0, heads * blocks, attend, 0)

    def finish(i, carry):
        at = pl.ds(pl.multiple_of(i * BLOCK, BLOCK), BLOCK)
        for half in range(2):
            row = jnp.concatenate(
                [held[half * per + local, at, :][:, :HEAD] for local in range(per)], 1
            )
            out_refs[half][at, :] = row.astype(jnp.bfloat16)
        return carry

    lax.fori_loop(0, blocks, finish, 0)
    end()


def attend(projected, tables, shards, heads, scale, ident):
    slots = projected[0].shape[0]
    count = len(shards)
    groups = grouped(range(count), shards[0].shape[0], 16)
    packed = jax.ShapeDtypeStruct((heads, slots, LANES), jnp.bfloat16)
    half = jax.ShapeDtypeStruct((slots, heads // 2 * HEAD), jnp.bfloat16)
    results = pl.pallas_call(
        partial(attend_kernel, heads, scale, groups),
        out_shape=[
            half,
            half,
            packed,
            packed,
            packed,
            jax.ShapeDtypeStruct((heads, slots, LANES), jnp.float32),
        ]
        + [whole_shape(shard) for shard in shards],
        in_specs=[VMEM] * (6 + count),
        out_specs=[VMEM] * 6 + [HBM] * count,
        scratch_shapes=[pltpu.VMEM((heads, slots, LANES), jnp.float32)]
        + gather_scratch(groups, count),
        compiler_params=pltpu.CompilerParams(
            collective_id=ident, has_side_effects=True, vmem_limit_bytes=60 * 2**20
        ),
        name="attend",
    )(*projected, *tables, *shards)
    return results[:2], results[2:6], results[6:]


def attend_back_kernel(heads, scale, groups, *refs):
    query_ref, key_ref, value_ref, logsum_ref = refs[:4]
    grads, (cos_ref, left_ref, right_ref) = refs[4:6], refs[6:9]
    parts, out_refs, sums = refs[9:11], refs[11:13], refs[13:15]
    held, grad_q, grad_k, grad_v = refs[15:19]
    buffers, semaphores = refs[19:26], refs[26:]
    slots = cos_ref.shape[0]
    per = heads // 2
    blocks = slots // BLOCK
    greet(line_peers())
    ticks, end = scatter_plan(groups, parts, sums, buffers, *semaphores)
    ticks[0]()

    def prepare(i, carry):
        at = pl.ds(pl.multiple_of(i * BLOCK, BLOCK), BLOCK)
        for head in range(heads):
            local = head % per
            piece = grads[head // per][at, local * HEAD : (local + 1) * HEAD]
            padding = jnp.zeros((BLOCK, LANES - HEAD), piece.dtype)
            held[head, at, :] = jnp.concatenate([piece, padding], 1)
        return carry

    lax.fori_loop(0, blocks, prepare, 0)

    def attend(i, carry):
        spread(ticks[1:], i, heads * blocks)
        head, block = i // blocks, i % blocks
        at = pl.ds(pl.multiple_of(block * BLOCK, BLOCK), BLOCK)
        query, grad = query_ref[head, at, :], held[head, at, :]
        key = key_ref[head]
        scores = contract(query, key, 1, 1)
        soft = jnp.exp2(scores * (scale * LOG2E) - logsum_ref[head, at, :1])
        grad_soft = contract(grad, value_ref[head], 1, 1)
        value_part = contract(soft.astype(jnp.bfloat16), grad, 0, 0)
        product = soft * grad_soft
        inner = jnp.sum(product, 1, keepdims=True)
        grad_scores = ((product - soft * inner) * scale).astype(jnp.bfloat16)
        grad_q[head, at, :] = jnp.dot(grad_scores, key, preferred_element_type=jnp.float32)
        key_part = contract(grad_scores, query, 0, 0)

        @pl.when(block == 0)
        def _():
            grad_v[head] = value_part
            grad_k[head] = key_part

        @pl.when(block > 0)
        def _():
            grad_v[head] += value_part
            grad_k[head] += key_part

        return carry

    lax.fori_loop(0, heads * blocks, attend, 0)

    def finish(i, carry):
        at = pl.ds(pl.multiple_of(i * BLOCK, BLOCK), BLOCK)
        tables = cos_ref[at, :], left_ref[at, :], right_ref[at, :]
        for half in range(2):
            pieces = []
            for part, source in enumerate((grad_q, grad_k, grad_v)):
                for local in range(per):
                    values = source[half * per + local, at, :]
                    if part < 2:
                        values = turn(values, tables, True)
                    pieces.append(values[:, :HEAD])
            out_refs[half][at, :] = jnp.concatenate(pieces, 1).astype(jnp.bfloat16)
        return carry

    lax.fori_loop(0, blocks, finish, 0)
    end()


def attend_back(saved, grads, tables, parts, heads, scale, ident):
    parts = [split_rows(part) for part in parts]
    count, rows, width = len(parts), parts[0].shape[2], parts[0].shape[3] // XS
    groups = grouped(range(count), rows, 16)
    slots = grads[0].shape[0]
    half = jax.ShapeDtypeStruct((slots, 3 * (heads // 2) * HEAD), jnp.bfloat16)
    wide = pltpu.VMEM((heads, slots, LANES), jnp.float32)
    results = pl.pallas_call(
        partial(attend_back_kernel, heads, scale, groups),
        out_shape=[half, half] + [jax.ShapeDtypeStruct((rows, width), jnp.float32)] * count,
        in_specs=[VMEM] * 9 + [HBM] * count,
        out_specs=[VMEM] * (2 + count),
        scratch_shapes=[pltpu.VMEM((heads, slots, LANES), jnp.bfloat16), wide, wide, wide]
        + scatter_scratch(groups, count, rows, width),
        compiler_params=pltpu.CompilerParams(
            collective_id=ident, has_side_effects=True, vmem_limit_bytes=63 * 2**20
        ),
        name="attend_back",
    )(*saved, *grads, *tables[:3], *parts)
    return results[:2], results[2:]


def turn_tables(positions, visible):
    lane = jnp.arange(LANES)
    inside = lane < HEAD
    frequency = rope_base ** (-(lane % QUARTER).astype(jnp.float32) / QUARTER)
    by_row = positions[:, :1].astype(jnp.float32) * frequency
    by_column = positions[:, 1:].astype(jnp.float32) * frequency
    angles = jnp.where(lane < HEAD // 2, by_row, by_column)
    cosine = jnp.where(inside, jnp.cos(angles), 0.0)
    sine = jnp.where(inside, jnp.sin(angles), 0.0)
    leads = lane // QUARTER % 2 == 0
    hide = jnp.where((lane == HEAD) & ~visible[:, None], -1e30, 0.0)
    return cosine, jnp.where(leads, -sine, 0.0), jnp.where(leads, 0.0, sine), hide


def image_device(
    block_input,
    conditioning,
    patch_counts,
    positions,
    w_mod,
    b_mod,
    w_qkv,
    b_qkv,
    w_out,
    b_out,
    w_up,
    b_up,
    w_down,
    b_down,
    cotangent,
):
    own_rows, model_width = block_input.shape
    slot_count = own_rows * CORES
    shard_rows, _, feat = w_qkv.shape
    units = w_up.shape[1]
    heads = CORES * feat // HEAD
    scale = 1.0 / math.sqrt(HEAD)
    images = ZS * YS * XS
    z, y, x, core = place()
    data = z * YS + y
    bf16 = jnp.bfloat16

    def swap(values):
        return lax.ppermute(values, "tensor", CORE_SWAP)

    def both(values):
        return jnp.concatenate([values, swap(values)], 0)

    def own_sum(terms):
        return terms[:own_rows] + swap(terms[own_rows:].astype(bf16)).astype(jnp.float32)

    silu_cond = jax.nn.silu(conditioning).astype(bf16)
    every = exchange(
        silu_cond.astype(jnp.float32).reshape(-1, LANES), "dp", 0, gather=True
    ).reshape(images, model_width)
    silu_rows = lax.dynamic_slice_in_dim(every, data * shard_rows, shard_rows, 1).astype(bf16)
    mod_matrix = w_mod.astype(bf16).reshape(shard_rows, 6 * feat)
    mod_part = jnp.dot(silu_rows, mod_matrix, preferred_element_type=jnp.float32)
    mod_part = mod_part + jnp.where(data == 0, b_mod.reshape(-1), 0.0)
    mod_part = jnp.broadcast_to(
        mod_part.reshape(images, 1, 8, -1), (images, CORES, 8, 6 * feat // 8)
    ).reshape(images * CORES, 8, -1)
    mod_parts = exchange(mod_part, "all", 1).reshape(ZS * YS, XS * CORES, 6, feat)
    mod = mod_parts.sum(0).transpose(1, 0, 2).reshape(6, model_width)
    shift_one, scale_one, gate_one, shift_two, scale_two, gate_two = (mod[i] for i in range(6))

    shards = [
        jnp.concatenate([w_qkv.reshape(shard_rows, 3 * feat), w_out.T], 1).astype(bf16),
        w_up.astype(bf16),
        w_down.T.astype(bf16),
    ]
    first = gather_weights(shards[:1], 2)[0].reshape(model_width, -1)
    biases = jnp.concatenate([b_qkv.reshape(-1), b_up])
    other_biases = lax.ppermute(biases, "tensor", X_SWAP)
    low_biases = jnp.where(x == 0, biases, other_biases)
    high_biases = jnp.where(x == 0, other_biases, biases)
    qkv_width = 3 * feat
    joined = first.shape[1] // XS

    own_slots = core * own_rows + jnp.arange(own_rows)
    other_slots = (1 - core) * own_rows + jnp.arange(own_rows)
    slots = jnp.concatenate([own_slots, other_slots])
    visible = slots < lax.dynamic_index_in_dim(patch_counts, x, 0, False)
    image_start = x * slot_count
    places = jnp.concatenate(
        [
            lax.dynamic_slice_in_dim(positions, image_start + core * own_rows, own_rows, 0),
            lax.dynamic_slice_in_dim(positions, image_start + (1 - core) * own_rows, own_rows, 0),
        ]
    )
    tables = turn_tables(places, visible)

    normal_one, inverse_one = row_norm(block_input)
    hidden_one = both((normal_one * (1.0 + scale_one) + shift_one).astype(bf16))
    projected = []
    for half, bias in enumerate((low_biases, high_biases)):
        matrix = first[:, half * joined : half * joined + 8 * LANES]
        row = jnp.pad(bias[:qkv_width], (0, 8 * LANES - qkv_width))
        projected.append(jnp.dot(hidden_one, matrix, preferred_element_type=jnp.float32) + row)
    attended, saved, wholes = attend(projected, tables, shards[1:], heads, scale, 3)
    up_full, down_full = (whole.reshape(model_width, -1) for whole in wholes)
    out_parts = [first[:, half * joined + qkv_width : (half + 1) * joined] for half in range(2)]
    branch_one = (
        own_sum(contract(attended[0], out_parts[0], 1, 1) + contract(attended[1], out_parts[1], 1, 1))
        + b_out
    )
    middle = block_input + gate_one * branch_one
    normal_two, inverse_two = row_norm(middle)
    hidden_two = both((normal_two * (1.0 + scale_two) + shift_two).astype(bf16))
    bias_up = jnp.concatenate([low_biases[qkv_width:], high_biases[qkv_width:]])
    up_pre = jnp.dot(hidden_two, up_full, preferred_element_type=jnp.float32) + bias_up
    activated = gelu_tanh(up_pre).astype(bf16)
    branch_two = own_sum(contract(activated, down_full, 1, 1)) + b_down
    block_output = middle + gate_two * branch_two

    def norm_back(grad_hidden, normal, inverse, factor):
        grad_normal = grad_hidden * (1.0 + factor)
        mean_plain = jnp.mean(grad_normal, 1, keepdims=True)
        mean_cross = jnp.mean(grad_normal * normal, 1, keepdims=True)
        return inverse[:, None] * (grad_normal - mean_plain - normal * mean_cross)

    def column_sum(values):
        return jnp.sum(values.astype(jnp.float32), 0)

    grad_gate_two = jnp.sum(cotangent * branch_two, 0)
    grad_rows_two = both((cotangent * gate_two).astype(bf16))
    grad_bdown = column_sum(grad_rows_two)
    grad_down = contract(grad_rows_two, activated, 0, 0).astype(bf16)
    grad_activated = jnp.dot(grad_rows_two, down_full, preferred_element_type=jnp.float32)
    grad_up = jax.vjp(gelu_tanh, up_pre)[1](grad_activated)[0].astype(bf16)
    grad_bup = column_sum(grad_up)
    grad_wup = contract(hidden_two, grad_up, 0, 0).astype(bf16)
    grad_hidden_two = own_sum(contract(grad_up, up_full, 1, 1))
    grad_shift_two = jnp.sum(grad_hidden_two, 0)
    grad_scale_two = jnp.sum(grad_hidden_two * normal_two, 0)
    grad_middle = cotangent + norm_back(grad_hidden_two, normal_two, inverse_two, scale_two)
    grad_gate_one = jnp.sum(grad_middle * branch_one, 0)
    grad_rows_one = both((grad_middle * gate_one).astype(bf16))
    grad_bout = column_sum(grad_rows_one)
    grad_attended = [
        jnp.dot(grad_rows_one, part, preferred_element_type=jnp.float32).astype(bf16)
        for part in out_parts
    ]
    grad_projected, (sum_down, sum_up) = attend_back(
        saved, grad_attended, tables, [grad_down, grad_wup], heads, scale, 6
    )
    first_parts, hidden_terms, bias_terms = [], 0.0, []
    for half in range(2):
        first_parts.append(contract(hidden_one, grad_projected[half], 0, 0).astype(bf16))
        first_parts.append(contract(grad_rows_one, attended[half], 0, 0).astype(bf16))
        matrix = first[:, half * joined : half * joined + qkv_width]
        hidden_terms = hidden_terms + contract(grad_projected[half], matrix, 1, 1)
        bias_terms.append(column_sum(grad_projected[half]))
    grad_first = jnp.concatenate(first_parts, 1)
    grad_hidden_one = own_sum(hidden_terms)
    grad_shift_one = jnp.sum(grad_hidden_one, 0)
    grad_scale_one = jnp.sum(grad_hidden_one * normal_one, 0)
    grad_input = grad_middle + norm_back(grad_hidden_one, normal_one, inverse_one, scale_one)

    sum_first = scatter_grads([grad_first], 7)[0]
    grad_wqkv = sum_first[:, :qkv_width].reshape(shard_rows, 3, feat)
    grad_wout = sum_first[:, qkv_width:].T
    grad_wdown = sum_down.T

    grad_mod = jnp.stack(
        [
            grad_shift_one,
            grad_scale_one,
            grad_gate_one,
            grad_shift_two,
            grad_scale_two,
            grad_gate_two,
        ]
    )
    grad_mod = (grad_mod + swap(grad_mod)).astype(bf16).astype(jnp.float32)
    grad_mod = grad_mod.reshape(6, XS, CORES, feat)
    grad_mod = lax.dynamic_index_in_dim(grad_mod, core, 2, False)
    small = 6 * feat + qkv_width + units + 2 * model_width
    lines = -(-small // LANES)
    sends = []
    for half in range(2):
        flat = jnp.concatenate(
            [
                grad_mod[:, half].reshape(-1),
                bias_terms[half],
                grad_bup[half * units : (half + 1) * units],
                grad_bout,
                grad_bdown,
            ]
        )
        sends.append(jnp.pad(flat, (0, lines * LANES - small)).reshape(1, lines, LANES))
    blocks = jnp.broadcast_to(jnp.stack(sends, 1), (ZS * YS, 2, lines, LANES))
    small_all = exchange(blocks.reshape(images, lines, LANES), "same_core", 4).reshape(images, -1)
    mod_all = small_all[:, : 6 * feat]
    summed = jnp.sum(small_all, 0)
    grad_bmod = summed[: 6 * feat].reshape(6, feat)
    offset = 6 * feat
    grad_bqkv = summed[offset : offset + qkv_width].reshape(3, feat)
    offset += qkv_width
    grad_bup = summed[offset : offset + units]
    offset += units
    grad_bout = summed[offset : offset + model_width]
    grad_bdown = summed[offset + model_width : offset + 2 * model_width]
    mod_all = mod_all.astype(bf16)
    grad_wmod = contract(silu_rows, mod_all, 0, 0).reshape(shard_rows, 6, feat)
    silu_part = contract(mod_all, mod_matrix, 1, 1).reshape(ZS * YS, 1, -1)
    silu_part = jnp.pad(silu_part, ((0, 0), (0, 0), (0, 8 * LANES - XS * shard_rows)))
    silu_part = jnp.broadcast_to(silu_part, (ZS * YS, XS * CORES, 8 * LANES))
    silu_all = exchange(silu_part.reshape(-1, 8, LANES), "all", 5)
    silu_all = silu_all.reshape(ZS * YS, XS * CORES, -1)[:, :, : XS * shard_rows].sum(1)
    grad_silu = silu_all.reshape(ZS * YS, XS, shard_rows).transpose(1, 0, 2).reshape(XS, model_width)
    grad_cond = jax.vjp(jax.nn.silu, conditioning)[1](grad_silu)[0]
    return (
        block_output,
        grad_input,
        grad_cond,
        grad_wmod,
        grad_bmod,
        grad_wqkv,
        grad_bqkv,
        grad_wout,
        grad_bout,
        sum_up,
        grad_bup,
        grad_wdown,
        grad_bdown,
    )


def solution(mesh):
    body = image_device if image_per_chip(mesh) else per_device
    placed = (
        P(("dp", "tensor"), None),
        P("dp", None),
        P("dp"),
        P("dp", None),
        P("dp", None, "tensor"),
        P(None, "tensor"),
        P("dp", None, "tensor"),
        P(None, "tensor"),
        P("tensor", "dp"),
        P(),
        P("dp", "tensor"),
        P("tensor"),
        P("tensor", "dp"),
        P(),
        P(("dp", "tensor"), None),
    )
    return jax.shard_map(
        body,
        mesh=mesh,
        in_specs=placed,
        out_specs=(
            P(("dp", "tensor"), None),
            P(("dp", "tensor"), None),
            P("dp", None),
            P("dp", None, "tensor"),
            P(None, "tensor"),
            P("dp", None, "tensor"),
            P(None, "tensor"),
            P("tensor", "dp"),
            P(),
            P("dp", "tensor"),
            P("tensor"),
            P("tensor", "dp"),
            P(),
        ),
        check_vma=False,
    )
```

```python
from functools import partial
import math

import jax
import jax.numpy as jnp
from jax import lax
from jax.experimental import pallas as pl
from jax.experimental.pallas import tpu as pltpu
from jax.sharding import PartitionSpec as P

HEAD = 72


epsilon = 1e-06
rope_base = 10000.0
gelu_coeff = 0.044715
root_two_pi = math.sqrt(2.0 / math.pi)


def gelu_tanh(values):
    return (
        0.5
        * values
        * (1.0 + jnp.tanh(root_two_pi * (values + gelu_coeff * values * values * values)))
    )


def rotate(values, positions, direction):
    quarter = values.shape[-1] // 4
    frequency = rope_base ** (-jnp.arange(quarter, dtype=jnp.float32) / quarter)
    pieces = []
    for column in range(2):
        angles = positions[:, column].astype(jnp.float32)[:, None, None] * frequency
        cosine = jnp.cos(angles)
        sine_term = direction * jnp.sin(angles)
        leading = values[..., 2 * column * quarter : (2 * column + 1) * quarter]
        trailing = values[..., (2 * column + 1) * quarter : (2 * column + 2) * quarter]
        pieces.append(leading * cosine - trailing * sine_term)
        pieces.append(leading * sine_term + trailing * cosine)
    return jnp.concatenate(pieces, -1)


def contract(left, right, left_dim, right_dim):
    return lax.dot_general(
        left, right, (((left_dim,), (right_dim,)), ((), ())), preferred_element_type=jnp.float32
    )


def exact_dot(left, right):
    return jnp.dot(left, right, precision=lax.Precision.HIGHEST, preferred_element_type=jnp.float32)


def row_norm(rows):
    average = jnp.mean(rows, 1)
    inverse = lax.rsqrt(jnp.mean(rows * rows, 1) - average * average + epsilon)
    return ((rows - average[:, None]) * inverse[:, None], inverse)


def masked_scores(query_rows, key_rows, patch_count, factor):
    raw_scores = (
        jnp.einsum("qhd,khd->hqk", query_rows, key_rows, preferred_element_type=jnp.float32)
        * factor
    )
    visible = jnp.arange(key_rows.shape[0]) < patch_count
    return jnp.where(visible[None, None, :], raw_scores, -1e30)


def attend_forward(factor, inputs):
    query_rows, key_rows, value_rows, patch_count = inputs
    scores = masked_scores(query_rows, key_rows, patch_count, factor)
    highest = jnp.max(scores, -1, keepdims=True)
    exponent = jnp.exp(scores - highest)
    denominator = jnp.sum(exponent, -1, keepdims=True)
    softmax_rows = (exponent / denominator).astype(jnp.bfloat16)
    attended = jnp.einsum(
        "hqk,khd->qhd", softmax_rows, value_rows, preferred_element_type=jnp.float32
    )
    return (attended, (highest + jnp.log(denominator))[..., 0])


def attend_backward(factor, inputs):
    query_rows, key_rows, value_rows, patch_count, logsum, grad_rows = inputs
    scores = masked_scores(query_rows, key_rows, patch_count, factor)
    softmax_rows = jnp.exp(scores - logsum[..., None])
    grad_soft = jnp.einsum(
        "qhd,khd->hqk", grad_rows, value_rows, preferred_element_type=jnp.float32
    )
    grad_values = jnp.einsum(
        "hqk,qhd->khd",
        softmax_rows.astype(jnp.bfloat16),
        grad_rows,
        preferred_element_type=jnp.float32,
    )
    inner_sum = jnp.sum(softmax_rows * grad_soft, -1, keepdims=True)
    grad_scores = (softmax_rows * (grad_soft - inner_sum) * factor).astype(jnp.bfloat16)
    grad_query = jnp.einsum(
        "hqk,khd->qhd", grad_scores, key_rows, preferred_element_type=jnp.float32
    )
    grad_keys = jnp.einsum(
        "hqk,qhd->khd", grad_scores, query_rows, preferred_element_type=jnp.float32
    )
    return (grad_query, grad_keys, grad_values)


def per_device(
    block_input,
    conditioning,
    patch_counts,
    positions,
    w_mod,
    b_mod,
    w_qkv,
    b_qkv,
    w_out,
    b_out,
    w_up,
    b_up,
    w_down,
    b_down,
    cotangent,
):
    own_rows, model_width = block_input.shape
    group_rows = positions.shape[0]
    images_local = conditioning.shape[0]
    slot_count = group_rows // images_local
    feat_local = w_qkv.shape[2]
    heads_local = feat_local // HEAD
    row_start = lax.axis_index("tensor") * own_rows
    factor = 1.0 / math.sqrt(HEAD)
    image_of = (row_start + jnp.arange(own_rows)) // slot_count
    one_hot = (image_of[:, None] == jnp.arange(images_local)[None, :]).astype(jnp.float32)

    def to_rows(vectors):
        return exact_dot(one_hot, vectors)

    def to_images(values):
        return exact_dot(one_hot.T, values)

    def per_image(stacked):
        return stacked.reshape((images_local, slot_count) + stacked.shape[1:])

    def modulate_group(values, shift, scale):
        shaped = values.reshape(images_local, slot_count, values.shape[1])
        return (shaped * (1.0 + scale[:, None, :]) + shift[:, None, :]).reshape(values.shape)

    mod_full, qkv_full, out_full, up_full, down_full = (
        lax.all_gather(w_mod.astype(jnp.bfloat16), "dp", axis=0, tiled=True),
        lax.all_gather(w_qkv.astype(jnp.bfloat16), "dp", axis=0, tiled=True),
        lax.all_gather(w_out.astype(jnp.bfloat16), "dp", axis=1, tiled=True),
        lax.all_gather(w_up.astype(jnp.bfloat16), "dp", axis=0, tiled=True),
        lax.all_gather(w_down.astype(jnp.bfloat16), "dp", axis=1, tiled=True),
    )
    silu_cond = jax.nn.silu(conditioning).astype(jnp.bfloat16)
    mod_cols = jnp.dot(
        silu_cond, mod_full.reshape(model_width, 6 * feat_local), preferred_element_type=jnp.float32
    )
    mod_cols = mod_cols.reshape(images_local, 6, feat_local) + b_mod
    mod_all = lax.all_gather(mod_cols, "tensor", axis=2, tiled=True)

    def norm_gather(rows_local, shift, scale):
        rows_group = lax.all_gather(rows_local, "tensor", axis=0, tiled=True)
        normal_group, inverse_group = row_norm(rows_group)
        hidden = modulate_group(normal_group, shift, scale).astype(jnp.bfloat16)
        normal = lax.dynamic_slice_in_dim(normal_group, row_start, own_rows, 0)
        inverse = lax.dynamic_slice_in_dim(inverse_group, row_start, own_rows, 0)
        return (hidden, normal, inverse)

    hidden_one, normal_one, inverse_one = norm_gather(block_input, mod_all[:, 0], mod_all[:, 1])
    projected = jnp.dot(
        hidden_one,
        qkv_full.reshape(model_width, 3 * feat_local),
        preferred_element_type=jnp.float32,
    ) + b_qkv.reshape(-1)
    projected = projected.reshape(group_rows, 3, heads_local, HEAD)
    query_rows = rotate(projected[:, 0], positions, 1.0).astype(jnp.bfloat16)
    key_rows = rotate(projected[:, 1], positions, 1.0).astype(jnp.bfloat16)
    value_rows = projected[:, 2].astype(jnp.bfloat16)
    attended, logsum = lax.map(
        partial(attend_forward, factor),
        (per_image(query_rows), per_image(key_rows), per_image(value_rows), patch_counts),
    )
    attended = attended.reshape(group_rows, feat_local).astype(jnp.bfloat16)

    def branch_sum(partial_terms, offset):
        return lax.psum_scatter(partial_terms, "tensor", scatter_dimension=0, tiled=True) + offset

    gate_one_rows = to_rows(mod_all[:, 2])
    gate_two_rows = to_rows(mod_all[:, 5])
    branch_one = branch_sum(jnp.dot(attended, out_full, preferred_element_type=jnp.float32), b_out)
    middle = block_input + gate_one_rows * branch_one
    hidden_two, normal_two, inverse_two = norm_gather(middle, mod_all[:, 3], mod_all[:, 4])
    up_pre = jnp.dot(hidden_two, up_full, preferred_element_type=jnp.float32) + b_up
    activated = gelu_tanh(up_pre).astype(jnp.bfloat16)
    branch_two = branch_sum(
        jnp.dot(activated, down_full, preferred_element_type=jnp.float32), b_down
    )
    block_output = middle + gate_two_rows * branch_two
    mod_back, qkv_back, out_back, up_back, down_back = (
        lax.all_gather(w_mod.astype(jnp.bfloat16), "dp", axis=0, tiled=True),
        lax.all_gather(w_qkv.astype(jnp.bfloat16), "dp", axis=0, tiled=True),
        lax.all_gather(w_out.astype(jnp.bfloat16), "dp", axis=1, tiled=True),
        lax.all_gather(w_up.astype(jnp.bfloat16), "dp", axis=0, tiled=True),
        lax.all_gather(w_down.astype(jnp.bfloat16), "dp", axis=1, tiled=True),
    )

    def spread_grad(grad_branch):
        return lax.all_gather(grad_branch, "tensor", axis=0, tiled=True)

    def input_sum(partial_terms):
        return lax.psum_scatter(partial_terms, "tensor", scatter_dimension=0, tiled=True)

    def norm_backward(grad_hidden, normal, inverse, scale):
        grad_normal = grad_hidden * (1.0 + to_rows(scale))
        mean_plain = jnp.mean(grad_normal, 1, keepdims=True)
        mean_cross = jnp.mean(grad_normal * normal, 1, keepdims=True)
        return inverse[:, None] * (grad_normal - mean_plain - normal * mean_cross)

    grad_gate_two = to_images(cotangent * branch_two)
    grad_branch_two = (cotangent * gate_two_rows).astype(jnp.bfloat16)
    grad_rows_two = spread_grad(grad_branch_two)
    grad_bdown_local = jnp.sum(grad_rows_two.astype(jnp.float32), 0)
    grad_wdown_local = contract(activated, grad_rows_two, 0, 0)
    grad_activated = contract(grad_rows_two, down_back, 1, 1)
    gelu_pull = jax.vjp(gelu_tanh, up_pre)[1]
    grad_up = gelu_pull(grad_activated)[0].astype(jnp.bfloat16)
    grad_bup_local = jnp.sum(grad_up.astype(jnp.float32), 0)
    grad_wup_local = contract(hidden_two, grad_up, 0, 0)
    grad_hidden_two = input_sum(contract(grad_up, up_back, 1, 1))
    grad_shift_two = to_images(grad_hidden_two)
    grad_scale_two = to_images(grad_hidden_two * normal_two)
    grad_middle = cotangent + norm_backward(grad_hidden_two, normal_two, inverse_two, mod_all[:, 4])
    grad_gate_one = to_images(grad_middle * branch_one)
    grad_branch_one = (grad_middle * gate_one_rows).astype(jnp.bfloat16)
    grad_rows_one = spread_grad(grad_branch_one)
    grad_bout_local = jnp.sum(grad_rows_one.astype(jnp.float32), 0)
    grad_wout_local = contract(attended, grad_rows_one, 0, 0)
    grad_attended = contract(grad_rows_one, out_back, 1, 1).astype(jnp.bfloat16)
    grad_attended = grad_attended.reshape(group_rows, heads_local, HEAD)
    grad_query, grad_keys, grad_values = lax.map(
        partial(attend_backward, factor),
        (
            per_image(query_rows),
            per_image(key_rows),
            per_image(value_rows),
            patch_counts,
            logsum,
            per_image(grad_attended),
        ),
    )
    head_shape = (group_rows, heads_local, HEAD)
    grad_projected = jnp.stack(
        [
            rotate(grad_query.reshape(head_shape), positions, -1.0),
            rotate(grad_keys.reshape(head_shape), positions, -1.0),
            grad_values.reshape(head_shape),
        ],
        1,
    )
    grad_projected = grad_projected.astype(jnp.bfloat16).reshape(group_rows, 3 * feat_local)
    grad_bqkv_local = jnp.sum(grad_projected.astype(jnp.float32), 0).reshape(3, feat_local)
    grad_wqkv_local = contract(hidden_one, grad_projected, 0, 0).reshape(model_width, 3, feat_local)
    grad_hidden_one = input_sum(
        contract(grad_projected, qkv_back.reshape(model_width, 3 * feat_local), 1, 1)
    )
    grad_shift_one = to_images(grad_hidden_one)
    grad_scale_one = to_images(grad_hidden_one * normal_one)
    grad_input = grad_middle + norm_backward(
        grad_hidden_one, normal_one, inverse_one, mod_all[:, 1]
    )
    grad_mod_part = jnp.stack(
        [
            grad_shift_one,
            grad_scale_one,
            grad_gate_one,
            grad_shift_two,
            grad_scale_two,
            grad_gate_two,
        ],
        1,
    )
    grad_mod = lax.psum_scatter(grad_mod_part, "tensor", scatter_dimension=2, tiled=True).astype(
        jnp.bfloat16
    )
    grad_bmod_local = jnp.sum(grad_mod.astype(jnp.float32), 0)
    grad_mod_flat = grad_mod.reshape(images_local, 6 * feat_local)
    grad_wmod_local = contract(silu_cond, grad_mod_flat, 0, 0).reshape(model_width, 6, feat_local)
    grad_silu = lax.psum(
        contract(grad_mod_flat, mod_back.reshape(model_width, 6 * feat_local), 1, 1), "tensor"
    )
    silu_pull = jax.vjp(jax.nn.silu, conditioning)[1]
    grad_cond = silu_pull(grad_silu)[0]
    grad_wmod, grad_wqkv, grad_wout, grad_wup, grad_wdown = (
        lax.psum_scatter(
            grad_wmod_local.astype(jnp.bfloat16), "dp", scatter_dimension=0, tiled=True
        ).astype(jnp.float32),
        lax.psum_scatter(
            grad_wqkv_local.astype(jnp.bfloat16), "dp", scatter_dimension=0, tiled=True
        ).astype(jnp.float32),
        lax.psum_scatter(
            grad_wout_local.astype(jnp.bfloat16), "dp", scatter_dimension=1, tiled=True
        ).astype(jnp.float32),
        lax.psum_scatter(
            grad_wup_local.astype(jnp.bfloat16), "dp", scatter_dimension=0, tiled=True
        ).astype(jnp.float32),
        lax.psum_scatter(
            grad_wdown_local.astype(jnp.bfloat16), "dp", scatter_dimension=1, tiled=True
        ).astype(jnp.float32),
    )
    grad_bmod, grad_bqkv, grad_bout, grad_bup, grad_bdown = lax.psum(
        (grad_bmod_local, grad_bqkv_local, grad_bout_local, grad_bup_local, grad_bdown_local), "dp"
    )
    return (
        block_output,
        grad_input,
        grad_cond,
        grad_wmod,
        grad_bmod,
        grad_wqkv,
        grad_bqkv,
        grad_wout,
        grad_bout,
        grad_wup,
        grad_bup,
        grad_wdown,
        grad_bdown,
    )


LANES = 128
ZS, YS, XS, CORES = 4, 2, 2, 2
MESH_ID = pl.DeviceIdType.MESH
CORE_SWAP = [(0, 1), (1, 0), (2, 3), (3, 2)]
X_SWAP = [(0, 2), (2, 0), (1, 3), (3, 1)]
Y_SWAP = [(i, i ^ 1) for i in range(ZS * YS)]
LOG2E = 1.0 / math.log(2.0)
HBM = pl.BlockSpec(memory_space=pl.ANY)
VMEM = pl.BlockSpec(memory_space=pltpu.VMEM)


def image_per_chip(mesh):
    return dict(mesh.shape) == {"dp": ZS * YS, "tensor": XS * CORES}


def place():
    data, tensor = lax.axis_index("dp"), lax.axis_index("tensor")
    return data // YS, data % YS, tensor // CORES, tensor % CORES


def flip_z(z, step):
    high, low = z // 2, z % 2
    if step & 2:
        high = 1 - high
    if step & 1:
        low = 1 - low
    return high * 2 + low


def device(z, y, x, core):
    return (z * YS + y, x * CORES + core)


def greet(targets):
    barrier = pltpu.get_barrier_semaphore()
    for target in targets:
        pl.semaphore_signal(barrier, inc=1, device_id=target, device_id_type=MESH_ID)
    pl.semaphore_wait(barrier, len(targets))


GATHER_STEPS, SCATTER_STEPS = 5, 5
GATHER_SPACING, SCATTER_SPACING = 8.0, 8.0
GATHER_WEIGHTS, SCATTER_WEIGHTS = (1, 1, 1, 1, 1), (1, 1, 1, 1, 1)


def grouped(matrices, rows, units):
    chunks = []
    for matrix in range(matrices):
        unit = units[matrix]
        for number, row in enumerate(range(0, rows, 3 * unit)):
            short = (matrix + number) % 2
            chunks.append((matrix, row, unit, 2))
            chunks.append((matrix, row + unit, unit, 3))
            chunks.append((matrix, row + 2 * unit, unit, short))
    return chunks


def in_order(count, steps, spacing, act):
    events = sorted((c + s * spacing, c, s) for c in range(count) for s in range(steps))
    return [(s, partial(act, c, s)) for time, c, s in events]


def run_all(events):
    for _, event in events:
        event()


def table_of(events, weights, trips):
    total = sum(weights[step] for step, _ in events)
    table, sent = [[] for _ in range(trips)], 0
    for step, event in events:
        table[min(sent * trips // total, trips - 1)].append(event)
        sent += weights[step]
    return table


def dispatch(table, index, low, high):
    if not any(table[low:high]):
        return
    if high - low == 1:
        for event in table[low]:
            event()
        return
    middle = (low + high) // 2
    pl.when(index < middle)(lambda: dispatch(table, index, low, middle))
    pl.when(index >= middle)(lambda: dispatch(table, index, middle, high))


def gather_plan(chunks, spacing, shards, wholes, sends, recvs, local):
    z, y, x, core = place()
    inner = jnp.logical_or(z == 1, z == 2)
    every = slice(None)

    def mine_of(matrix):
        width = shards[matrix].shape[1]
        return pl.ds(pl.multiple_of(x * width, LANES), width)

    at_x, at_y = device(z, y, 1 - x, core), device(z, 1 - y, x, core)
    beside, mirror = device(flip_z(z, 1), y, x, core), device(3 - z, y, x, core)
    pair = pl.ds(z // 2 * 2, 2)
    far = pl.ds(2 - z // 2 * 2, 2)

    def copy(number, send, recv, source, target, where):
        return pltpu.make_async_remote_copy(
            src_ref=source,
            dst_ref=target,
            send_sem=sends.at[number * 5 + send],
            recv_sem=recvs.at[number * 4 + recv],
            device_id=where,
            device_id_type=MESH_ID,
        )

    def moves(number):
        matrix, row, rows, route = chunks[number]
        whole, span, mine = wholes[matrix], pl.ds(row, rows), mine_of(matrix)
        own, shard = whole.at[z, y, span, mine], shards[matrix].at[span, :]
        lines, columns = (every if route == 3 else y), (every if route == 2 else mine)
        made = {}
        near = shard if route < 2 else whole.at[z, lines, span, columns]
        near_to = own if route < 2 else near
        made["near"] = partial(copy, number, 0, 0, near, near_to, beside)
        both = whole.at[pair, lines, span, columns]
        made["mirror"] = partial(copy, number, 1, 1, both, both, mirror)
        there = whole.at[far, lines, span, columns]
        made["forward"] = partial(copy, number, 2, 1, there, there, beside)
        if route < 2:
            column = whole.at[:, y, span, mine]
            made["second"] = partial(copy, number, 3, 2, column, column, at_x if route == 0 else at_y)
        else:
            made["first"] = partial(copy, number, 3, 2, shard, own, at_x if route == 2 else at_y)
        if route in (0, 2):
            last = whole.at[:, y, span, :]
        else:
            last = whole.at[:, :, span, mine]
        made["third"] = partial(copy, number, 4, 3, last, last, at_y if route in (0, 2) else at_x)
        return made

    def keep(matrix):
        return pltpu.make_async_copy(
            shards[matrix], wholes[matrix].at[z, y, :, mine_of(matrix)], local.at[matrix]
        )

    kept = []

    def ready(number):
        matrix = chunks[number][0]
        if matrix not in kept:
            kept.append(matrix)
            keep(matrix).wait()

    def act(number, step):
        made = moves(number)
        straight = chunks[number][3] < 2
        if step == 0:
            made["near" if straight else "first"]().start()
        elif step == 1:
            ready(number)
            if straight:
                made["near"]().wait_recv()
                pl.when(inner)(lambda: made["mirror"]().start())
            else:
                made["first"]().wait_recv()
                made["near"]().start()
        elif step == 2:
            if straight:
                made["mirror"]().wait_recv()
                pl.when(inner)(lambda: made["forward"]().start())
                made["second"]().start()
            else:
                made["near"]().wait_recv()
                pl.when(inner)(lambda: made["mirror"]().start())
        elif step == 3:
            if straight:
                made["second"]().wait_recv()
            else:
                made["mirror"]().wait_recv()
                pl.when(inner)(lambda: made["forward"]().start())
            made["third"]().start()
        else:
            made["third"]().wait_recv()

    def start():
        for matrix in sorted({chunk[0] for chunk in chunks}):
            keep(matrix).start()

    def finish():
        for number in range(len(chunks)):
            made = moves(number)
            for name in made:
                if name not in ("mirror", "forward"):
                    made[name]().wait_send()

            def rest(made=made):
                made["mirror"]().wait_send()
                made["forward"]().wait_send()

            pl.when(inner)(rest)

    return start, in_order(len(chunks), GATHER_STEPS, spacing, act), finish


def gather_scratch(chunks, matrices):
    count = len(chunks)
    return [
        pltpu.SemaphoreType.DMA((count * 5,)),
        pltpu.SemaphoreType.DMA((count * 4,)),
        pltpu.SemaphoreType.DMA((matrices,)),
    ]


def send_off(part, flip, after):
    z, y, x, core = place()
    rows, width = part.shape[0] // (ZS * YS), part.shape[1] // XS
    blocks = part.reshape(ZS, YS, rows, XS * width)
    split = rows // 32 * 16
    split = split if flip else rows - split
    by_y, by_x = blocks[:, :, :split], blocks[:, :, split:]
    low, high = by_x[..., :width], by_x[..., width:]
    send_y = lax.dynamic_index_in_dim(by_y, 1 - y, 1, False)
    keep_y = lax.dynamic_index_in_dim(by_y, y, 1, False)
    send_x, keep_x = jnp.where(x == 0, high, low), jnp.where(x == 0, low, high)
    send_y, send_x, after = lax.optimization_barrier((send_y, send_x, after))
    got_y = lax.ppermute(send_y, "dp", Y_SWAP)
    got_x = lax.ppermute(send_x, "tensor", X_SWAP)
    return (keep_y, got_y, keep_x, got_x), after


def arrive_before(sent, after):
    keep_y, got_y, keep_x, got_x = sent
    got_y, got_x, after = lax.optimization_barrier((got_y, got_x, after))
    return (keep_y, got_y, keep_x, got_x), after


def settle(sent):
    z, y, x, core = place()
    keep_y, got_y, keep_x, got_x = sent
    sum_y = (keep_y.astype(jnp.float32) + got_y.astype(jnp.float32)).astype(jnp.bfloat16)
    sum_x = (keep_x.astype(jnp.float32) + got_x.astype(jnp.float32)).astype(jnp.bfloat16)
    width = sum_x.shape[-1]
    low, high = sum_y[..., :width], sum_y[..., width:]
    return [
        jnp.where(x == 0, low, high),
        jnp.where(x == 0, high, low),
        lax.dynamic_index_in_dim(sum_x, y, 1, False),
        lax.dynamic_index_in_dim(sum_x, 1 - y, 1, False),
    ]


def scatter_chunks(pieces, units):
    chunks = []
    for matrix, unit in enumerate(units):
        parts, start = [], 0
        for side in range(2):
            rows = pieces[matrix][2 * side].shape[1]
            parts.append(
                [(matrix, side, row, start + row, min(unit, rows - row)) for row in range(0, rows, unit)]
            )
            start += rows
        for i in range(max(len(part) for part in parts)):
            chunks.extend(part[i] for part in parts if i < len(part))
    return chunks


def scatter_plan(chunks, spacing, pieces, sums, buffers, sends, recvs):
    z, y, x, core = place()
    inner = jnp.logical_or(z == 1, z == 2)
    outer = jnp.logical_or(z == 0, z == 3)
    at_x, at_y = device(z, y, 1 - x, core), device(z, 1 - y, x, core)
    z_near = flip_z(z, 1)
    beside, mirror = device(z_near, y, x, core), device(3 - z, y, x, core)
    pair_at, far_at = z // 2 * 2, 2 - z // 2 * 2
    far = pl.ds(far_at, 2)

    def copy(number, index, source, target, where):
        return pltpu.make_async_remote_copy(
            src_ref=source,
            dst_ref=target,
            send_sem=sends.at[number * 4 + index],
            recv_sem=recvs.at[number * 4 + index],
            device_id=where,
            device_id_type=MESH_ID,
        )

    def moves(number):
        matrix, side, row, at, rows = chunks[number]
        here, span = pl.ds(row, rows), pl.ds(at, rows)
        arrived, outer_in, mirror_in, near_in = buffers[4 * matrix : 4 * matrix + 4]
        give, two = pieces[4 * matrix + 2 * side + 1], arrived.at[far, span, :]
        return {
            "first": partial(
                copy,
                number,
                0,
                give.at[:, here, :],
                arrived.at[:, span, :],
                at_y if side else at_x,
            ),
            "outer": partial(copy, number, 1, two, outer_in.at[:, span, :], beside),
            "mirror": partial(copy, number, 2, two, mirror_in.at[:, span, :], mirror),
            "near": partial(
                copy, number, 3, arrived.at[z_near, span, :], near_in.at[span, :], beside
            ),
        }

    def add(number, count, base, source, from_row):
        matrix, side, row, at, rows = chunks[number]
        arrived, tiles = buffers[4 * matrix], rows // 16

        def one(i, carry):
            block, line = i // tiles, i % tiles
            to = pl.ds(pl.multiple_of(at + line * 16, 16), 16)
            origin = pl.ds(pl.multiple_of(from_row + line * 16, 16), 16)
            held = arrived[base + block, to, :].astype(jnp.float32)
            arrived[base + block, to, :] = (
                held + source[block, origin, :].astype(jnp.float32)
            ).astype(jnp.bfloat16)
            return carry

        lax.fori_loop(0, count * tiles, one, 0)

    def finalize(number):
        matrix, side, row, at, rows = chunks[number]
        arrived, near_in = buffers[4 * matrix], buffers[4 * matrix + 3]

        def one(i, carry):
            to = pl.ds(pl.multiple_of(at + i * 16, 16), 16)
            sums[matrix][to, :] = arrived[z, to, :].astype(jnp.float32) + near_in[to, :].astype(
                jnp.float32
            )
            return carry

        lax.fori_loop(0, rows // 16, one, 0)

    def act(number, step):
        matrix, side, row, at, rows = chunks[number]
        made = moves(number)
        stay = pieces[4 * matrix + 2 * side]
        arrived, outer_in, mirror_in, near_in = buffers[4 * matrix : 4 * matrix + 4]

        def from_outer():
            made["outer"]().wait_recv()
            add(number, 2, far_at, outer_in, at)
            made["mirror"]().start()

        def from_mirror():
            made["mirror"]().wait_recv()
            add(number, 2, pair_at, mirror_in, at)

        if step == 0:
            made["first"]().start()
        elif step == 1:
            made["first"]().wait_recv()
            add(number, ZS, 0, stay, row)
            pl.when(outer)(lambda: made["outer"]().start())
        elif step == 2:
            pl.when(inner)(from_outer)
        elif step == 3:
            pl.when(inner)(from_mirror)
            made["near"]().start()
        else:
            made["near"]().wait_recv()
            finalize(number)

    def finish():
        for number in range(len(chunks)):
            made = moves(number)
            made["first"]().wait_send()
            made["near"]().wait_send()
            pl.when(outer)(lambda made=made: made["outer"]().wait_send())
            pl.when(inner)(lambda made=made: made["mirror"]().wait_send())

    return in_order(len(chunks), SCATTER_STEPS, spacing, act), finish


def scatter_scratch(chunks, shapes):
    wide = []
    for rows, width in shapes:
        for lead in ((ZS,), (2,), (2,), ()):
            wide.append(pltpu.VMEM((*lead, rows, width), jnp.bfloat16))
    count = len(chunks) * 4
    return wide + [pltpu.SemaphoreType.DMA((count,)), pltpu.SemaphoreType.DMA((count,))]


def sum_shape(piece):
    rows = piece[0].shape[1] + piece[2].shape[1]
    return rows, piece[0].shape[2]


def line_peers():
    z, y, x, core = place()
    return [
        device(z, y, 1 - x, core),
        device(z, 1 - y, x, core),
        device(flip_z(z, 1), y, x, core),
        device(3 - z, y, x, core),
    ]


DEVICES = ZS * YS * XS * CORES


def numbers():
    z, y, x, core = place()
    data = z * YS + y
    return (data * XS + x) * CORES + core, data, data * XS + x


def device_at(number):
    return (number // (XS * CORES), number % (XS * CORES))


def greet_all():
    me = numbers()[0]
    greet([device_at((me + step) % DEVICES) for step in range(1, DEVICES)])


def send_each(count, me, source_of, arrived, device_of, sends, recvs):
    copies = []
    for step in range(1, count):
        target = (me + step) % count
        copy = pltpu.make_async_remote_copy(
            src_ref=source_of(target),
            dst_ref=arrived.at[me],
            send_sem=sends.at[step - 1],
            recv_sem=recvs.at[step - 1],
            device_id=device_of(target),
            device_id_type=MESH_ID,
        )
        copy.start()
        copies.append(copy)
    return copies


def receive(copies):
    for copy in copies:
        copy.wait_recv()


def semaphores_of(*counts):
    return [pltpu.SemaphoreType.DMA((count,)) for count in counts for _ in range(2)]


def gather_kernel(chunks, *refs):
    shard, silu_blocks, matrix_ref, bias_ref = refs[:4]
    whole, silu_in, mod_ref = refs[4:7]
    parts, mod_in, silu_sends, silu_recvs, mod_sends, mod_recvs = refs[7:13]
    me, data, _ = numbers()
    z, y, x, core = place()
    greet_all()
    silu_copies = send_each(
        ZS * YS,
        data,
        lambda target: silu_blocks.at[target],
        silu_in,
        lambda target: (target, lax.axis_index("tensor")),
        silu_sends,
        silu_recvs,
    )
    start, events, finish = gather_plan(chunks, GATHER_SPACING, [shard], [whole], *refs[13:])
    start()
    early = len(chunks) // 2
    run_all(events[:early])
    silu_in[data] = silu_blocks[data]
    receive(silu_copies)
    rows = silu_in[...].reshape(silu_in.shape[0] * silu_in.shape[1], silu_in.shape[2])
    product = jnp.dot(
        rows.astype(jnp.bfloat16), matrix_ref[...], preferred_element_type=jnp.float32
    )
    product = product + bias_ref[...]
    lines = product.shape[1] // LANES
    for line in range(lines):
        piece = product[:, line * LANES : (line + 1) * LANES]
        parts[:, :, line, :] = piece.reshape(parts.shape[0], parts.shape[1], LANES)
    for line in range(lines, parts.shape[2]):
        parts[:, :, line, :] = jnp.zeros((parts.shape[0], parts.shape[1], LANES), jnp.float32)
    run_all(events[early : 2 * early])
    mod_copies = send_each(
        DEVICES,
        me,
        lambda target: parts.at[target // (XS * CORES), target % (XS * CORES) // CORES],
        mod_in,
        device_at,
        mod_sends,
        mod_recvs,
    )
    mod_in[me] = parts[data, x]
    run_all(events[2 * early :])
    receive(mod_copies)
    for column in range(XS * CORES):
        total = mod_in[column]
        for row in range(1, ZS * YS):
            total = total + mod_in[row * XS * CORES + column]
        mod_ref[column] = total
    for copy in silu_copies + mod_copies:
        copy.wait_send()
    finish()


def whole_shape(shard):
    rows, width = shard.shape
    return jax.ShapeDtypeStruct((ZS, YS, rows, XS * width), jnp.bfloat16)


def gather_first(shard, silu_blocks, matrix, bias, ident):
    chunks = grouped(1, shard.shape[0], [16])
    groups, rows, _ = silu_blocks.shape
    lines = -(-matrix.shape[1] // (8 * LANES)) * 8
    return pl.pallas_call(
        partial(gather_kernel, chunks),
        out_shape=[
            whole_shape(shard),
            jax.ShapeDtypeStruct(silu_blocks.shape, jnp.float32),
            jax.ShapeDtypeStruct((XS * CORES, lines, LANES), jnp.float32),
        ],
        in_specs=[VMEM] * 4,
        out_specs=[HBM, VMEM, VMEM],
        scratch_shapes=[
            pltpu.VMEM((groups, rows, lines, LANES), jnp.float32),
            pltpu.VMEM((DEVICES, lines, LANES), jnp.float32),
        ]
        + semaphores_of(groups - 1, DEVICES - 1)
        + gather_scratch(chunks, 1),
        compiler_params=pltpu.CompilerParams(collective_id=ident, has_side_effects=True),
        name="gather_first",
    )(shard, silu_blocks, matrix, bias)


def scatter_kernel(chunks, matrices, lines, *refs):
    pieces, (small_ref, matrix_ref) = refs[: 4 * matrices], refs[4 * matrices : 4 * matrices + 2]
    refs = refs[4 * matrices + 2 :]
    sums, (small_in, cond_ref), refs = refs[:matrices], refs[matrices : matrices + 2], refs[matrices + 2 :]
    silu_parts, cond_in, small_sends, small_recvs, cond_sends, cond_recvs = refs[:6]
    buffers, semaphores = refs[6 : 6 + 4 * matrices], refs[6 + 4 * matrices :]
    me, data, chip = numbers()
    z, y, x, core = place()
    chips = ZS * YS * XS
    greet_all()
    small_copies = send_each(
        chips,
        chip,
        lambda target: small_ref.at[target % XS],
        small_in,
        lambda target: (target // XS, target % XS * CORES + core),
        small_sends,
        small_recvs,
    )
    events, finish = scatter_plan(chunks, SCATTER_SPACING, pieces, sums, buffers, *semaphores)
    run_all(events[: len(chunks)])
    small_in[chip] = small_ref[x]
    silu_parts[...] = jnp.zeros_like(silu_parts)
    receive(small_copies)
    total = jnp.zeros((chips, matrix_ref.shape[0]), jnp.float32)
    for line in range(lines):
        total = total + contract(
            small_in[:, line, :].astype(jnp.bfloat16),
            matrix_ref[:, line * LANES : (line + 1) * LANES],
            1,
            1,
        )
    for image in range(chips):
        at = image % XS
        silu_parts[image // XS, at : at + 1, :] = total[image : image + 1, :]
    middle = 2 * len(chunks)
    run_all(events[len(chunks) : middle])
    cond_copies = send_each(
        DEVICES,
        me,
        lambda target: silu_parts.at[target // (XS * CORES)],
        cond_in,
        device_at,
        cond_sends,
        cond_recvs,
    )
    cond_in[me] = silu_parts[data]
    run_all(events[middle:])
    receive(cond_copies)
    for row in range(ZS * YS):
        total = cond_in[row * XS * CORES]
        for column in range(1, XS * CORES):
            total = total + cond_in[row * XS * CORES + column]
        cond_ref[row] = total
    for copy in small_copies + cond_copies:
        copy.wait_send()
    finish()


def scatter_last(pieces, units, small, matrix, lines, ident):
    count = len(pieces)
    chunks = scatter_chunks(pieces, units)
    shapes = [sum_shape(piece) for piece in pieces]
    depth = matrix.shape[0]
    results = pl.pallas_call(
        partial(scatter_kernel, chunks, count, lines),
        out_shape=[jax.ShapeDtypeStruct(shape, jnp.float32) for shape in shapes]
        + [
            jax.ShapeDtypeStruct((ZS * YS * XS,) + small.shape[1:], jnp.float32),
            jax.ShapeDtypeStruct((ZS * YS, 8, depth), jnp.float32),
        ],
        in_specs=[VMEM] * (4 * count + 2),
        out_specs=[VMEM] * (count + 2),
        scratch_shapes=[
            pltpu.VMEM((ZS * YS, 8, depth), jnp.float32),
            pltpu.VMEM((DEVICES, 8, depth), jnp.float32),
        ]
        + semaphores_of(ZS * YS * XS - 1, DEVICES - 1)
        + scatter_scratch(chunks, shapes),
        compiler_params=pltpu.CompilerParams(
            collective_id=ident, has_side_effects=True, vmem_limit_bytes=60 * 2**20
        ),
        name="scatter_last",
    )(*[array for piece in pieces for array in piece], small, matrix)
    return results[:count], results[count], results[count + 1]


QUARTER = HEAD // 4
BLOCK = 256


def turn(values, tables, back):
    cosine, to_left, to_right = tables
    swapped = (
        pltpu.roll(values, LANES - QUARTER, axis=1) * to_left
        + pltpu.roll(values, QUARTER, axis=1) * to_right
    )
    return values * cosine - swapped if back else values * cosine + swapped


def head_lanes(source, at, start, end):
    short = max(start + LANES - end, 0)
    values = source[at, start - short : start - short + LANES]
    return pltpu.roll(values, LANES - short, axis=1) if short else values


def attend_kernel(heads, scale, chunks, matrices, *refs):
    projected, (cos_ref, left_ref, right_ref, hide_ref) = refs[0], refs[1:5]
    shards, refs = refs[5 : 5 + matrices], refs[5 + matrices :]
    out_ref, (query_ref, key_ref, value_ref, logsum_ref) = refs[0], refs[1:5]
    wholes, held, gather_refs = refs[5 : 5 + matrices], refs[5 + matrices], refs[6 + matrices :]
    slots, half_width = cos_ref.shape[0], projected.shape[1] // XS
    per = heads // 2
    blocks = slots // BLOCK
    greet(line_peers())
    start, events, end = gather_plan(chunks, GATHER_SPACING, shards, wholes, *gather_refs)
    start()
    table = table_of(events, GATHER_WEIGHTS, heads * blocks + 1)
    for event in table[0]:
        event()

    def prepare(i, carry):
        at = pl.ds(pl.multiple_of(i * BLOCK, BLOCK), BLOCK)
        tables = cos_ref[at, :], left_ref[at, :], right_ref[at, :]
        hide = hide_ref[at, :]
        lane = lax.broadcasted_iota(jnp.int32, (BLOCK, LANES), 1)
        for head in range(heads):
            half, local = head // per, head % per
            for part, target in enumerate((query_ref, key_ref, value_ref)):
                start = half * half_width + (part * per + local) * HEAD
                values = head_lanes(projected, at, start, XS * half_width)
                if part == 2:
                    values = jnp.where(lane < HEAD, values, 0.0)
                else:
                    values = turn(values, tables, False)
                    values = values + (jnp.where(lane == HEAD, 1.0, 0.0) if part == 0 else hide)
                target[head, at, :] = values.astype(jnp.bfloat16)
        return carry

    lax.fori_loop(0, blocks, prepare, 0)

    def attend(i, carry):
        dispatch(table[1:], i, 0, heads * blocks)
        head, block = i // blocks, i % blocks
        at = pl.ds(pl.multiple_of(block * BLOCK, BLOCK), BLOCK)
        scores = contract(query_ref[head, at, :], key_ref[head], 1, 1)
        highest = jnp.max(scores, 1, keepdims=True)
        exponent = jnp.exp2((scores - highest) * (scale * LOG2E))
        denominator = jnp.sum(exponent, 1, keepdims=True)
        result = jnp.dot(
            exponent.astype(jnp.bfloat16), value_ref[head], preferred_element_type=jnp.float32
        )
        held[head, at, :] = result / denominator
        logsum_ref[head, at, :] = jnp.broadcast_to(
            (highest * scale + jnp.log(denominator)) * LOG2E, (BLOCK, LANES)
        )
        return carry

    lax.fori_loop(0, heads * blocks, attend, 0)
    out_half = out_ref.shape[1] // XS

    def finish(i, carry):
        at = pl.ds(pl.multiple_of(i * BLOCK, BLOCK), BLOCK)
        padding = jnp.zeros((BLOCK, out_half - per * HEAD), jnp.float32)
        for half in range(2):
            pieces = [held[half * per + local, at, :][:, :HEAD] for local in range(per)]
            row = jnp.concatenate(pieces + [padding], 1)
            out_ref[at, half * out_half : (half + 1) * out_half] = row.astype(jnp.bfloat16)
        return carry

    lax.fori_loop(0, blocks, finish, 0)
    end()


def attend(projected, tables, shards, units, out_half, heads, scale, ident):
    slots = projected.shape[0]
    count = len(shards)
    chunks = grouped(count, shards[0].shape[0], units)
    packed = jax.ShapeDtypeStruct((heads, slots, LANES), jnp.bfloat16)
    results = pl.pallas_call(
        partial(attend_kernel, heads, scale, chunks, count),
        out_shape=[
            jax.ShapeDtypeStruct((slots, XS * out_half), jnp.bfloat16),
            packed,
            packed,
            packed,
            jax.ShapeDtypeStruct((heads, slots, LANES), jnp.float32),
        ]
        + [whole_shape(shard) for shard in shards],
        in_specs=[VMEM] * (5 + count),
        out_specs=[VMEM] * 5 + [HBM] * count,
        scratch_shapes=[pltpu.VMEM((heads, slots, LANES), jnp.float32)]
        + gather_scratch(chunks, count),
        compiler_params=pltpu.CompilerParams(
            collective_id=ident, has_side_effects=True, vmem_limit_bytes=60 * 2**20
        ),
        name="attend",
    )(projected, *tables, *shards)
    return results[0], results[1:5], results[5:]


def attend_back_kernel(heads, scale, chunks, matrices, *refs):
    query_ref, key_ref, value_ref, logsum_ref = refs[:4]
    grads, (cos_ref, left_ref, right_ref) = refs[4], refs[5:8]
    pieces, refs = refs[8 : 8 + 4 * matrices], refs[8 + 4 * matrices :]
    out_ref, sums, refs = refs[0], refs[1 : 1 + matrices], refs[1 + matrices :]
    held, grad_q, grad_k, grad_v = refs[:4]
    buffers, semaphores = refs[4 : 4 + 4 * matrices], refs[4 + 4 * matrices :]
    slots, grad_half, out_half = cos_ref.shape[0], grads.shape[1] // XS, out_ref.shape[1] // XS
    per = heads // 2
    blocks = slots // BLOCK
    greet(line_peers())
    events, end = scatter_plan(chunks, SCATTER_SPACING, pieces, sums, buffers, *semaphores)
    table = table_of(events, SCATTER_WEIGHTS, heads * blocks + 1)
    for event in table[0]:
        event()

    def prepare(i, carry):
        at = pl.ds(pl.multiple_of(i * BLOCK, BLOCK), BLOCK)
        for head in range(heads):
            start = head // per * grad_half + head % per * HEAD
            piece = grads[at, start : start + HEAD]
            padding = jnp.zeros((BLOCK, LANES - HEAD), piece.dtype)
            held[head, at, :] = jnp.concatenate([piece, padding], 1)
        return carry

    lax.fori_loop(0, blocks, prepare, 0)

    def attend(i, carry):
        dispatch(table[1:], i, 0, heads * blocks)
        head, block = i // blocks, i % blocks
        at = pl.ds(pl.multiple_of(block * BLOCK, BLOCK), BLOCK)
        query, grad = query_ref[head, at, :], held[head, at, :]
        key = key_ref[head]
        scores = contract(query, key, 1, 1)
        soft = jnp.exp2(scores * (scale * LOG2E) - logsum_ref[head, at, :1])
        grad_soft = contract(grad, value_ref[head], 1, 1)
        value_part = contract(soft.astype(jnp.bfloat16), grad, 0, 0)
        product = soft * grad_soft
        inner = jnp.sum(product, 1, keepdims=True)
        grad_scores = ((product - soft * inner) * scale).astype(jnp.bfloat16)
        grad_q[head, at, :] = jnp.dot(grad_scores, key, preferred_element_type=jnp.float32)
        key_part = contract(grad_scores, query, 0, 0)

        @pl.when(block == 0)
        def _():
            grad_v[head] = value_part
            grad_k[head] = key_part

        @pl.when(block > 0)
        def _():
            grad_v[head] += value_part
            grad_k[head] += key_part

        return carry

    lax.fori_loop(0, heads * blocks, attend, 0)

    def finish(i, carry):
        at = pl.ds(pl.multiple_of(i * BLOCK, BLOCK), BLOCK)
        tables = cos_ref[at, :], left_ref[at, :], right_ref[at, :]
        padding = jnp.zeros((BLOCK, out_half - 3 * per * HEAD), jnp.float32)
        for half in range(2):
            row = []
            for part, source in enumerate((grad_q, grad_k, grad_v)):
                for local in range(per):
                    values = source[half * per + local, at, :]
                    if part < 2:
                        values = turn(values, tables, True)
                    row.append(values[:, :HEAD])
            row = jnp.concatenate(row + [padding], 1)
            out_ref[at, half * out_half : (half + 1) * out_half] = row.astype(jnp.bfloat16)
        return carry

    lax.fori_loop(0, blocks, finish, 0)
    end()


def attend_back(saved, grads, tables, pieces, units, out_half, heads, scale, ident):
    count = len(pieces)
    chunks = scatter_chunks(pieces, units)
    shapes = [sum_shape(piece) for piece in pieces]
    slots = grads.shape[0]
    wide = pltpu.VMEM((heads, slots, LANES), jnp.float32)
    results = pl.pallas_call(
        partial(attend_back_kernel, heads, scale, chunks, count),
        out_shape=[jax.ShapeDtypeStruct((slots, XS * out_half), jnp.bfloat16)]
        + [jax.ShapeDtypeStruct(shape, jnp.float32) for shape in shapes],
        in_specs=[VMEM] * (8 + 4 * count),
        out_specs=[VMEM] * (1 + count),
        scratch_shapes=[pltpu.VMEM((heads, slots, LANES), jnp.bfloat16), wide, wide, wide]
        + scatter_scratch(chunks, shapes),
        compiler_params=pltpu.CompilerParams(
            collective_id=ident, has_side_effects=True, vmem_limit_bytes=63 * 2**20
        ),
        name="attend_back",
    )(*saved, grads, *tables[:3], *[array for piece in pieces for array in piece])
    return results[0], results[1:]


def turn_tables(positions, visible):
    lane = jnp.arange(LANES)
    inside = lane < HEAD
    frequency = rope_base ** (-(lane % QUARTER).astype(jnp.float32) / QUARTER)
    by_row = positions[:, :1].astype(jnp.float32) * frequency
    by_column = positions[:, 1:].astype(jnp.float32) * frequency
    angles = jnp.where(lane < HEAD // 2, by_row, by_column)
    cosine = jnp.where(inside, jnp.cos(angles), 0.0)
    sine = jnp.where(inside, jnp.sin(angles), 0.0)
    leads = lane // QUARTER % 2 == 0
    hide = jnp.where((lane == HEAD) & ~visible[:, None], -1e30, 0.0)
    return cosine, jnp.where(leads, -sine, 0.0), jnp.where(leads, 0.0, sine), hide


def image_device(
    block_input,
    conditioning,
    patch_counts,
    positions,
    w_mod,
    b_mod,
    w_qkv,
    b_qkv,
    w_out,
    b_out,
    w_up,
    b_up,
    w_down,
    b_down,
    cotangent,
):
    own_rows, model_width = block_input.shape
    slot_count = own_rows * CORES
    shard_rows, _, feat = w_qkv.shape
    units = w_up.shape[1]
    heads = CORES * feat // HEAD
    scale = 1.0 / math.sqrt(HEAD)
    images = ZS * YS * XS
    z, y, x, core = place()
    data = z * YS + y
    bf16 = jnp.bfloat16

    def swap(values):
        return lax.ppermute(values, "tensor", CORE_SWAP)

    def both(values):
        return jnp.concatenate([values, swap(values)], 0)

    def own_sum(terms):
        return terms[:own_rows] + swap(terms[own_rows:].astype(bf16)).astype(jnp.float32)

    qkv_width = 3 * feat
    qkv_half, out_half = -(-qkv_width // LANES) * LANES, -(-feat // LANES) * LANES
    qkv_shard = jnp.pad(
        w_qkv.reshape(shard_rows, qkv_width).astype(bf16), ((0, 0), (0, qkv_half - qkv_width))
    )
    out_shard = jnp.pad(w_out.T.astype(bf16), ((0, 0), (0, out_half - feat)))
    shards = [out_shard, w_up.astype(bf16), w_down.T.astype(bf16)]

    depth, lines = -(-shard_rows // LANES) * LANES, 6 * out_half // LANES
    silu_cond = jax.nn.silu(conditioning).astype(bf16).astype(jnp.float32)
    silu_blocks = silu_cond.reshape(XS, ZS * YS, shard_rows).transpose(1, 0, 2)
    silu_blocks = jnp.pad(silu_blocks, ((0, 0), (0, 8 - XS), (0, depth - shard_rows)))
    mod_matrix = jnp.pad(
        w_mod.astype(bf16), ((0, depth - shard_rows), (0, 0), (0, out_half - feat))
    ).reshape(depth, -1)
    mod_bias = jnp.pad(jnp.where(data == 0, b_mod, 0.0), ((0, 0), (0, out_half - feat)))
    whole, silu_in, mod_parts = gather_first(
        qkv_shard, silu_blocks, mod_matrix, mod_bias.reshape(1, -1), 2
    )
    qkv_full = whole.reshape(model_width, -1)
    silu_rows = silu_in[:, :XS, :shard_rows].reshape(images, shard_rows).astype(bf16)
    mod_parts = mod_parts[:, :lines].reshape(XS * CORES, 6, out_half)[:, :, :feat]
    mod = mod_parts.transpose(1, 0, 2).reshape(6, model_width)
    shift_one, scale_one, gate_one, shift_two, scale_two, gate_two = (mod[i] for i in range(6))
    biases = jnp.concatenate([jnp.pad(b_qkv.reshape(-1), (0, qkv_half - qkv_width)), b_up])
    other_biases = lax.ppermute(biases, "tensor", X_SWAP)
    low_biases = jnp.where(x == 0, biases, other_biases)
    high_biases = jnp.where(x == 0, other_biases, biases)
    bias_qkv = jnp.concatenate([low_biases[:qkv_half], high_biases[:qkv_half]])
    bias_up = jnp.concatenate([low_biases[qkv_half:], high_biases[qkv_half:]])

    own_slots = core * own_rows + jnp.arange(own_rows)
    other_slots = (1 - core) * own_rows + jnp.arange(own_rows)
    slots = jnp.concatenate([own_slots, other_slots])
    visible = slots < lax.dynamic_index_in_dim(patch_counts, x, 0, False)
    image_start = x * slot_count
    places = jnp.concatenate(
        [
            lax.dynamic_slice_in_dim(positions, image_start + core * own_rows, own_rows, 0),
            lax.dynamic_slice_in_dim(positions, image_start + (1 - core) * own_rows, own_rows, 0),
        ]
    )
    tables = turn_tables(places, visible)

    normal_one, inverse_one = row_norm(block_input)
    normal_other = row_norm(swap(block_input))[0]
    hidden_one = jnp.concatenate(
        [
            (normal * (1.0 + scale_one) + shift_one).astype(bf16)
            for normal in (normal_one, normal_other)
        ]
    )
    projected = jnp.dot(hidden_one, qkv_full, preferred_element_type=jnp.float32) + bias_qkv
    attended, saved, wholes = attend(
        projected, tables, shards, [48, 16, 16], out_half, heads, scale, 3
    )
    out_full, up_full, down_full = (whole.reshape(model_width, -1) for whole in wholes)
    branch_one = own_sum(contract(attended, out_full, 1, 1)) + b_out
    middle = block_input + gate_one * branch_one
    normal_two, inverse_two = row_norm(middle)
    hidden_two = both((normal_two * (1.0 + scale_two) + shift_two).astype(bf16))
    up_pre = jnp.dot(hidden_two, up_full, preferred_element_type=jnp.float32) + bias_up
    activated = gelu_tanh(up_pre).astype(bf16)
    branch_two = own_sum(contract(activated, down_full, 1, 1)) + b_down
    block_output = middle + gate_two * branch_two

    def norm_back(grad_hidden, normal, inverse, factor):
        grad_normal = grad_hidden * (1.0 + factor)
        mean_plain = jnp.mean(grad_normal, 1, keepdims=True)
        mean_cross = jnp.mean(grad_normal * normal, 1, keepdims=True)
        return inverse[:, None] * (grad_normal - mean_plain - normal * mean_cross)

    def column_sum(values):
        return jnp.sum(values.astype(jnp.float32), 0)

    grad_gate_two = jnp.sum(cotangent * branch_two, 0)
    grad_rows_two = both((cotangent * gate_two).astype(bf16))
    grad_bdown = column_sum(grad_rows_two)
    grad_down = contract(grad_rows_two, activated, 0, 0).astype(bf16)
    sent_down, grad_rows_two = send_off(grad_down, 0, grad_rows_two)
    grad_activated = jnp.dot(grad_rows_two, down_full, preferred_element_type=jnp.float32)
    grad_up = jax.vjp(gelu_tanh, up_pre)[1](grad_activated)[0].astype(bf16)
    grad_bup = column_sum(grad_up)
    grad_wup = contract(hidden_two, grad_up, 0, 0).astype(bf16)
    sent_down, grad_up = arrive_before(sent_down, grad_up)
    sent_up, grad_up = send_off(grad_wup, 1, grad_up)
    grad_hidden_two = own_sum(contract(grad_up, up_full, 1, 1))
    grad_shift_two = jnp.sum(grad_hidden_two, 0)
    grad_scale_two = jnp.sum(grad_hidden_two * normal_two, 0)
    grad_middle = cotangent + norm_back(grad_hidden_two, normal_two, inverse_two, scale_two)
    grad_gate_one = jnp.sum(grad_middle * branch_one, 0)
    grad_rows_one = both((grad_middle * gate_one).astype(bf16))
    grad_bout = column_sum(grad_rows_one)
    grad_out = contract(grad_rows_one, attended, 0, 0).astype(bf16)
    sent_out, grad_rows_one = send_off(grad_out, 1, grad_rows_one)
    grad_attended = jnp.dot(grad_rows_one, out_full, preferred_element_type=jnp.float32)
    grad_projected, (sum_down, sum_up) = attend_back(
        saved,
        grad_attended.astype(bf16),
        tables,
        [settle(sent_down), settle(sent_up)],
        [16, 16],
        qkv_half,
        heads,
        scale,
        6,
    )
    grad_qkv = contract(hidden_one, grad_projected, 0, 0).astype(bf16)
    sent_qkv, grad_projected = send_off(grad_qkv, 0, grad_projected)
    bias_terms = column_sum(grad_projected).reshape(2, qkv_half)
    grad_hidden_one = own_sum(contract(grad_projected, qkv_full, 1, 1))
    grad_shift_one = jnp.sum(grad_hidden_one, 0)
    grad_scale_one = jnp.sum(grad_hidden_one * normal_one, 0)
    grad_input = grad_middle + norm_back(grad_hidden_one, normal_one, inverse_one, scale_one)

    grad_mod = jnp.stack(
        [
            grad_shift_one,
            grad_scale_one,
            grad_gate_one,
            grad_shift_two,
            grad_scale_two,
            grad_gate_two,
        ]
    )
    grad_mod = (grad_mod + swap(grad_mod)).astype(bf16).astype(jnp.float32)
    grad_mod = grad_mod.reshape(6, XS, CORES, feat)
    grad_mod = lax.dynamic_index_in_dim(grad_mod, core, 2, False)
    grad_mod = jnp.pad(grad_mod, ((0, 0), (0, 0), (0, out_half - feat)))
    small = qkv_half + units + 2 * model_width
    rest = -(-(lines * LANES + small) // (8 * LANES)) * 8 * LANES - lines * LANES - small
    sends = []
    for half in range(2):
        flat = jnp.concatenate(
            [
                grad_mod[:, half].reshape(-1),
                bias_terms[half],
                grad_bup[half * units : (half + 1) * units],
                grad_bout,
                grad_bdown,
                jnp.zeros(rest, jnp.float32),
            ]
        )
        sends.append(flat.reshape(-1, LANES))
    (sum_out, sum_qkv), small_all, silu_sum = scatter_last(
        [settle(sent_out), settle(sent_qkv)], [48, 16], jnp.stack(sends), mod_matrix, lines, 7
    )
    grad_wqkv = sum_qkv[:, :qkv_width].reshape(shard_rows, 3, feat)
    grad_wout = sum_out[:, :feat].T
    grad_wdown = sum_down.T
    summed = jnp.sum(small_all, 0)
    grad_bmod = summed[:lines].reshape(6, out_half)[:, :feat]
    summed = summed[lines:].reshape(-1)
    grad_bqkv = summed[:qkv_width].reshape(3, feat)
    grad_bup = summed[qkv_half : qkv_half + units]
    offset = qkv_half + units
    grad_bout = summed[offset : offset + model_width]
    grad_bdown = summed[offset + model_width : offset + 2 * model_width]
    mod_all = small_all[:, :lines].reshape(images, 6, out_half)[:, :, :feat]
    mod_all = mod_all.reshape(images, 6 * feat).astype(bf16)
    grad_wmod = contract(silu_rows, mod_all, 0, 0).reshape(shard_rows, 6, feat)
    grad_silu = silu_sum[:, :XS, :shard_rows].transpose(1, 0, 2).reshape(XS, model_width)
    grad_cond = jax.vjp(jax.nn.silu, conditioning)[1](grad_silu)[0]
    return (
        block_output,
        grad_input,
        grad_cond,
        grad_wmod,
        grad_bmod,
        grad_wqkv,
        grad_bqkv,
        grad_wout,
        grad_bout,
        sum_up,
        grad_bup,
        grad_wdown,
        grad_bdown,
    )

def solution(mesh):
    body = image_device if image_per_chip(mesh) else per_device
    placed = (
        P(("dp", "tensor"), None),
        P("dp", None),
        P("dp"),
        P("dp", None),
        P("dp", None, "tensor"),
        P(None, "tensor"),
        P("dp", None, "tensor"),
        P(None, "tensor"),
        P("tensor", "dp"),
        P(),
        P("dp", "tensor"),
        P("tensor"),
        P("tensor", "dp"),
        P(),
        P(("dp", "tensor"), None),
    )
    return jax.shard_map(
        body,
        mesh=mesh,
        in_specs=placed,
        out_specs=(
            P(("dp", "tensor"), None),
            P(("dp", "tensor"), None),
            P("dp", None),
            P("dp", None, "tensor"),
            P(None, "tensor"),
            P("dp", None, "tensor"),
            P(None, "tensor"),
            P("tensor", "dp"),
            P(),
            P("dp", "tensor"),
            P("tensor"),
            P("tensor", "dp"),
            P(),
        ),
        check_vma=False,
    )
```

```python
from functools import partial
import math

import jax
import jax.numpy as jnp
from jax import lax
from jax.experimental import pallas as pl
from jax.experimental.pallas import tpu as pltpu
from jax.sharding import PartitionSpec as P

HEAD = 72


epsilon = 1e-06
rope_base = 10000.0
gelu_coeff = 0.044715
root_two_pi = math.sqrt(2.0 / math.pi)


def gelu_tanh(values):
    return (
        0.5
        * values
        * (1.0 + jnp.tanh(root_two_pi * (values + gelu_coeff * values * values * values)))
    )


def rotate(values, positions, direction):
    quarter = values.shape[-1] // 4
    frequency = rope_base ** (-jnp.arange(quarter, dtype=jnp.float32) / quarter)
    pieces = []
    for column in range(2):
        angles = positions[:, column].astype(jnp.float32)[:, None, None] * frequency
        cosine = jnp.cos(angles)
        sine_term = direction * jnp.sin(angles)
        leading = values[..., 2 * column * quarter : (2 * column + 1) * quarter]
        trailing = values[..., (2 * column + 1) * quarter : (2 * column + 2) * quarter]
        pieces.append(leading * cosine - trailing * sine_term)
        pieces.append(leading * sine_term + trailing * cosine)
    return jnp.concatenate(pieces, -1)


def contract(left, right, left_dim, right_dim):
    return lax.dot_general(
        left, right, (((left_dim,), (right_dim,)), ((), ())), preferred_element_type=jnp.float32
    )


def exact_dot(left, right):
    return jnp.dot(left, right, precision=lax.Precision.HIGHEST, preferred_element_type=jnp.float32)


def row_norm(rows):
    average = jnp.mean(rows, 1)
    inverse = lax.rsqrt(jnp.mean(rows * rows, 1) - average * average + epsilon)
    return ((rows - average[:, None]) * inverse[:, None], inverse)


def masked_scores(query_rows, key_rows, patch_count, factor):
    raw_scores = (
        jnp.einsum("qhd,khd->hqk", query_rows, key_rows, preferred_element_type=jnp.float32)
        * factor
    )
    visible = jnp.arange(key_rows.shape[0]) < patch_count
    return jnp.where(visible[None, None, :], raw_scores, -1e30)


def attend_forward(factor, inputs):
    query_rows, key_rows, value_rows, patch_count = inputs
    scores = masked_scores(query_rows, key_rows, patch_count, factor)
    highest = jnp.max(scores, -1, keepdims=True)
    exponent = jnp.exp(scores - highest)
    denominator = jnp.sum(exponent, -1, keepdims=True)
    softmax_rows = (exponent / denominator).astype(jnp.bfloat16)
    attended = jnp.einsum(
        "hqk,khd->qhd", softmax_rows, value_rows, preferred_element_type=jnp.float32
    )
    return (attended, (highest + jnp.log(denominator))[..., 0])


def attend_backward(factor, inputs):
    query_rows, key_rows, value_rows, patch_count, logsum, grad_rows = inputs
    scores = masked_scores(query_rows, key_rows, patch_count, factor)
    softmax_rows = jnp.exp(scores - logsum[..., None])
    grad_soft = jnp.einsum(
        "qhd,khd->hqk", grad_rows, value_rows, preferred_element_type=jnp.float32
    )
    grad_values = jnp.einsum(
        "hqk,qhd->khd",
        softmax_rows.astype(jnp.bfloat16),
        grad_rows,
        preferred_element_type=jnp.float32,
    )
    inner_sum = jnp.sum(softmax_rows * grad_soft, -1, keepdims=True)
    grad_scores = (softmax_rows * (grad_soft - inner_sum) * factor).astype(jnp.bfloat16)
    grad_query = jnp.einsum(
        "hqk,khd->qhd", grad_scores, key_rows, preferred_element_type=jnp.float32
    )
    grad_keys = jnp.einsum(
        "hqk,qhd->khd", grad_scores, query_rows, preferred_element_type=jnp.float32
    )
    return (grad_query, grad_keys, grad_values)


def per_device(
    block_input,
    conditioning,
    patch_counts,
    positions,
    w_mod,
    b_mod,
    w_qkv,
    b_qkv,
    w_out,
    b_out,
    w_up,
    b_up,
    w_down,
    b_down,
    cotangent,
):
    own_rows, model_width = block_input.shape
    group_rows = positions.shape[0]
    images_local = conditioning.shape[0]
    slot_count = group_rows // images_local
    feat_local = w_qkv.shape[2]
    heads_local = feat_local // HEAD
    row_start = lax.axis_index("tensor") * own_rows
    factor = 1.0 / math.sqrt(HEAD)
    image_of = (row_start + jnp.arange(own_rows)) // slot_count
    one_hot = (image_of[:, None] == jnp.arange(images_local)[None, :]).astype(jnp.float32)

    def to_rows(vectors):
        return exact_dot(one_hot, vectors)

    def to_images(values):
        return exact_dot(one_hot.T, values)

    def per_image(stacked):
        return stacked.reshape((images_local, slot_count) + stacked.shape[1:])

    def modulate_group(values, shift, scale):
        shaped = values.reshape(images_local, slot_count, values.shape[1])
        return (shaped * (1.0 + scale[:, None, :]) + shift[:, None, :]).reshape(values.shape)

    mod_full, qkv_full, out_full, up_full, down_full = (
        lax.all_gather(w_mod.astype(jnp.bfloat16), "dp", axis=0, tiled=True),
        lax.all_gather(w_qkv.astype(jnp.bfloat16), "dp", axis=0, tiled=True),
        lax.all_gather(w_out.astype(jnp.bfloat16), "dp", axis=1, tiled=True),
        lax.all_gather(w_up.astype(jnp.bfloat16), "dp", axis=0, tiled=True),
        lax.all_gather(w_down.astype(jnp.bfloat16), "dp", axis=1, tiled=True),
    )
    silu_cond = jax.nn.silu(conditioning).astype(jnp.bfloat16)
    mod_cols = jnp.dot(
        silu_cond, mod_full.reshape(model_width, 6 * feat_local), preferred_element_type=jnp.float32
    )
    mod_cols = mod_cols.reshape(images_local, 6, feat_local) + b_mod
    mod_all = lax.all_gather(mod_cols, "tensor", axis=2, tiled=True)

    def norm_gather(rows_local, shift, scale):
        rows_group = lax.all_gather(rows_local, "tensor", axis=0, tiled=True)
        normal_group, inverse_group = row_norm(rows_group)
        hidden = modulate_group(normal_group, shift, scale).astype(jnp.bfloat16)
        normal = lax.dynamic_slice_in_dim(normal_group, row_start, own_rows, 0)
        inverse = lax.dynamic_slice_in_dim(inverse_group, row_start, own_rows, 0)
        return (hidden, normal, inverse)

    hidden_one, normal_one, inverse_one = norm_gather(block_input, mod_all[:, 0], mod_all[:, 1])
    projected = jnp.dot(
        hidden_one,
        qkv_full.reshape(model_width, 3 * feat_local),
        preferred_element_type=jnp.float32,
    ) + b_qkv.reshape(-1)
    projected = projected.reshape(group_rows, 3, heads_local, HEAD)
    query_rows = rotate(projected[:, 0], positions, 1.0).astype(jnp.bfloat16)
    key_rows = rotate(projected[:, 1], positions, 1.0).astype(jnp.bfloat16)
    value_rows = projected[:, 2].astype(jnp.bfloat16)
    attended, logsum = lax.map(
        partial(attend_forward, factor),
        (per_image(query_rows), per_image(key_rows), per_image(value_rows), patch_counts),
    )
    attended = attended.reshape(group_rows, feat_local).astype(jnp.bfloat16)

    def branch_sum(partial_terms, offset):
        return lax.psum_scatter(partial_terms, "tensor", scatter_dimension=0, tiled=True) + offset

    gate_one_rows = to_rows(mod_all[:, 2])
    gate_two_rows = to_rows(mod_all[:, 5])
    branch_one = branch_sum(jnp.dot(attended, out_full, preferred_element_type=jnp.float32), b_out)
    middle = block_input + gate_one_rows * branch_one
    hidden_two, normal_two, inverse_two = norm_gather(middle, mod_all[:, 3], mod_all[:, 4])
    up_pre = jnp.dot(hidden_two, up_full, preferred_element_type=jnp.float32) + b_up
    activated = gelu_tanh(up_pre).astype(jnp.bfloat16)
    branch_two = branch_sum(
        jnp.dot(activated, down_full, preferred_element_type=jnp.float32), b_down
    )
    block_output = middle + gate_two_rows * branch_two
    mod_back, qkv_back, out_back, up_back, down_back = (
        lax.all_gather(w_mod.astype(jnp.bfloat16), "dp", axis=0, tiled=True),
        lax.all_gather(w_qkv.astype(jnp.bfloat16), "dp", axis=0, tiled=True),
        lax.all_gather(w_out.astype(jnp.bfloat16), "dp", axis=1, tiled=True),
        lax.all_gather(w_up.astype(jnp.bfloat16), "dp", axis=0, tiled=True),
        lax.all_gather(w_down.astype(jnp.bfloat16), "dp", axis=1, tiled=True),
    )

    def spread_grad(grad_branch):
        return lax.all_gather(grad_branch, "tensor", axis=0, tiled=True)

    def input_sum(partial_terms):
        return lax.psum_scatter(partial_terms, "tensor", scatter_dimension=0, tiled=True)

    def norm_backward(grad_hidden, normal, inverse, scale):
        grad_normal = grad_hidden * (1.0 + to_rows(scale))
        mean_plain = jnp.mean(grad_normal, 1, keepdims=True)
        mean_cross = jnp.mean(grad_normal * normal, 1, keepdims=True)
        return inverse[:, None] * (grad_normal - mean_plain - normal * mean_cross)

    grad_gate_two = to_images(cotangent * branch_two)
    grad_branch_two = (cotangent * gate_two_rows).astype(jnp.bfloat16)
    grad_rows_two = spread_grad(grad_branch_two)
    grad_bdown_local = jnp.sum(grad_rows_two.astype(jnp.float32), 0)
    grad_wdown_local = contract(activated, grad_rows_two, 0, 0)
    grad_activated = contract(grad_rows_two, down_back, 1, 1)
    gelu_pull = jax.vjp(gelu_tanh, up_pre)[1]
    grad_up = gelu_pull(grad_activated)[0].astype(jnp.bfloat16)
    grad_bup_local = jnp.sum(grad_up.astype(jnp.float32), 0)
    grad_wup_local = contract(hidden_two, grad_up, 0, 0)
    grad_hidden_two = input_sum(contract(grad_up, up_back, 1, 1))
    grad_shift_two = to_images(grad_hidden_two)
    grad_scale_two = to_images(grad_hidden_two * normal_two)
    grad_middle = cotangent + norm_backward(grad_hidden_two, normal_two, inverse_two, mod_all[:, 4])
    grad_gate_one = to_images(grad_middle * branch_one)
    grad_branch_one = (grad_middle * gate_one_rows).astype(jnp.bfloat16)
    grad_rows_one = spread_grad(grad_branch_one)
    grad_bout_local = jnp.sum(grad_rows_one.astype(jnp.float32), 0)
    grad_wout_local = contract(attended, grad_rows_one, 0, 0)
    grad_attended = contract(grad_rows_one, out_back, 1, 1).astype(jnp.bfloat16)
    grad_attended = grad_attended.reshape(group_rows, heads_local, HEAD)
    grad_query, grad_keys, grad_values = lax.map(
        partial(attend_backward, factor),
        (
            per_image(query_rows),
            per_image(key_rows),
            per_image(value_rows),
            patch_counts,
            logsum,
            per_image(grad_attended),
        ),
    )
    head_shape = (group_rows, heads_local, HEAD)
    grad_projected = jnp.stack(
        [
            rotate(grad_query.reshape(head_shape), positions, -1.0),
            rotate(grad_keys.reshape(head_shape), positions, -1.0),
            grad_values.reshape(head_shape),
        ],
        1,
    )
    grad_projected = grad_projected.astype(jnp.bfloat16).reshape(group_rows, 3 * feat_local)
    grad_bqkv_local = jnp.sum(grad_projected.astype(jnp.float32), 0).reshape(3, feat_local)
    grad_wqkv_local = contract(hidden_one, grad_projected, 0, 0).reshape(model_width, 3, feat_local)
    grad_hidden_one = input_sum(
        contract(grad_projected, qkv_back.reshape(model_width, 3 * feat_local), 1, 1)
    )
    grad_shift_one = to_images(grad_hidden_one)
    grad_scale_one = to_images(grad_hidden_one * normal_one)
    grad_input = grad_middle + norm_backward(
        grad_hidden_one, normal_one, inverse_one, mod_all[:, 1]
    )
    grad_mod_part = jnp.stack(
        [
            grad_shift_one,
            grad_scale_one,
            grad_gate_one,
            grad_shift_two,
            grad_scale_two,
            grad_gate_two,
        ],
        1,
    )
    grad_mod = lax.psum_scatter(grad_mod_part, "tensor", scatter_dimension=2, tiled=True).astype(
        jnp.bfloat16
    )
    grad_bmod_local = jnp.sum(grad_mod.astype(jnp.float32), 0)
    grad_mod_flat = grad_mod.reshape(images_local, 6 * feat_local)
    grad_wmod_local = contract(silu_cond, grad_mod_flat, 0, 0).reshape(model_width, 6, feat_local)
    grad_silu = lax.psum(
        contract(grad_mod_flat, mod_back.reshape(model_width, 6 * feat_local), 1, 1), "tensor"
    )
    silu_pull = jax.vjp(jax.nn.silu, conditioning)[1]
    grad_cond = silu_pull(grad_silu)[0]
    grad_wmod, grad_wqkv, grad_wout, grad_wup, grad_wdown = (
        lax.psum_scatter(
            grad_wmod_local.astype(jnp.bfloat16), "dp", scatter_dimension=0, tiled=True
        ).astype(jnp.float32),
        lax.psum_scatter(
            grad_wqkv_local.astype(jnp.bfloat16), "dp", scatter_dimension=0, tiled=True
        ).astype(jnp.float32),
        lax.psum_scatter(
            grad_wout_local.astype(jnp.bfloat16), "dp", scatter_dimension=1, tiled=True
        ).astype(jnp.float32),
        lax.psum_scatter(
            grad_wup_local.astype(jnp.bfloat16), "dp", scatter_dimension=0, tiled=True
        ).astype(jnp.float32),
        lax.psum_scatter(
            grad_wdown_local.astype(jnp.bfloat16), "dp", scatter_dimension=1, tiled=True
        ).astype(jnp.float32),
    )
    grad_bmod, grad_bqkv, grad_bout, grad_bup, grad_bdown = lax.psum(
        (grad_bmod_local, grad_bqkv_local, grad_bout_local, grad_bup_local, grad_bdown_local), "dp"
    )
    return (
        block_output,
        grad_input,
        grad_cond,
        grad_wmod,
        grad_bmod,
        grad_wqkv,
        grad_bqkv,
        grad_wout,
        grad_bout,
        grad_wup,
        grad_bup,
        grad_wdown,
        grad_bdown,
    )


LANES = 128
ZS, YS, XS, CORES = 4, 2, 2, 2
MESH_ID = pl.DeviceIdType.MESH
CORE_SWAP = [(0, 1), (1, 0), (2, 3), (3, 2)]
X_SWAP = [(0, 2), (2, 0), (1, 3), (3, 1)]
Y_SWAP = [(i, i ^ 1) for i in range(ZS * YS)]
LOG2E = 1.0 / math.log(2.0)
HBM = pl.BlockSpec(memory_space=pl.ANY)
VMEM = pl.BlockSpec(memory_space=pltpu.VMEM)


def image_per_chip(mesh):
    return dict(mesh.shape) == {"dp": ZS * YS, "tensor": XS * CORES}


def place():
    data, tensor = lax.axis_index("dp"), lax.axis_index("tensor")
    return data // YS, data % YS, tensor // CORES, tensor % CORES


def flip_z(z, step):
    high, low = z // 2, z % 2
    if step & 2:
        high = 1 - high
    if step & 1:
        low = 1 - low
    return high * 2 + low


def device(z, y, x, core):
    return (z * YS + y, x * CORES + core)


def greet(targets):
    barrier = pltpu.get_barrier_semaphore()
    for target in targets:
        pl.semaphore_signal(barrier, inc=1, device_id=target, device_id_type=MESH_ID)
    pl.semaphore_wait(barrier, len(targets))


GATHER_STEPS, SCATTER_STEPS = 5, 5
GATHER_SPACING, SCATTER_SPACING = 8.0, 8.0
GATHER_WEIGHTS, SCATTER_WEIGHTS = (1, 1, 1, 1, 1), (1, 1, 1, 1, 1)


def grouped(matrices, rows, units):
    chunks = []
    for matrix in range(matrices):
        unit = units[matrix]
        for number, row in enumerate(range(0, rows, 3 * unit)):
            short = (matrix + number) % 2
            chunks.append((matrix, row, unit, 2))
            chunks.append((matrix, row + unit, unit, 3))
            chunks.append((matrix, row + 2 * unit, unit, short))
    return chunks


def in_order(count, steps, spacing, act):
    events = sorted((c + s * spacing, c, s) for c in range(count) for s in range(steps))
    return [(s, partial(act, c, s)) for time, c, s in events]


def run_all(events):
    for _, event in events:
        event()


def table_of(events, weights, trips):
    total = sum(weights[step] for step, _ in events)
    table, sent = [[] for _ in range(trips)], 0
    for step, event in events:
        table[min(sent * trips // total, trips - 1)].append(event)
        sent += weights[step]
    return table


def dispatch(table, index, low, high):
    if not any(table[low:high]):
        return
    if high - low == 1:
        for event in table[low]:
            event()
        return
    middle = (low + high) // 2
    pl.when(index < middle)(lambda: dispatch(table, index, low, middle))
    pl.when(index >= middle)(lambda: dispatch(table, index, middle, high))


def gather_plan(chunks, spacing, shards, wholes, sends, recvs, local):
    z, y, x, core = place()
    inner = jnp.logical_or(z == 1, z == 2)
    every = slice(None)

    def mine_of(matrix):
        width = shards[matrix].shape[1]
        return pl.ds(pl.multiple_of(x * width, LANES), width)

    at_x, at_y = device(z, y, 1 - x, core), device(z, 1 - y, x, core)
    beside, mirror = device(flip_z(z, 1), y, x, core), device(3 - z, y, x, core)
    pair = pl.ds(z // 2 * 2, 2)
    far = pl.ds(2 - z // 2 * 2, 2)

    def copy(number, send, recv, source, target, where):
        return pltpu.make_async_remote_copy(
            src_ref=source,
            dst_ref=target,
            send_sem=sends.at[number * 5 + send],
            recv_sem=recvs.at[number * 4 + recv],
            device_id=where,
            device_id_type=MESH_ID,
        )

    def moves(number):
        matrix, row, rows, route = chunks[number]
        whole, span, mine = wholes[matrix], pl.ds(row, rows), mine_of(matrix)
        own, shard = whole.at[z, y, span, mine], shards[matrix].at[span, :]
        lines, columns = (every if route == 3 else y), (every if route == 2 else mine)
        made = {}
        near = shard if route < 2 else whole.at[z, lines, span, columns]
        near_to = own if route < 2 else near
        made["near"] = partial(copy, number, 0, 0, near, near_to, beside)
        both = whole.at[pair, lines, span, columns]
        made["mirror"] = partial(copy, number, 1, 1, both, both, mirror)
        there = whole.at[far, lines, span, columns]
        made["forward"] = partial(copy, number, 2, 1, there, there, beside)
        if route < 2:
            column = whole.at[:, y, span, mine]
            made["second"] = partial(copy, number, 3, 2, column, column, at_x if route == 0 else at_y)
        else:
            made["first"] = partial(copy, number, 3, 2, shard, own, at_x if route == 2 else at_y)
        if route in (0, 2):
            last = whole.at[:, y, span, :]
        else:
            last = whole.at[:, :, span, mine]
        made["third"] = partial(copy, number, 4, 3, last, last, at_y if route in (0, 2) else at_x)
        return made

    def keep(matrix):
        return pltpu.make_async_copy(
            shards[matrix], wholes[matrix].at[z, y, :, mine_of(matrix)], local.at[matrix]
        )

    kept = []

    def ready(number):
        matrix = chunks[number][0]
        if matrix not in kept:
            kept.append(matrix)
            keep(matrix).wait()

    def act(number, step):
        made = moves(number)
        straight = chunks[number][3] < 2
        if step == 0:
            made["near" if straight else "first"]().start()
        elif step == 1:
            ready(number)
            if straight:
                made["near"]().wait_recv()
                pl.when(inner)(lambda: made["mirror"]().start())
            else:
                made["first"]().wait_recv()
                made["near"]().start()
        elif step == 2:
            if straight:
                made["mirror"]().wait_recv()
                pl.when(inner)(lambda: made["forward"]().start())
                made["second"]().start()
            else:
                made["near"]().wait_recv()
                pl.when(inner)(lambda: made["mirror"]().start())
        elif step == 3:
            if straight:
                made["second"]().wait_recv()
            else:
                made["mirror"]().wait_recv()
                pl.when(inner)(lambda: made["forward"]().start())
            made["third"]().start()
        else:
            made["third"]().wait_recv()

    def start():
        for matrix in sorted({chunk[0] for chunk in chunks}):
            keep(matrix).start()

    def finish():
        for number in range(len(chunks)):
            made = moves(number)
            for name in made:
                if name not in ("mirror", "forward"):
                    made[name]().wait_send()

            def rest(made=made):
                made["mirror"]().wait_send()
                made["forward"]().wait_send()

            pl.when(inner)(rest)

    return start, in_order(len(chunks), GATHER_STEPS, spacing, act), finish


def gather_scratch(chunks, matrices):
    count = len(chunks)
    return [
        pltpu.SemaphoreType.DMA((count * 5,)),
        pltpu.SemaphoreType.DMA((count * 4,)),
        pltpu.SemaphoreType.DMA((matrices,)),
    ]


def send_off(part, flip, after):
    z, y, x, core = place()
    rows, width = part.shape[0] // (ZS * YS), part.shape[1] // XS
    blocks = part.reshape(ZS, YS, rows, XS * width)
    split = rows // 32 * 16
    split = split if flip else rows - split
    by_y, by_x = blocks[:, :, :split], blocks[:, :, split:]
    low, high = by_x[..., :width], by_x[..., width:]
    send_y = lax.dynamic_index_in_dim(by_y, 1 - y, 1, False)
    keep_y = lax.dynamic_index_in_dim(by_y, y, 1, False)
    send_x, keep_x = jnp.where(x == 0, high, low), jnp.where(x == 0, low, high)
    send_y, send_x, after = lax.optimization_barrier((send_y, send_x, after))
    got_y = lax.ppermute(send_y, "dp", Y_SWAP)
    got_x = lax.ppermute(send_x, "tensor", X_SWAP)
    return (keep_y, got_y, keep_x, got_x), after


def arrive_before(sent, after):
    keep_y, got_y, keep_x, got_x = sent
    got_y, got_x, after = lax.optimization_barrier((got_y, got_x, after))
    return (keep_y, got_y, keep_x, got_x), after


def settle(sent):
    z, y, x, core = place()
    keep_y, got_y, keep_x, got_x = sent
    sum_y = (keep_y.astype(jnp.float32) + got_y.astype(jnp.float32)).astype(jnp.bfloat16)
    sum_x = (keep_x.astype(jnp.float32) + got_x.astype(jnp.float32)).astype(jnp.bfloat16)
    width = sum_x.shape[-1]
    low, high = sum_y[..., :width], sum_y[..., width:]
    return [
        jnp.where(x == 0, low, high),
        jnp.where(x == 0, high, low),
        lax.dynamic_index_in_dim(sum_x, y, 1, False),
        lax.dynamic_index_in_dim(sum_x, 1 - y, 1, False),
    ]


def scatter_chunks(pieces, units):
    chunks = []
    for matrix, unit in enumerate(units):
        parts, start = [], 0
        for side in range(2):
            rows = pieces[matrix][2 * side].shape[1]
            parts.append(
                [(matrix, side, row, start + row, min(unit, rows - row)) for row in range(0, rows, unit)]
            )
            start += rows
        for i in range(max(len(part) for part in parts)):
            chunks.extend(part[i] for part in parts if i < len(part))
    return chunks


def scatter_plan(chunks, spacing, pieces, sums, buffers, sends, recvs):
    z, y, x, core = place()
    inner = jnp.logical_or(z == 1, z == 2)
    outer = jnp.logical_or(z == 0, z == 3)
    at_x, at_y = device(z, y, 1 - x, core), device(z, 1 - y, x, core)
    z_near = flip_z(z, 1)
    beside, mirror = device(z_near, y, x, core), device(3 - z, y, x, core)
    pair_at, far_at = z // 2 * 2, 2 - z // 2 * 2
    far = pl.ds(far_at, 2)

    def copy(number, index, source, target, where):
        return pltpu.make_async_remote_copy(
            src_ref=source,
            dst_ref=target,
            send_sem=sends.at[number * 4 + index],
            recv_sem=recvs.at[number * 4 + index],
            device_id=where,
            device_id_type=MESH_ID,
        )

    def moves(number):
        matrix, side, row, at, rows = chunks[number]
        here, span = pl.ds(row, rows), pl.ds(at, rows)
        arrived, outer_in, mirror_in, near_in = buffers[4 * matrix : 4 * matrix + 4]
        give, two = pieces[4 * matrix + 2 * side + 1], arrived.at[far, span, :]
        return {
            "first": partial(
                copy,
                number,
                0,
                give.at[:, here, :],
                arrived.at[:, span, :],
                at_y if side else at_x,
            ),
            "outer": partial(copy, number, 1, two, outer_in.at[:, span, :], beside),
            "mirror": partial(copy, number, 2, two, mirror_in.at[:, span, :], mirror),
            "near": partial(
                copy, number, 3, arrived.at[z_near, span, :], near_in.at[span, :], beside
            ),
        }

    def add(number, count, base, source, from_row):
        matrix, side, row, at, rows = chunks[number]
        arrived, tiles = buffers[4 * matrix], rows // 16

        def one(i, carry):
            block, line = i // tiles, i % tiles
            to = pl.ds(pl.multiple_of(at + line * 16, 16), 16)
            origin = pl.ds(pl.multiple_of(from_row + line * 16, 16), 16)
            held = arrived[base + block, to, :].astype(jnp.float32)
            arrived[base + block, to, :] = (
                held + source[block, origin, :].astype(jnp.float32)
            ).astype(jnp.bfloat16)
            return carry

        lax.fori_loop(0, count * tiles, one, 0)

    def finalize(number):
        matrix, side, row, at, rows = chunks[number]
        arrived, near_in = buffers[4 * matrix], buffers[4 * matrix + 3]

        def one(i, carry):
            to = pl.ds(pl.multiple_of(at + i * 16, 16), 16)
            sums[matrix][to, :] = arrived[z, to, :].astype(jnp.float32) + near_in[to, :].astype(
                jnp.float32
            )
            return carry

        lax.fori_loop(0, rows // 16, one, 0)

    def act(number, step):
        matrix, side, row, at, rows = chunks[number]
        made = moves(number)
        stay = pieces[4 * matrix + 2 * side]
        arrived, outer_in, mirror_in, near_in = buffers[4 * matrix : 4 * matrix + 4]

        def from_outer():
            made["outer"]().wait_recv()
            add(number, 2, far_at, outer_in, at)
            made["mirror"]().start()

        def from_mirror():
            made["mirror"]().wait_recv()
            add(number, 2, pair_at, mirror_in, at)

        if step == 0:
            made["first"]().start()
        elif step == 1:
            made["first"]().wait_recv()
            add(number, ZS, 0, stay, row)
            pl.when(outer)(lambda: made["outer"]().start())
        elif step == 2:
            pl.when(inner)(from_outer)
        elif step == 3:
            pl.when(inner)(from_mirror)
            made["near"]().start()
        else:
            made["near"]().wait_recv()
            finalize(number)

    def finish():
        for number in range(len(chunks)):
            made = moves(number)
            made["first"]().wait_send()
            made["near"]().wait_send()
            pl.when(outer)(lambda made=made: made["outer"]().wait_send())
            pl.when(inner)(lambda made=made: made["mirror"]().wait_send())

    return in_order(len(chunks), SCATTER_STEPS, spacing, act), finish


def scatter_scratch(chunks, shapes):
    wide = []
    for rows, width in shapes:
        for lead in ((ZS,), (2,), (2,), ()):
            wide.append(pltpu.VMEM((*lead, rows, width), jnp.bfloat16))
    count = len(chunks) * 4
    return wide + [pltpu.SemaphoreType.DMA((count,)), pltpu.SemaphoreType.DMA((count,))]


def sum_shape(piece):
    rows = piece[0].shape[1] + piece[2].shape[1]
    return rows, piece[0].shape[2]


def line_peers():
    z, y, x, core = place()
    return [
        device(z, y, 1 - x, core),
        device(z, 1 - y, x, core),
        device(flip_z(z, 1), y, x, core),
        device(3 - z, y, x, core),
    ]


DEVICES = ZS * YS * XS * CORES


def numbers():
    z, y, x, core = place()
    data = z * YS + y
    return (data * XS + x) * CORES + core, data, data * XS + x


def device_at(number):
    return (number // (XS * CORES), number % (XS * CORES))


def greet_all():
    me = numbers()[0]
    greet([device_at((me + step) % DEVICES) for step in range(1, DEVICES)])


def send_each(count, me, source_of, arrived, device_of, sends, recvs):
    copies = []
    for step in range(1, count):
        target = (me + step) % count
        copy = pltpu.make_async_remote_copy(
            src_ref=source_of(target),
            dst_ref=arrived.at[me],
            send_sem=sends.at[step - 1],
            recv_sem=recvs.at[step - 1],
            device_id=device_of(target),
            device_id_type=MESH_ID,
        )
        copy.start()
        copies.append(copy)
    return copies


def receive(copies):
    for copy in copies:
        copy.wait_recv()


def semaphores_of(*counts):
    return [pltpu.SemaphoreType.DMA((count,)) for count in counts for _ in range(2)]


def gather_kernel(chunks, *refs):
    shard, silu_blocks, matrix_ref, bias_ref = refs[:4]
    whole, silu_in, mod_ref = refs[4:7]
    parts, mod_in, silu_sends, silu_recvs, mod_sends, mod_recvs = refs[7:13]
    me, data, _ = numbers()
    z, y, x, core = place()
    greet_all()
    silu_copies = send_each(
        ZS * YS,
        data,
        lambda target: silu_blocks.at[target],
        silu_in,
        lambda target: (target, lax.axis_index("tensor")),
        silu_sends,
        silu_recvs,
    )
    start, events, finish = gather_plan(chunks, GATHER_SPACING, [shard], [whole], *refs[13:])
    start()
    early = len(chunks) // 2
    run_all(events[:early])
    silu_in[data] = silu_blocks[data]
    receive(silu_copies)
    rows = silu_in[...].reshape(silu_in.shape[0] * silu_in.shape[1], silu_in.shape[2])
    product = jnp.dot(
        rows.astype(jnp.bfloat16), matrix_ref[...], preferred_element_type=jnp.float32
    )
    product = product + bias_ref[...]
    lines = product.shape[1] // LANES
    for line in range(lines):
        piece = product[:, line * LANES : (line + 1) * LANES]
        parts[:, :, line, :] = piece.reshape(parts.shape[0], parts.shape[1], LANES)
    for line in range(lines, parts.shape[2]):
        parts[:, :, line, :] = jnp.zeros((parts.shape[0], parts.shape[1], LANES), jnp.float32)
    run_all(events[early : 2 * early])
    mod_copies = send_each(
        DEVICES,
        me,
        lambda target: parts.at[target // (XS * CORES), target % (XS * CORES) // CORES],
        mod_in,
        device_at,
        mod_sends,
        mod_recvs,
    )
    mod_in[me] = parts[data, x]
    run_all(events[2 * early :])
    receive(mod_copies)
    for column in range(XS * CORES):
        total = mod_in[column]
        for row in range(1, ZS * YS):
            total = total + mod_in[row * XS * CORES + column]
        mod_ref[column] = total
    for copy in silu_copies + mod_copies:
        copy.wait_send()
    finish()


def whole_shape(shard):
    rows, width = shard.shape
    return jax.ShapeDtypeStruct((ZS, YS, rows, XS * width), jnp.bfloat16)


def gather_first(shard, silu_blocks, matrix, bias, ident):
    chunks = grouped(1, shard.shape[0], [16])
    groups, rows, _ = silu_blocks.shape
    lines = -(-matrix.shape[1] // (8 * LANES)) * 8
    return pl.pallas_call(
        partial(gather_kernel, chunks),
        out_shape=[
            whole_shape(shard),
            jax.ShapeDtypeStruct(silu_blocks.shape, jnp.float32),
            jax.ShapeDtypeStruct((XS * CORES, lines, LANES), jnp.float32),
        ],
        in_specs=[VMEM] * 4,
        out_specs=[HBM, VMEM, VMEM],
        scratch_shapes=[
            pltpu.VMEM((groups, rows, lines, LANES), jnp.float32),
            pltpu.VMEM((DEVICES, lines, LANES), jnp.float32),
        ]
        + semaphores_of(groups - 1, DEVICES - 1)
        + gather_scratch(chunks, 1),
        compiler_params=pltpu.CompilerParams(collective_id=ident, has_side_effects=True),
        name="gather_first",
    )(shard, silu_blocks, matrix, bias)


def scatter_kernel(chunks, matrices, lines, *refs):
    pieces, (small_ref, matrix_ref) = refs[: 4 * matrices], refs[4 * matrices : 4 * matrices + 2]
    refs = refs[4 * matrices + 2 :]
    sums, (small_in, cond_ref), refs = refs[:matrices], refs[matrices : matrices + 2], refs[matrices + 2 :]
    silu_parts, cond_in, small_sends, small_recvs, cond_sends, cond_recvs = refs[:6]
    buffers, semaphores = refs[6 : 6 + 4 * matrices], refs[6 + 4 * matrices :]
    me, data, chip = numbers()
    z, y, x, core = place()
    chips = ZS * YS * XS
    greet_all()
    small_copies = send_each(
        chips,
        chip,
        lambda target: small_ref.at[target % XS],
        small_in,
        lambda target: (target // XS, target % XS * CORES + core),
        small_sends,
        small_recvs,
    )
    events, finish = scatter_plan(chunks, SCATTER_SPACING, pieces, sums, buffers, *semaphores)
    run_all(events[: len(chunks)])
    small_in[chip] = small_ref[x]
    silu_parts[...] = jnp.zeros_like(silu_parts)
    receive(small_copies)
    total = jnp.zeros((chips, matrix_ref.shape[0]), jnp.float32)
    for line in range(lines):
        total = total + contract(
            small_in[:, line, :].astype(jnp.bfloat16),
            matrix_ref[:, line * LANES : (line + 1) * LANES],
            1,
            1,
        )
    for image in range(chips):
        at = image % XS
        silu_parts[image // XS, at : at + 1, :] = total[image : image + 1, :]
    middle = 2 * len(chunks)
    run_all(events[len(chunks) : middle])
    cond_copies = send_each(
        DEVICES,
        me,
        lambda target: silu_parts.at[target // (XS * CORES)],
        cond_in,
        device_at,
        cond_sends,
        cond_recvs,
    )
    cond_in[me] = silu_parts[data]
    run_all(events[middle:])
    receive(cond_copies)
    for row in range(ZS * YS):
        total = cond_in[row * XS * CORES]
        for column in range(1, XS * CORES):
            total = total + cond_in[row * XS * CORES + column]
        cond_ref[row] = total
    for copy in small_copies + cond_copies:
        copy.wait_send()
    finish()


def scatter_last(pieces, units, small, matrix, lines, ident):
    count = len(pieces)
    chunks = scatter_chunks(pieces, units)
    shapes = [sum_shape(piece) for piece in pieces]
    depth = matrix.shape[0]
    results = pl.pallas_call(
        partial(scatter_kernel, chunks, count, lines),
        out_shape=[jax.ShapeDtypeStruct(shape, jnp.float32) for shape in shapes]
        + [
            jax.ShapeDtypeStruct((ZS * YS * XS,) + small.shape[1:], jnp.float32),
            jax.ShapeDtypeStruct((ZS * YS, 8, depth), jnp.float32),
        ],
        in_specs=[VMEM] * (4 * count + 2),
        out_specs=[VMEM] * (count + 2),
        scratch_shapes=[
            pltpu.VMEM((ZS * YS, 8, depth), jnp.float32),
            pltpu.VMEM((DEVICES, 8, depth), jnp.float32),
        ]
        + semaphores_of(ZS * YS * XS - 1, DEVICES - 1)
        + scatter_scratch(chunks, shapes),
        compiler_params=pltpu.CompilerParams(
            collective_id=ident, has_side_effects=True, vmem_limit_bytes=60 * 2**20
        ),
        name="scatter_last",
    )(*[array for piece in pieces for array in piece], small, matrix)
    return results[:count], results[count], results[count + 1]


QUARTER = HEAD // 4
BLOCK = 256


def turn(values, tables, back):
    cosine, to_left, to_right = tables
    swapped = (
        pltpu.roll(values, LANES - QUARTER, axis=1) * to_left
        + pltpu.roll(values, QUARTER, axis=1) * to_right
    )
    return values * cosine - swapped if back else values * cosine + swapped


def head_lanes(source, at, start, end):
    short = max(start + LANES - end, 0)
    values = source[at, start - short : start - short + LANES]
    return pltpu.roll(values, LANES - short, axis=1) if short else values


def attend_kernel(heads, scale, chunks, matrices, *refs):
    projected, (cos_ref, left_ref, right_ref, hide_ref) = refs[0], refs[1:5]
    shards, refs = refs[5 : 5 + matrices], refs[5 + matrices :]
    out_ref, (query_ref, key_ref, value_ref, logsum_ref) = refs[0], refs[1:5]
    wholes, held, gather_refs = refs[5 : 5 + matrices], refs[5 + matrices], refs[6 + matrices :]
    slots, half_width = cos_ref.shape[0], projected.shape[1] // XS
    per = heads // 2
    blocks = slots // BLOCK
    greet(line_peers())
    start, events, end = gather_plan(chunks, GATHER_SPACING, shards, wholes, *gather_refs)
    start()
    table = table_of(events, GATHER_WEIGHTS, heads * blocks + 1)
    for event in table[0]:
        event()

    def prepare(i, carry):
        at = pl.ds(pl.multiple_of(i * BLOCK, BLOCK), BLOCK)
        tables = cos_ref[at, :], left_ref[at, :], right_ref[at, :]
        hide = hide_ref[at, :]
        lane = lax.broadcasted_iota(jnp.int32, (BLOCK, LANES), 1)
        for head in range(heads):
            half, local = head // per, head % per
            for part, target in enumerate((query_ref, key_ref, value_ref)):
                start = half * half_width + (part * per + local) * HEAD
                values = head_lanes(projected, at, start, XS * half_width)
                if part == 2:
                    values = jnp.where(lane < HEAD, values, 0.0)
                else:
                    values = turn(values, tables, False)
                    values = values + (jnp.where(lane == HEAD, 1.0, 0.0) if part == 0 else hide)
                target[head, at, :] = values.astype(jnp.bfloat16)
        return carry

    lax.fori_loop(0, blocks, prepare, 0)

    def attend(i, carry):
        dispatch(table[1:], i, 0, heads * blocks)
        head, block = i // blocks, i % blocks
        at = pl.ds(pl.multiple_of(block * BLOCK, BLOCK), BLOCK)
        scores = contract(query_ref[head, at, :], key_ref[head], 1, 1)
        highest = jnp.max(scores, 1, keepdims=True)
        exponent = jnp.exp2((scores - highest) * (scale * LOG2E))
        denominator = jnp.sum(exponent, 1, keepdims=True)
        result = jnp.dot(
            exponent.astype(jnp.bfloat16), value_ref[head], preferred_element_type=jnp.float32
        )
        held[head, at, :] = result / denominator
        logsum_ref[head, at, :] = jnp.broadcast_to(
            (highest * scale + jnp.log(denominator)) * LOG2E, (BLOCK, LANES)
        )
        return carry

    lax.fori_loop(0, heads * blocks, attend, 0)
    out_half = out_ref.shape[1] // XS

    def finish(i, carry):
        at = pl.ds(pl.multiple_of(i * BLOCK, BLOCK), BLOCK)
        padding = jnp.zeros((BLOCK, out_half - per * HEAD), jnp.float32)
        for half in range(2):
            pieces = [held[half * per + local, at, :][:, :HEAD] for local in range(per)]
            row = jnp.concatenate(pieces + [padding], 1)
            out_ref[at, half * out_half : (half + 1) * out_half] = row.astype(jnp.bfloat16)
        return carry

    lax.fori_loop(0, blocks, finish, 0)
    end()


def attend(projected, tables, shards, units, out_half, heads, scale, ident):
    slots = projected.shape[0]
    count = len(shards)
    chunks = grouped(count, shards[0].shape[0], units)
    packed = jax.ShapeDtypeStruct((heads, slots, LANES), jnp.bfloat16)
    results = pl.pallas_call(
        partial(attend_kernel, heads, scale, chunks, count),
        out_shape=[
            jax.ShapeDtypeStruct((slots, XS * out_half), jnp.bfloat16),
            packed,
            packed,
            packed,
            jax.ShapeDtypeStruct((heads, slots, LANES), jnp.float32),
        ]
        + [whole_shape(shard) for shard in shards],
        in_specs=[VMEM] * (5 + count),
        out_specs=[VMEM] * 5 + [HBM] * count,
        scratch_shapes=[pltpu.VMEM((heads, slots, LANES), jnp.float32)]
        + gather_scratch(chunks, count),
        compiler_params=pltpu.CompilerParams(
            collective_id=ident, has_side_effects=True, vmem_limit_bytes=60 * 2**20
        ),
        name="attend",
    )(projected, *tables, *shards)
    return results[0], results[1:5], results[5:]


def attend_back_kernel(heads, scale, chunks, matrices, *refs):
    query_ref, key_ref, value_ref, logsum_ref = refs[:4]
    grads, (cos_ref, left_ref, right_ref) = refs[4], refs[5:8]
    pieces, refs = refs[8 : 8 + 4 * matrices], refs[8 + 4 * matrices :]
    out_ref, sums, refs = refs[0], refs[1 : 1 + matrices], refs[1 + matrices :]
    held, grad_q, grad_k, grad_v = refs[:4]
    buffers, semaphores = refs[4 : 4 + 4 * matrices], refs[4 + 4 * matrices :]
    slots, grad_half, out_half = cos_ref.shape[0], grads.shape[1] // XS, out_ref.shape[1] // XS
    per = heads // 2
    blocks = slots // BLOCK
    greet(line_peers())
    events, end = scatter_plan(chunks, SCATTER_SPACING, pieces, sums, buffers, *semaphores)
    table = table_of(events, SCATTER_WEIGHTS, heads * blocks + 1)
    for event in table[0]:
        event()

    def prepare(i, carry):
        at = pl.ds(pl.multiple_of(i * BLOCK, BLOCK), BLOCK)
        for head in range(heads):
            start = head // per * grad_half + head % per * HEAD
            piece = grads[at, start : start + HEAD]
            padding = jnp.zeros((BLOCK, LANES - HEAD), piece.dtype)
            held[head, at, :] = jnp.concatenate([piece, padding], 1)
        return carry

    lax.fori_loop(0, blocks, prepare, 0)

    def attend(i, carry):
        dispatch(table[1:], i, 0, heads * blocks)
        head, block = i // blocks, i % blocks
        at = pl.ds(pl.multiple_of(block * BLOCK, BLOCK), BLOCK)
        query, grad = query_ref[head, at, :], held[head, at, :]
        key = key_ref[head]
        scores = contract(query, key, 1, 1)
        soft = jnp.exp2(scores * (scale * LOG2E) - logsum_ref[head, at, :1])
        grad_soft = contract(grad, value_ref[head], 1, 1)
        value_part = contract(soft.astype(jnp.bfloat16), grad, 0, 0)
        product = soft * grad_soft
        inner = jnp.sum(product, 1, keepdims=True)
        grad_scores = ((product - soft * inner) * scale).astype(jnp.bfloat16)
        grad_q[head, at, :] = jnp.dot(grad_scores, key, preferred_element_type=jnp.float32)
        key_part = contract(grad_scores, query, 0, 0)

        @pl.when(block == 0)
        def _():
            grad_v[head] = value_part
            grad_k[head] = key_part

        @pl.when(block > 0)
        def _():
            grad_v[head] += value_part
            grad_k[head] += key_part

        return carry

    lax.fori_loop(0, heads * blocks, attend, 0)

    def finish(i, carry):
        at = pl.ds(pl.multiple_of(i * BLOCK, BLOCK), BLOCK)
        tables = cos_ref[at, :], left_ref[at, :], right_ref[at, :]
        padding = jnp.zeros((BLOCK, out_half - 3 * per * HEAD), jnp.float32)
        for half in range(2):
            row = []
            for part, source in enumerate((grad_q, grad_k, grad_v)):
                for local in range(per):
                    values = source[half * per + local, at, :]
                    if part < 2:
                        values = turn(values, tables, True)
                    row.append(values[:, :HEAD])
            row = jnp.concatenate(row + [padding], 1)
            out_ref[at, half * out_half : (half + 1) * out_half] = row.astype(jnp.bfloat16)
        return carry

    lax.fori_loop(0, blocks, finish, 0)
    end()


def attend_back(saved, grads, tables, pieces, units, out_half, heads, scale, ident):
    count = len(pieces)
    chunks = scatter_chunks(pieces, units)
    shapes = [sum_shape(piece) for piece in pieces]
    slots = grads.shape[0]
    wide = pltpu.VMEM((heads, slots, LANES), jnp.float32)
    results = pl.pallas_call(
        partial(attend_back_kernel, heads, scale, chunks, count),
        out_shape=[jax.ShapeDtypeStruct((slots, XS * out_half), jnp.bfloat16)]
        + [jax.ShapeDtypeStruct(shape, jnp.float32) for shape in shapes],
        in_specs=[VMEM] * (8 + 4 * count),
        out_specs=[VMEM] * (1 + count),
        scratch_shapes=[pltpu.VMEM((heads, slots, LANES), jnp.bfloat16), wide, wide, wide]
        + scatter_scratch(chunks, shapes),
        compiler_params=pltpu.CompilerParams(
            collective_id=ident, has_side_effects=True, vmem_limit_bytes=63 * 2**20
        ),
        name="attend_back",
    )(*saved, grads, *tables[:3], *[array for piece in pieces for array in piece])
    return results[0], results[1:]


def turn_tables(positions, visible):
    lane = jnp.arange(LANES)
    inside = lane < HEAD
    frequency = rope_base ** (-(lane % QUARTER).astype(jnp.float32) / QUARTER)
    by_row = positions[:, :1].astype(jnp.float32) * frequency
    by_column = positions[:, 1:].astype(jnp.float32) * frequency
    angles = jnp.where(lane < HEAD // 2, by_row, by_column)
    cosine = jnp.where(inside, jnp.cos(angles), 0.0)
    sine = jnp.where(inside, jnp.sin(angles), 0.0)
    leads = lane // QUARTER % 2 == 0
    hide = jnp.where((lane == HEAD) & ~visible[:, None], -1e30, 0.0)
    return cosine, jnp.where(leads, -sine, 0.0), jnp.where(leads, 0.0, sine), hide


def image_device(
    block_input,
    conditioning,
    patch_counts,
    positions,
    w_mod,
    b_mod,
    w_qkv,
    b_qkv,
    w_out,
    b_out,
    w_up,
    b_up,
    w_down,
    b_down,
    cotangent,
):
    own_rows, model_width = block_input.shape
    slot_count = own_rows * CORES
    shard_rows, _, feat = w_qkv.shape
    units = w_up.shape[1]
    heads = CORES * feat // HEAD
    scale = 1.0 / math.sqrt(HEAD)
    images = ZS * YS * XS
    z, y, x, core = place()
    data = z * YS + y
    bf16 = jnp.bfloat16

    def swap(values):
        return lax.ppermute(values, "tensor", CORE_SWAP)

    def both(values):
        return jnp.concatenate([values, swap(values)], 0)

    def own_sum(terms):
        return terms[:own_rows] + swap(terms[own_rows:].astype(bf16)).astype(jnp.float32)

    qkv_width = 3 * feat
    qkv_half, out_half = -(-qkv_width // LANES) * LANES, -(-feat // LANES) * LANES
    qkv_shard = jnp.pad(
        w_qkv.reshape(shard_rows, qkv_width).astype(bf16), ((0, 0), (0, qkv_half - qkv_width))
    )
    out_shard = jnp.pad(w_out.T.astype(bf16), ((0, 0), (0, out_half - feat)))
    shards = [out_shard, w_up.astype(bf16), w_down.T.astype(bf16)]

    depth, lines = -(-shard_rows // LANES) * LANES, 6 * out_half // LANES
    silu_cond = jax.nn.silu(conditioning).astype(bf16).astype(jnp.float32)
    silu_blocks = silu_cond.reshape(XS, ZS * YS, shard_rows).transpose(1, 0, 2)
    silu_blocks = jnp.pad(silu_blocks, ((0, 0), (0, 8 - XS), (0, depth - shard_rows)))
    mod_matrix = jnp.pad(
        w_mod.astype(bf16), ((0, depth - shard_rows), (0, 0), (0, out_half - feat))
    ).reshape(depth, -1)
    mod_bias = jnp.pad(jnp.where(data == 0, b_mod, 0.0), ((0, 0), (0, out_half - feat)))
    whole, silu_in, mod_parts = gather_first(
        qkv_shard, silu_blocks, mod_matrix, mod_bias.reshape(1, -1), 2
    )
    qkv_full = whole.reshape(model_width, -1)
    silu_rows = silu_in[:, :XS, :shard_rows].reshape(images, shard_rows).astype(bf16)
    mod_parts = mod_parts[:, :lines].reshape(XS * CORES, 6, out_half)[:, :, :feat]
    mod = mod_parts.transpose(1, 0, 2).reshape(6, model_width)
    shift_one, scale_one, gate_one, shift_two, scale_two, gate_two = (mod[i] for i in range(6))
    biases = jnp.concatenate([jnp.pad(b_qkv.reshape(-1), (0, qkv_half - qkv_width)), b_up])
    other_biases = lax.ppermute(biases, "tensor", X_SWAP)
    low_biases = jnp.where(x == 0, biases, other_biases)
    high_biases = jnp.where(x == 0, other_biases, biases)
    bias_qkv = jnp.concatenate([low_biases[:qkv_half], high_biases[:qkv_half]])
    bias_up = jnp.concatenate([low_biases[qkv_half:], high_biases[qkv_half:]])

    own_slots = core * own_rows + jnp.arange(own_rows)
    other_slots = (1 - core) * own_rows + jnp.arange(own_rows)
    slots = jnp.concatenate([own_slots, other_slots])
    visible = slots < lax.dynamic_index_in_dim(patch_counts, x, 0, False)
    image_start = x * slot_count
    places = jnp.concatenate(
        [
            lax.dynamic_slice_in_dim(positions, image_start + core * own_rows, own_rows, 0),
            lax.dynamic_slice_in_dim(positions, image_start + (1 - core) * own_rows, own_rows, 0),
        ]
    )
    tables = turn_tables(places, visible)

    normal_one, inverse_one = row_norm(block_input)
    normal_other = row_norm(swap(block_input))[0]
    hidden_one = jnp.concatenate(
        [
            (normal * (1.0 + scale_one) + shift_one).astype(bf16)
            for normal in (normal_one, normal_other)
        ]
    )
    projected = jnp.dot(hidden_one, qkv_full, preferred_element_type=jnp.float32) + bias_qkv
    attended, saved, wholes = attend(
        projected, tables, shards, [48, 16, 16], out_half, heads, scale, 3
    )
    out_full, up_full, down_full = (whole.reshape(model_width, -1) for whole in wholes)
    branch_one = own_sum(contract(attended, out_full, 1, 1)) + b_out
    middle = block_input + gate_one * branch_one
    normal_two, inverse_two = row_norm(middle)
    hidden_two = both((normal_two * (1.0 + scale_two) + shift_two).astype(bf16))
    up_pre = jnp.dot(hidden_two, up_full, preferred_element_type=jnp.float32) + bias_up
    activated = gelu_tanh(up_pre).astype(bf16)

    def norm_back(grad_hidden, normal, inverse, factor):
        grad_normal = grad_hidden * (1.0 + factor)
        mean_plain = jnp.mean(grad_normal, 1, keepdims=True)
        mean_cross = jnp.mean(grad_normal * normal, 1, keepdims=True)
        return inverse[:, None] * (grad_normal - mean_plain - normal * mean_cross)

    def column_sum(values):
        return jnp.sum(values.astype(jnp.float32), 0)

    grad_rows_two = both((cotangent * gate_two).astype(bf16))
    grad_bdown = column_sum(grad_rows_two)
    grad_down = contract(grad_rows_two, activated, 0, 0).astype(bf16)
    sent_down, grad_rows_two = send_off(grad_down, 0, grad_rows_two)
    grad_activated = jnp.dot(grad_rows_two, down_full, preferred_element_type=jnp.float32)
    grad_up = jax.vjp(gelu_tanh, up_pre)[1](grad_activated)[0].astype(bf16)
    grad_bup = column_sum(grad_up)
    grad_wup = contract(hidden_two, grad_up, 0, 0).astype(bf16)
    sent_down, grad_up = arrive_before(sent_down, grad_up)
    sent_up, grad_up = send_off(grad_wup, 1, grad_up)
    hidden_terms = contract(grad_up, up_full, 1, 1)
    other_terms = swap(hidden_terms[own_rows:].astype(bf16))
    other_terms, activated = lax.optimization_barrier((other_terms, activated))
    grad_hidden_two = hidden_terms[:own_rows] + other_terms.astype(jnp.float32)
    branch_two = own_sum(contract(activated, down_full, 1, 1)) + b_down
    block_output = middle + gate_two * branch_two
    grad_gate_two = jnp.sum(cotangent * branch_two, 0)
    grad_shift_two = jnp.sum(grad_hidden_two, 0)
    grad_scale_two = jnp.sum(grad_hidden_two * normal_two, 0)
    grad_middle = cotangent + norm_back(grad_hidden_two, normal_two, inverse_two, scale_two)
    grad_gate_one = jnp.sum(grad_middle * branch_one, 0)
    grad_rows_one = both((grad_middle * gate_one).astype(bf16))
    grad_bout = column_sum(grad_rows_one)
    sent_up, grad_rows_one = arrive_before(sent_up, grad_rows_one)
    grad_out = contract(grad_rows_one, attended, 0, 0).astype(bf16)
    sent_out, grad_rows_one = send_off(grad_out, 1, grad_rows_one)
    grad_attended = jnp.dot(grad_rows_one, out_full, preferred_element_type=jnp.float32)
    grad_projected, (sum_down, sum_up) = attend_back(
        saved,
        grad_attended.astype(bf16),
        tables,
        [settle(sent_down), settle(sent_up)],
        [16, 16],
        qkv_half,
        heads,
        scale,
        6,
    )
    grad_qkv = contract(hidden_one, grad_projected, 0, 0).astype(bf16)
    sent_qkv, grad_projected = send_off(grad_qkv, 0, grad_projected)
    bias_terms = column_sum(grad_projected).reshape(2, qkv_half)
    grad_hidden_one = own_sum(contract(grad_projected, qkv_full, 1, 1))
    grad_shift_one = jnp.sum(grad_hidden_one, 0)
    grad_scale_one = jnp.sum(grad_hidden_one * normal_one, 0)
    grad_input = grad_middle + norm_back(grad_hidden_one, normal_one, inverse_one, scale_one)

    grad_mod = jnp.stack(
        [
            grad_shift_one,
            grad_scale_one,
            grad_gate_one,
            grad_shift_two,
            grad_scale_two,
            grad_gate_two,
        ]
    )
    grad_mod = (grad_mod + swap(grad_mod)).astype(bf16).astype(jnp.float32)
    grad_mod = grad_mod.reshape(6, XS, CORES, feat)
    grad_mod = lax.dynamic_index_in_dim(grad_mod, core, 2, False)
    grad_mod = jnp.pad(grad_mod, ((0, 0), (0, 0), (0, out_half - feat)))
    small = qkv_half + units + 2 * model_width
    rest = -(-(lines * LANES + small) // (8 * LANES)) * 8 * LANES - lines * LANES - small
    sends = []
    for half in range(2):
        flat = jnp.concatenate(
            [
                grad_mod[:, half].reshape(-1),
                bias_terms[half],
                grad_bup[half * units : (half + 1) * units],
                grad_bout,
                grad_bdown,
                jnp.zeros(rest, jnp.float32),
            ]
        )
        sends.append(flat.reshape(-1, LANES))
    (sum_out, sum_qkv), small_all, silu_sum = scatter_last(
        [settle(sent_out), settle(sent_qkv)], [48, 16], jnp.stack(sends), mod_matrix, lines, 7
    )
    grad_wqkv = sum_qkv[:, :qkv_width].reshape(shard_rows, 3, feat)
    grad_wout = sum_out[:, :feat].T
    grad_wdown = sum_down.T
    summed = jnp.sum(small_all, 0)
    grad_bmod = summed[:lines].reshape(6, out_half)[:, :feat]
    summed = summed[lines:].reshape(-1)
    grad_bqkv = summed[:qkv_width].reshape(3, feat)
    grad_bup = summed[qkv_half : qkv_half + units]
    offset = qkv_half + units
    grad_bout = summed[offset : offset + model_width]
    grad_bdown = summed[offset + model_width : offset + 2 * model_width]
    mod_all = small_all[:, :lines].reshape(images, 6, out_half)[:, :, :feat]
    mod_all = mod_all.reshape(images, 6 * feat).astype(bf16)
    grad_wmod = contract(silu_rows, mod_all, 0, 0).reshape(shard_rows, 6, feat)
    grad_silu = silu_sum[:, :XS, :shard_rows].transpose(1, 0, 2).reshape(XS, model_width)
    grad_cond = jax.vjp(jax.nn.silu, conditioning)[1](grad_silu)[0]
    return (
        block_output,
        grad_input,
        grad_cond,
        grad_wmod,
        grad_bmod,
        grad_wqkv,
        grad_bqkv,
        grad_wout,
        grad_bout,
        sum_up,
        grad_bup,
        grad_wdown,
        grad_bdown,
    )

def solution(mesh):
    body = image_device if image_per_chip(mesh) else per_device
    placed = (
        P(("dp", "tensor"), None),
        P("dp", None),
        P("dp"),
        P("dp", None),
        P("dp", None, "tensor"),
        P(None, "tensor"),
        P("dp", None, "tensor"),
        P(None, "tensor"),
        P("tensor", "dp"),
        P(),
        P("dp", "tensor"),
        P("tensor"),
        P("tensor", "dp"),
        P(),
        P(("dp", "tensor"), None),
    )
    return jax.shard_map(
        body,
        mesh=mesh,
        in_specs=placed,
        out_specs=(
            P(("dp", "tensor"), None),
            P(("dp", "tensor"), None),
            P("dp", None),
            P("dp", None, "tensor"),
            P(None, "tensor"),
            P("dp", None, "tensor"),
            P(None, "tensor"),
            P("tensor", "dp"),
            P(),
            P("dp", "tensor"),
            P("tensor"),
            P("tensor", "dp"),
            P(),
        ),
        check_vma=False,
    )
```

```python
from functools import partial
import math

import jax
import jax.numpy as jnp
from jax import lax
from jax.experimental import pallas as pl
from jax.experimental.pallas import tpu as pltpu
from jax.sharding import PartitionSpec as P

HEAD = 72


epsilon = 1e-06
rope_base = 10000.0
gelu_coeff = 0.044715
root_two_pi = math.sqrt(2.0 / math.pi)


def gelu_tanh(values):
    return (
        0.5
        * values
        * (1.0 + jnp.tanh(root_two_pi * (values + gelu_coeff * values * values * values)))
    )


def rotate(values, positions, direction):
    quarter = values.shape[-1] // 4
    frequency = rope_base ** (-jnp.arange(quarter, dtype=jnp.float32) / quarter)
    pieces = []
    for column in range(2):
        angles = positions[:, column].astype(jnp.float32)[:, None, None] * frequency
        cosine = jnp.cos(angles)
        sine_term = direction * jnp.sin(angles)
        leading = values[..., 2 * column * quarter : (2 * column + 1) * quarter]
        trailing = values[..., (2 * column + 1) * quarter : (2 * column + 2) * quarter]
        pieces.append(leading * cosine - trailing * sine_term)
        pieces.append(leading * sine_term + trailing * cosine)
    return jnp.concatenate(pieces, -1)


def contract(left, right, left_dim, right_dim):
    return lax.dot_general(
        left, right, (((left_dim,), (right_dim,)), ((), ())), preferred_element_type=jnp.float32
    )


def exact_dot(left, right):
    return jnp.dot(left, right, precision=lax.Precision.HIGHEST, preferred_element_type=jnp.float32)


def row_norm(rows):
    average = jnp.mean(rows, 1)
    inverse = lax.rsqrt(jnp.mean(rows * rows, 1) - average * average + epsilon)
    return ((rows - average[:, None]) * inverse[:, None], inverse)


def masked_scores(query_rows, key_rows, patch_count, factor):
    raw_scores = (
        jnp.einsum("qhd,khd->hqk", query_rows, key_rows, preferred_element_type=jnp.float32)
        * factor
    )
    visible = jnp.arange(key_rows.shape[0]) < patch_count
    return jnp.where(visible[None, None, :], raw_scores, -1e30)


def attend_forward(factor, inputs):
    query_rows, key_rows, value_rows, patch_count = inputs
    scores = masked_scores(query_rows, key_rows, patch_count, factor)
    highest = jnp.max(scores, -1, keepdims=True)
    exponent = jnp.exp(scores - highest)
    denominator = jnp.sum(exponent, -1, keepdims=True)
    softmax_rows = (exponent / denominator).astype(jnp.bfloat16)
    attended = jnp.einsum(
        "hqk,khd->qhd", softmax_rows, value_rows, preferred_element_type=jnp.float32
    )
    return (attended, (highest + jnp.log(denominator))[..., 0])


def attend_backward(factor, inputs):
    query_rows, key_rows, value_rows, patch_count, logsum, grad_rows = inputs
    scores = masked_scores(query_rows, key_rows, patch_count, factor)
    softmax_rows = jnp.exp(scores - logsum[..., None])
    grad_soft = jnp.einsum(
        "qhd,khd->hqk", grad_rows, value_rows, preferred_element_type=jnp.float32
    )
    grad_values = jnp.einsum(
        "hqk,qhd->khd",
        softmax_rows.astype(jnp.bfloat16),
        grad_rows,
        preferred_element_type=jnp.float32,
    )
    inner_sum = jnp.sum(softmax_rows * grad_soft, -1, keepdims=True)
    grad_scores = (softmax_rows * (grad_soft - inner_sum) * factor).astype(jnp.bfloat16)
    grad_query = jnp.einsum(
        "hqk,khd->qhd", grad_scores, key_rows, preferred_element_type=jnp.float32
    )
    grad_keys = jnp.einsum(
        "hqk,qhd->khd", grad_scores, query_rows, preferred_element_type=jnp.float32
    )
    return (grad_query, grad_keys, grad_values)


def per_device(
    block_input,
    conditioning,
    patch_counts,
    positions,
    w_mod,
    b_mod,
    w_qkv,
    b_qkv,
    w_out,
    b_out,
    w_up,
    b_up,
    w_down,
    b_down,
    cotangent,
):
    own_rows, model_width = block_input.shape
    group_rows = positions.shape[0]
    images_local = conditioning.shape[0]
    slot_count = group_rows // images_local
    feat_local = w_qkv.shape[2]
    heads_local = feat_local // HEAD
    row_start = lax.axis_index("tensor") * own_rows
    factor = 1.0 / math.sqrt(HEAD)
    image_of = (row_start + jnp.arange(own_rows)) // slot_count
    one_hot = (image_of[:, None] == jnp.arange(images_local)[None, :]).astype(jnp.float32)

    def to_rows(vectors):
        return exact_dot(one_hot, vectors)

    def to_images(values):
        return exact_dot(one_hot.T, values)

    def per_image(stacked):
        return stacked.reshape((images_local, slot_count) + stacked.shape[1:])

    def modulate_group(values, shift, scale):
        shaped = values.reshape(images_local, slot_count, values.shape[1])
        return (shaped * (1.0 + scale[:, None, :]) + shift[:, None, :]).reshape(values.shape)

    mod_full, qkv_full, out_full, up_full, down_full = (
        lax.all_gather(w_mod.astype(jnp.bfloat16), "dp", axis=0, tiled=True),
        lax.all_gather(w_qkv.astype(jnp.bfloat16), "dp", axis=0, tiled=True),
        lax.all_gather(w_out.astype(jnp.bfloat16), "dp", axis=1, tiled=True),
        lax.all_gather(w_up.astype(jnp.bfloat16), "dp", axis=0, tiled=True),
        lax.all_gather(w_down.astype(jnp.bfloat16), "dp", axis=1, tiled=True),
    )
    silu_cond = jax.nn.silu(conditioning).astype(jnp.bfloat16)
    mod_cols = jnp.dot(
        silu_cond, mod_full.reshape(model_width, 6 * feat_local), preferred_element_type=jnp.float32
    )
    mod_cols = mod_cols.reshape(images_local, 6, feat_local) + b_mod
    mod_all = lax.all_gather(mod_cols, "tensor", axis=2, tiled=True)

    def norm_gather(rows_local, shift, scale):
        rows_group = lax.all_gather(rows_local, "tensor", axis=0, tiled=True)
        normal_group, inverse_group = row_norm(rows_group)
        hidden = modulate_group(normal_group, shift, scale).astype(jnp.bfloat16)
        normal = lax.dynamic_slice_in_dim(normal_group, row_start, own_rows, 0)
        inverse = lax.dynamic_slice_in_dim(inverse_group, row_start, own_rows, 0)
        return (hidden, normal, inverse)

    hidden_one, normal_one, inverse_one = norm_gather(block_input, mod_all[:, 0], mod_all[:, 1])
    projected = jnp.dot(
        hidden_one,
        qkv_full.reshape(model_width, 3 * feat_local),
        preferred_element_type=jnp.float32,
    ) + b_qkv.reshape(-1)
    projected = projected.reshape(group_rows, 3, heads_local, HEAD)
    query_rows = rotate(projected[:, 0], positions, 1.0).astype(jnp.bfloat16)
    key_rows = rotate(projected[:, 1], positions, 1.0).astype(jnp.bfloat16)
    value_rows = projected[:, 2].astype(jnp.bfloat16)
    attended, logsum = lax.map(
        partial(attend_forward, factor),
        (per_image(query_rows), per_image(key_rows), per_image(value_rows), patch_counts),
    )
    attended = attended.reshape(group_rows, feat_local).astype(jnp.bfloat16)

    def branch_sum(partial_terms, offset):
        return lax.psum_scatter(partial_terms, "tensor", scatter_dimension=0, tiled=True) + offset

    gate_one_rows = to_rows(mod_all[:, 2])
    gate_two_rows = to_rows(mod_all[:, 5])
    branch_one = branch_sum(jnp.dot(attended, out_full, preferred_element_type=jnp.float32), b_out)
    middle = block_input + gate_one_rows * branch_one
    hidden_two, normal_two, inverse_two = norm_gather(middle, mod_all[:, 3], mod_all[:, 4])
    up_pre = jnp.dot(hidden_two, up_full, preferred_element_type=jnp.float32) + b_up
    activated = gelu_tanh(up_pre).astype(jnp.bfloat16)
    branch_two = branch_sum(
        jnp.dot(activated, down_full, preferred_element_type=jnp.float32), b_down
    )
    block_output = middle + gate_two_rows * branch_two
    mod_back, qkv_back, out_back, up_back, down_back = (
        lax.all_gather(w_mod.astype(jnp.bfloat16), "dp", axis=0, tiled=True),
        lax.all_gather(w_qkv.astype(jnp.bfloat16), "dp", axis=0, tiled=True),
        lax.all_gather(w_out.astype(jnp.bfloat16), "dp", axis=1, tiled=True),
        lax.all_gather(w_up.astype(jnp.bfloat16), "dp", axis=0, tiled=True),
        lax.all_gather(w_down.astype(jnp.bfloat16), "dp", axis=1, tiled=True),
    )

    def spread_grad(grad_branch):
        return lax.all_gather(grad_branch, "tensor", axis=0, tiled=True)

    def input_sum(partial_terms):
        return lax.psum_scatter(partial_terms, "tensor", scatter_dimension=0, tiled=True)

    def norm_backward(grad_hidden, normal, inverse, scale):
        grad_normal = grad_hidden * (1.0 + to_rows(scale))
        mean_plain = jnp.mean(grad_normal, 1, keepdims=True)
        mean_cross = jnp.mean(grad_normal * normal, 1, keepdims=True)
        return inverse[:, None] * (grad_normal - mean_plain - normal * mean_cross)

    grad_gate_two = to_images(cotangent * branch_two)
    grad_branch_two = (cotangent * gate_two_rows).astype(jnp.bfloat16)
    grad_rows_two = spread_grad(grad_branch_two)
    grad_bdown_local = jnp.sum(grad_rows_two.astype(jnp.float32), 0)
    grad_wdown_local = contract(activated, grad_rows_two, 0, 0)
    grad_activated = contract(grad_rows_two, down_back, 1, 1)
    gelu_pull = jax.vjp(gelu_tanh, up_pre)[1]
    grad_up = gelu_pull(grad_activated)[0].astype(jnp.bfloat16)
    grad_bup_local = jnp.sum(grad_up.astype(jnp.float32), 0)
    grad_wup_local = contract(hidden_two, grad_up, 0, 0)
    grad_hidden_two = input_sum(contract(grad_up, up_back, 1, 1))
    grad_shift_two = to_images(grad_hidden_two)
    grad_scale_two = to_images(grad_hidden_two * normal_two)
    grad_middle = cotangent + norm_backward(grad_hidden_two, normal_two, inverse_two, mod_all[:, 4])
    grad_gate_one = to_images(grad_middle * branch_one)
    grad_branch_one = (grad_middle * gate_one_rows).astype(jnp.bfloat16)
    grad_rows_one = spread_grad(grad_branch_one)
    grad_bout_local = jnp.sum(grad_rows_one.astype(jnp.float32), 0)
    grad_wout_local = contract(attended, grad_rows_one, 0, 0)
    grad_attended = contract(grad_rows_one, out_back, 1, 1).astype(jnp.bfloat16)
    grad_attended = grad_attended.reshape(group_rows, heads_local, HEAD)
    grad_query, grad_keys, grad_values = lax.map(
        partial(attend_backward, factor),
        (
            per_image(query_rows),
            per_image(key_rows),
            per_image(value_rows),
            patch_counts,
            logsum,
            per_image(grad_attended),
        ),
    )
    head_shape = (group_rows, heads_local, HEAD)
    grad_projected = jnp.stack(
        [
            rotate(grad_query.reshape(head_shape), positions, -1.0),
            rotate(grad_keys.reshape(head_shape), positions, -1.0),
            grad_values.reshape(head_shape),
        ],
        1,
    )
    grad_projected = grad_projected.astype(jnp.bfloat16).reshape(group_rows, 3 * feat_local)
    grad_bqkv_local = jnp.sum(grad_projected.astype(jnp.float32), 0).reshape(3, feat_local)
    grad_wqkv_local = contract(hidden_one, grad_projected, 0, 0).reshape(model_width, 3, feat_local)
    grad_hidden_one = input_sum(
        contract(grad_projected, qkv_back.reshape(model_width, 3 * feat_local), 1, 1)
    )
    grad_shift_one = to_images(grad_hidden_one)
    grad_scale_one = to_images(grad_hidden_one * normal_one)
    grad_input = grad_middle + norm_backward(
        grad_hidden_one, normal_one, inverse_one, mod_all[:, 1]
    )
    grad_mod_part = jnp.stack(
        [
            grad_shift_one,
            grad_scale_one,
            grad_gate_one,
            grad_shift_two,
            grad_scale_two,
            grad_gate_two,
        ],
        1,
    )
    grad_mod = lax.psum_scatter(grad_mod_part, "tensor", scatter_dimension=2, tiled=True).astype(
        jnp.bfloat16
    )
    grad_bmod_local = jnp.sum(grad_mod.astype(jnp.float32), 0)
    grad_mod_flat = grad_mod.reshape(images_local, 6 * feat_local)
    grad_wmod_local = contract(silu_cond, grad_mod_flat, 0, 0).reshape(model_width, 6, feat_local)
    grad_silu = lax.psum(
        contract(grad_mod_flat, mod_back.reshape(model_width, 6 * feat_local), 1, 1), "tensor"
    )
    silu_pull = jax.vjp(jax.nn.silu, conditioning)[1]
    grad_cond = silu_pull(grad_silu)[0]
    grad_wmod, grad_wqkv, grad_wout, grad_wup, grad_wdown = (
        lax.psum_scatter(
            grad_wmod_local.astype(jnp.bfloat16), "dp", scatter_dimension=0, tiled=True
        ).astype(jnp.float32),
        lax.psum_scatter(
            grad_wqkv_local.astype(jnp.bfloat16), "dp", scatter_dimension=0, tiled=True
        ).astype(jnp.float32),
        lax.psum_scatter(
            grad_wout_local.astype(jnp.bfloat16), "dp", scatter_dimension=1, tiled=True
        ).astype(jnp.float32),
        lax.psum_scatter(
            grad_wup_local.astype(jnp.bfloat16), "dp", scatter_dimension=0, tiled=True
        ).astype(jnp.float32),
        lax.psum_scatter(
            grad_wdown_local.astype(jnp.bfloat16), "dp", scatter_dimension=1, tiled=True
        ).astype(jnp.float32),
    )
    grad_bmod, grad_bqkv, grad_bout, grad_bup, grad_bdown = lax.psum(
        (grad_bmod_local, grad_bqkv_local, grad_bout_local, grad_bup_local, grad_bdown_local), "dp"
    )
    return (
        block_output,
        grad_input,
        grad_cond,
        grad_wmod,
        grad_bmod,
        grad_wqkv,
        grad_bqkv,
        grad_wout,
        grad_bout,
        grad_wup,
        grad_bup,
        grad_wdown,
        grad_bdown,
    )


LANES = 128
ZS, YS, XS, CORES = 4, 2, 2, 2
MESH_ID = pl.DeviceIdType.MESH
CORE_SWAP = [(0, 1), (1, 0), (2, 3), (3, 2)]
X_SWAP = [(0, 2), (2, 0), (1, 3), (3, 1)]
Y_SWAP = [(i, i ^ 1) for i in range(ZS * YS)]
LOG2E = 1.0 / math.log(2.0)
HBM = pl.BlockSpec(memory_space=pl.ANY)
VMEM = pl.BlockSpec(memory_space=pltpu.VMEM)


def image_per_chip(mesh):
    return dict(mesh.shape) == {"dp": ZS * YS, "tensor": XS * CORES}


def place():
    data, tensor = lax.axis_index("dp"), lax.axis_index("tensor")
    return data // YS, data % YS, tensor // CORES, tensor % CORES


def flip_z(z, step):
    high, low = z // 2, z % 2
    if step & 2:
        high = 1 - high
    if step & 1:
        low = 1 - low
    return high * 2 + low


def device(z, y, x, core):
    return (z * YS + y, x * CORES + core)


def greet(targets):
    barrier = pltpu.get_barrier_semaphore()
    for target in targets:
        pl.semaphore_signal(barrier, inc=1, device_id=target, device_id_type=MESH_ID)
    pl.semaphore_wait(barrier, len(targets))


GATHER_STEPS, SCATTER_STEPS = 5, 5
GATHER_SPACING, SCATTER_SPACING = 8.0, 8.0
GATHER_WEIGHTS, SCATTER_WEIGHTS = (1, 1, 1, 1, 1), (1, 1, 1, 1, 1)


def grouped(matrices, rows, units):
    chunks = []
    for matrix in range(matrices):
        unit = units[matrix]
        for number, row in enumerate(range(0, rows, 3 * unit)):
            short = (matrix + number) % 2
            chunks.append((matrix, row, unit, 2))
            chunks.append((matrix, row + unit, unit, 3))
            chunks.append((matrix, row + 2 * unit, unit, short))
    return chunks


def two_hops(matrix, rows):
    split = y_rows(rows)
    return [(matrix, row, 16, 4 if row < split else 5) for row in range(0, rows, 16)]


def y_rows(rows):
    return rows - rows // 32 * 16


def in_order(count, steps, spacing, act):
    events = sorted((c + s * spacing, c, s) for c in range(count) for s in range(steps))
    return [(s, partial(act, c, s)) for time, c, s in events]


def run_all(events):
    for _, event in events:
        event()


def table_of(events, weights, trips):
    total = sum(weights[step] for step, _ in events)
    table, sent = [[] for _ in range(trips)], 0
    for step, event in events:
        table[min(sent * trips // total, trips - 1)].append(event)
        sent += weights[step]
    return table


def dispatch(table, index, low, high):
    if not any(table[low:high]):
        return
    if high - low == 1:
        for event in table[low]:
            event()
        return
    middle = (low + high) // 2
    pl.when(index < middle)(lambda: dispatch(table, index, low, middle))
    pl.when(index >= middle)(lambda: dispatch(table, index, middle, high))


def gather_plan(chunks, spacing, shards, wholes, sends, recvs, local):
    z, y, x, core = place()
    inner = jnp.logical_or(z == 1, z == 2)
    every = slice(None)

    def mine_of(matrix):
        width = shards[matrix].shape[1]
        return pl.ds(pl.multiple_of(x * width, LANES), width)

    at_x, at_y = device(z, y, 1 - x, core), device(z, 1 - y, x, core)
    beside, mirror = device(flip_z(z, 1), y, x, core), device(3 - z, y, x, core)
    pair = pl.ds(z // 2 * 2, 2)
    far = pl.ds(2 - z // 2 * 2, 2)

    def copy(number, send, recv, source, target, where):
        return pltpu.make_async_remote_copy(
            src_ref=source,
            dst_ref=target,
            send_sem=sends.at[number * 5 + send],
            recv_sem=recvs.at[number * 4 + recv],
            device_id=where,
            device_id_type=MESH_ID,
        )

    def moves(number):
        matrix, row, rows, route = chunks[number]
        complete, route = route < 4, route % 4
        whole, span, mine = wholes[matrix], pl.ds(row, rows), mine_of(matrix)
        own, shard = whole.at[z, y, span, mine], shards[matrix].at[span, :]
        lines, columns = (every if route == 3 else y), (every if route == 2 else mine)
        made = {}
        near = shard if route < 2 else whole.at[z, lines, span, columns]
        near_to = own if route < 2 else near
        made["near"] = partial(copy, number, 0, 0, near, near_to, beside)
        both = whole.at[pair, lines, span, columns]
        made["mirror"] = partial(copy, number, 1, 1, both, both, mirror)
        there = whole.at[far, lines, span, columns]
        made["forward"] = partial(copy, number, 2, 1, there, there, beside)
        if route < 2:
            column = whole.at[:, y, span, mine]
            made["second"] = partial(copy, number, 3, 2, column, column, at_x if route == 0 else at_y)
        else:
            made["first"] = partial(copy, number, 3, 2, shard, own, at_x if route == 2 else at_y)
        if route in (0, 2):
            last = whole.at[:, y, span, :]
        else:
            last = whole.at[:, :, span, mine]
        if complete:
            where = at_y if route in (0, 2) else at_x
            made["third"] = partial(copy, number, 4, 3, last, last, where)
        return made

    def keep(matrix):
        return pltpu.make_async_copy(
            shards[matrix], wholes[matrix].at[z, y, :, mine_of(matrix)], local.at[matrix]
        )

    kept = []

    def ready(number):
        matrix = chunks[number][0]
        if matrix not in kept:
            kept.append(matrix)
            keep(matrix).wait()

    def act(number, step):
        made = moves(number)
        straight = chunks[number][3] % 4 < 2
        if step == 0:
            made["near" if straight else "first"]().start()
        elif step == 1:
            ready(number)
            if straight:
                made["near"]().wait_recv()
                pl.when(inner)(lambda: made["mirror"]().start())
            else:
                made["first"]().wait_recv()
                made["near"]().start()
        elif step == 2:
            if straight:
                made["mirror"]().wait_recv()
                pl.when(inner)(lambda: made["forward"]().start())
                made["second"]().start()
            else:
                made["near"]().wait_recv()
                pl.when(inner)(lambda: made["mirror"]().start())
        elif step == 3:
            if straight:
                made["second"]().wait_recv()
            else:
                made["mirror"]().wait_recv()
                pl.when(inner)(lambda: made["forward"]().start())
            if "third" in made:
                made["third"]().start()
        elif "third" in made:
            made["third"]().wait_recv()

    def start():
        for matrix in sorted({chunk[0] for chunk in chunks}):
            keep(matrix).start()

    def finish():
        for number in range(len(chunks)):
            made = moves(number)
            for name in made:
                if name not in ("mirror", "forward"):
                    made[name]().wait_send()

            def rest(made=made):
                made["mirror"]().wait_send()
                made["forward"]().wait_send()

            pl.when(inner)(rest)

    return start, in_order(len(chunks), GATHER_STEPS, spacing, act), finish


def gather_scratch(chunks, matrices):
    count = len(chunks)
    return [
        pltpu.SemaphoreType.DMA((count * 5,)),
        pltpu.SemaphoreType.DMA((count * 4,)),
        pltpu.SemaphoreType.DMA((matrices,)),
    ]


def send_off(part, flip, after):
    z, y, x, core = place()
    rows, width = part.shape[0] // (ZS * YS), part.shape[1] // XS
    blocks = part.reshape(ZS, YS, rows, XS * width)
    split = rows // 32 * 16
    split = split if flip else rows - split
    by_y, by_x = blocks[:, :, :split], blocks[:, :, split:]
    low, high = by_x[..., :width], by_x[..., width:]
    send_y = lax.dynamic_index_in_dim(by_y, 1 - y, 1, False)
    keep_y = lax.dynamic_index_in_dim(by_y, y, 1, False)
    send_x, keep_x = jnp.where(x == 0, high, low), jnp.where(x == 0, low, high)
    send_y, send_x, after = lax.optimization_barrier((send_y, send_x, after))
    got_y = lax.ppermute(send_y, "dp", Y_SWAP)
    got_x = lax.ppermute(send_x, "tensor", X_SWAP)
    return (keep_y, got_y, keep_x, got_x), after


def arrive_before(sent, after):
    keep_y, got_y, keep_x, got_x = sent
    got_y, got_x, after = lax.optimization_barrier((got_y, got_x, after))
    return (keep_y, got_y, keep_x, got_x), after


def settle(sent):
    z, y, x, core = place()
    keep_y, got_y, keep_x, got_x = sent
    sum_y = (keep_y.astype(jnp.float32) + got_y.astype(jnp.float32)).astype(jnp.bfloat16)
    sum_x = (keep_x.astype(jnp.float32) + got_x.astype(jnp.float32)).astype(jnp.bfloat16)
    width = sum_x.shape[-1]
    low, high = sum_y[..., :width], sum_y[..., width:]
    return [
        jnp.where(x == 0, low, high),
        jnp.where(x == 0, high, low),
        lax.dynamic_index_in_dim(sum_x, y, 1, False),
        lax.dynamic_index_in_dim(sum_x, 1 - y, 1, False),
    ]


def scatter_chunks(pieces, units):
    chunks = []
    for matrix, unit in enumerate(units):
        parts, start = [], 0
        for side in range(2):
            rows = pieces[matrix][2 * side].shape[1]
            parts.append(
                [(matrix, side, row, start + row, min(unit, rows - row)) for row in range(0, rows, unit)]
            )
            start += rows
        for i in range(max(len(part) for part in parts)):
            chunks.extend(part[i] for part in parts if i < len(part))
    return chunks


def scatter_plan(chunks, spacing, pieces, sums, buffers, sends, recvs):
    z, y, x, core = place()
    inner = jnp.logical_or(z == 1, z == 2)
    outer = jnp.logical_or(z == 0, z == 3)
    at_x, at_y = device(z, y, 1 - x, core), device(z, 1 - y, x, core)
    z_near = flip_z(z, 1)
    beside, mirror = device(z_near, y, x, core), device(3 - z, y, x, core)
    pair_at, far_at = z // 2 * 2, 2 - z // 2 * 2
    far = pl.ds(far_at, 2)

    def copy(number, index, source, target, where):
        return pltpu.make_async_remote_copy(
            src_ref=source,
            dst_ref=target,
            send_sem=sends.at[number * 4 + index],
            recv_sem=recvs.at[number * 4 + index],
            device_id=where,
            device_id_type=MESH_ID,
        )

    def moves(number):
        matrix, side, row, at, rows = chunks[number]
        here, span = pl.ds(row, rows), pl.ds(at, rows)
        arrived, outer_in, mirror_in, near_in = buffers[4 * matrix : 4 * matrix + 4]
        give, two = pieces[4 * matrix + 2 * side + 1], arrived.at[far, span, :]
        return {
            "first": partial(
                copy,
                number,
                0,
                give.at[:, here, :],
                arrived.at[:, span, :],
                at_y if side else at_x,
            ),
            "outer": partial(copy, number, 1, two, outer_in.at[:, span, :], beside),
            "mirror": partial(copy, number, 2, two, mirror_in.at[:, span, :], mirror),
            "near": partial(
                copy, number, 3, arrived.at[z_near, span, :], near_in.at[span, :], beside
            ),
        }

    def add(number, count, base, source, from_row):
        matrix, side, row, at, rows = chunks[number]
        arrived, tiles = buffers[4 * matrix], rows // 16

        def one(i, carry):
            block, line = i // tiles, i % tiles
            to = pl.ds(pl.multiple_of(at + line * 16, 16), 16)
            origin = pl.ds(pl.multiple_of(from_row + line * 16, 16), 16)
            held = arrived[base + block, to, :].astype(jnp.float32)
            arrived[base + block, to, :] = (
                held + source[block, origin, :].astype(jnp.float32)
            ).astype(jnp.bfloat16)
            return carry

        lax.fori_loop(0, count * tiles, one, 0)

    def finalize(number):
        matrix, side, row, at, rows = chunks[number]
        arrived, near_in = buffers[4 * matrix], buffers[4 * matrix + 3]

        def one(i, carry):
            to = pl.ds(pl.multiple_of(at + i * 16, 16), 16)
            sums[matrix][to, :] = arrived[z, to, :].astype(jnp.float32) + near_in[to, :].astype(
                jnp.float32
            )
            return carry

        lax.fori_loop(0, rows // 16, one, 0)

    def act(number, step):
        matrix, side, row, at, rows = chunks[number]
        made = moves(number)
        stay = pieces[4 * matrix + 2 * side]
        arrived, outer_in, mirror_in, near_in = buffers[4 * matrix : 4 * matrix + 4]

        def from_outer():
            made["outer"]().wait_recv()
            add(number, 2, far_at, outer_in, at)
            made["mirror"]().start()

        def from_mirror():
            made["mirror"]().wait_recv()
            add(number, 2, pair_at, mirror_in, at)

        if step == 0:
            made["first"]().start()
        elif step == 1:
            made["first"]().wait_recv()
            add(number, ZS, 0, stay, row)
            pl.when(outer)(lambda: made["outer"]().start())
        elif step == 2:
            pl.when(inner)(from_outer)
        elif step == 3:
            pl.when(inner)(from_mirror)
            made["near"]().start()
        else:
            made["near"]().wait_recv()
            finalize(number)

    def finish():
        for number in range(len(chunks)):
            made = moves(number)
            made["first"]().wait_send()
            made["near"]().wait_send()
            pl.when(outer)(lambda made=made: made["outer"]().wait_send())
            pl.when(inner)(lambda made=made: made["mirror"]().wait_send())

    return in_order(len(chunks), SCATTER_STEPS, spacing, act), finish


def scatter_scratch(chunks, shapes):
    wide = []
    for rows, width in shapes:
        for lead in ((ZS,), (2,), (2,), ()):
            wide.append(pltpu.VMEM((*lead, rows, width), jnp.bfloat16))
    count = len(chunks) * 4
    return wide + [pltpu.SemaphoreType.DMA((count,)), pltpu.SemaphoreType.DMA((count,))]


def sum_shape(piece):
    rows = piece[0].shape[1] + piece[2].shape[1]
    return rows, piece[0].shape[2]


def line_peers():
    z, y, x, core = place()
    return [
        device(z, y, 1 - x, core),
        device(z, 1 - y, x, core),
        device(flip_z(z, 1), y, x, core),
        device(3 - z, y, x, core),
    ]


DEVICES = ZS * YS * XS * CORES


def numbers():
    z, y, x, core = place()
    data = z * YS + y
    return (data * XS + x) * CORES + core, data, data * XS + x


def device_at(number):
    return (number // (XS * CORES), number % (XS * CORES))


def greet_all():
    me = numbers()[0]
    greet([device_at((me + step) % DEVICES) for step in range(1, DEVICES)])


def send_each(count, me, source_of, arrived, device_of, sends, recvs):
    copies = []
    for step in range(1, count):
        target = (me + step) % count
        copy = pltpu.make_async_remote_copy(
            src_ref=source_of(target),
            dst_ref=arrived.at[me],
            send_sem=sends.at[step - 1],
            recv_sem=recvs.at[step - 1],
            device_id=device_of(target),
            device_id_type=MESH_ID,
        )
        copy.start()
        copies.append(copy)
    return copies


def receive(copies):
    for copy in copies:
        copy.wait_recv()


def semaphores_of(*counts):
    return [pltpu.SemaphoreType.DMA((count,)) for count in counts for _ in range(2)]


def gather_kernel(chunks, *refs):
    shard, silu_blocks, matrix_ref, bias_ref = refs[:4]
    whole, silu_in, mod_ref = refs[4:7]
    parts, mod_in, silu_sends, silu_recvs, mod_sends, mod_recvs = refs[7:13]
    me, data, _ = numbers()
    z, y, x, core = place()
    greet_all()
    silu_copies = send_each(
        ZS * YS,
        data,
        lambda target: silu_blocks.at[target],
        silu_in,
        lambda target: (target, lax.axis_index("tensor")),
        silu_sends,
        silu_recvs,
    )
    start, events, finish = gather_plan(chunks, GATHER_SPACING, [shard], [whole], *refs[13:])
    start()
    early = len(chunks) // 2
    run_all(events[:early])
    silu_in[data] = silu_blocks[data]
    receive(silu_copies)
    rows = silu_in[...].reshape(silu_in.shape[0] * silu_in.shape[1], silu_in.shape[2])
    product = jnp.dot(
        rows.astype(jnp.bfloat16), matrix_ref[...], preferred_element_type=jnp.float32
    )
    product = product + bias_ref[...]
    lines = product.shape[1] // LANES
    for line in range(lines):
        piece = product[:, line * LANES : (line + 1) * LANES]
        parts[:, :, line, :] = piece.reshape(parts.shape[0], parts.shape[1], LANES)
    for line in range(lines, parts.shape[2]):
        parts[:, :, line, :] = jnp.zeros((parts.shape[0], parts.shape[1], LANES), jnp.float32)
    run_all(events[early : 2 * early])
    mod_copies = send_each(
        DEVICES,
        me,
        lambda target: parts.at[target // (XS * CORES), target % (XS * CORES) // CORES],
        mod_in,
        device_at,
        mod_sends,
        mod_recvs,
    )
    mod_in[me] = parts[data, x]
    run_all(events[2 * early :])
    receive(mod_copies)
    for column in range(XS * CORES):
        total = mod_in[column]
        for row in range(1, ZS * YS):
            total = total + mod_in[row * XS * CORES + column]
        mod_ref[column] = total
    for copy in silu_copies + mod_copies:
        copy.wait_send()
    finish()


def whole_shape(shard):
    rows, width = shard.shape
    return jax.ShapeDtypeStruct((ZS, YS, rows, XS * width), jnp.bfloat16)


def gather_first(shard, silu_blocks, matrix, bias, ident):
    chunks = grouped(1, shard.shape[0], [16])
    groups, rows, _ = silu_blocks.shape
    lines = -(-matrix.shape[1] // (8 * LANES)) * 8
    return pl.pallas_call(
        partial(gather_kernel, chunks),
        out_shape=[
            whole_shape(shard),
            jax.ShapeDtypeStruct(silu_blocks.shape, jnp.float32),
            jax.ShapeDtypeStruct((XS * CORES, lines, LANES), jnp.float32),
        ],
        in_specs=[VMEM] * 4,
        out_specs=[HBM, VMEM, VMEM],
        scratch_shapes=[
            pltpu.VMEM((groups, rows, lines, LANES), jnp.float32),
            pltpu.VMEM((DEVICES, lines, LANES), jnp.float32),
        ]
        + semaphores_of(groups - 1, DEVICES - 1)
        + gather_scratch(chunks, 1),
        compiler_params=pltpu.CompilerParams(collective_id=ident, has_side_effects=True),
        name="gather_first",
    )(shard, silu_blocks, matrix, bias)


def scatter_kernel(chunks, matrices, lines, *refs):
    pieces, (small_ref, matrix_ref) = refs[: 4 * matrices], refs[4 * matrices : 4 * matrices + 2]
    refs = refs[4 * matrices + 2 :]
    sums, (small_in, cond_ref), refs = refs[:matrices], refs[matrices : matrices + 2], refs[matrices + 2 :]
    silu_parts, cond_in, small_sends, small_recvs, cond_sends, cond_recvs = refs[:6]
    buffers, semaphores = refs[6 : 6 + 4 * matrices], refs[6 + 4 * matrices :]
    me, data, chip = numbers()
    z, y, x, core = place()
    chips = ZS * YS * XS
    greet_all()
    small_copies = send_each(
        chips,
        chip,
        lambda target: small_ref.at[target % XS],
        small_in,
        lambda target: (target // XS, target % XS * CORES + core),
        small_sends,
        small_recvs,
    )
    events, finish = scatter_plan(chunks, SCATTER_SPACING, pieces, sums, buffers, *semaphores)
    run_all(events[: len(chunks)])
    small_in[chip] = small_ref[x]
    silu_parts[...] = jnp.zeros_like(silu_parts)
    receive(small_copies)
    total = jnp.zeros((chips, matrix_ref.shape[0]), jnp.float32)
    for line in range(lines):
        total = total + contract(
            small_in[:, line, :].astype(jnp.bfloat16),
            matrix_ref[:, line * LANES : (line + 1) * LANES],
            1,
            1,
        )
    for image in range(chips):
        at = image % XS
        silu_parts[image // XS, at : at + 1, :] = total[image : image + 1, :]
    middle = 2 * len(chunks)
    run_all(events[len(chunks) : middle])
    cond_copies = send_each(
        DEVICES,
        me,
        lambda target: silu_parts.at[target // (XS * CORES)],
        cond_in,
        device_at,
        cond_sends,
        cond_recvs,
    )
    cond_in[me] = silu_parts[data]
    run_all(events[middle:])
    receive(cond_copies)
    for row in range(ZS * YS):
        total = cond_in[row * XS * CORES]
        for column in range(1, XS * CORES):
            total = total + cond_in[row * XS * CORES + column]
        cond_ref[row] = total
    for copy in small_copies + cond_copies:
        copy.wait_send()
    finish()


def scatter_last(pieces, units, small, matrix, lines, ident):
    count = len(pieces)
    chunks = scatter_chunks(pieces, units)
    shapes = [sum_shape(piece) for piece in pieces]
    depth = matrix.shape[0]
    results = pl.pallas_call(
        partial(scatter_kernel, chunks, count, lines),
        out_shape=[jax.ShapeDtypeStruct(shape, jnp.float32) for shape in shapes]
        + [
            jax.ShapeDtypeStruct((ZS * YS * XS,) + small.shape[1:], jnp.float32),
            jax.ShapeDtypeStruct((ZS * YS, 8, depth), jnp.float32),
        ],
        in_specs=[VMEM] * (4 * count + 2),
        out_specs=[VMEM] * (count + 2),
        scratch_shapes=[
            pltpu.VMEM((ZS * YS, 8, depth), jnp.float32),
            pltpu.VMEM((DEVICES, 8, depth), jnp.float32),
        ]
        + semaphores_of(ZS * YS * XS - 1, DEVICES - 1)
        + scatter_scratch(chunks, shapes),
        compiler_params=pltpu.CompilerParams(
            collective_id=ident, has_side_effects=True, vmem_limit_bytes=60 * 2**20
        ),
        name="scatter_last",
    )(*[array for piece in pieces for array in piece], small, matrix)
    return results[:count], results[count], results[count + 1]


QUARTER = HEAD // 4
BLOCK = 256


def turn(values, tables, back):
    cosine, to_left, to_right = tables
    swapped = (
        pltpu.roll(values, LANES - QUARTER, axis=1) * to_left
        + pltpu.roll(values, QUARTER, axis=1) * to_right
    )
    return values * cosine - swapped if back else values * cosine + swapped


def head_lanes(source, at, start, end):
    short = max(start + LANES - end, 0)
    values = source[at, start - short : start - short + LANES]
    return pltpu.roll(values, LANES - short, axis=1) if short else values


def attend_kernel(heads, scale, chunks, matrices, *refs):
    projected, (cos_ref, left_ref, right_ref, hide_ref) = refs[0], refs[1:5]
    shards, refs = refs[5 : 5 + matrices], refs[5 + matrices :]
    out_ref, (query_ref, key_ref, value_ref, logsum_ref) = refs[0], refs[1:5]
    wholes, held, gather_refs = refs[5 : 5 + matrices], refs[5 + matrices], refs[6 + matrices :]
    slots, half_width = cos_ref.shape[0], projected.shape[1] // XS
    per = heads // 2
    blocks = slots // BLOCK
    greet(line_peers())
    start, events, end = gather_plan(chunks, GATHER_SPACING, shards, wholes, *gather_refs)
    start()
    table = table_of(events, GATHER_WEIGHTS, heads * blocks + 1)
    for event in table[0]:
        event()

    def prepare(i, carry):
        at = pl.ds(pl.multiple_of(i * BLOCK, BLOCK), BLOCK)
        tables = cos_ref[at, :], left_ref[at, :], right_ref[at, :]
        hide = hide_ref[at, :]
        lane = lax.broadcasted_iota(jnp.int32, (BLOCK, LANES), 1)
        for head in range(heads):
            half, local = head // per, head % per
            for part, target in enumerate((query_ref, key_ref, value_ref)):
                start = half * half_width + (part * per + local) * HEAD
                values = head_lanes(projected, at, start, XS * half_width)
                if part == 2:
                    values = jnp.where(lane < HEAD, values, 0.0)
                else:
                    values = turn(values, tables, False)
                    values = values + (jnp.where(lane == HEAD, 1.0, 0.0) if part == 0 else hide)
                target[head, at, :] = values.astype(jnp.bfloat16)
        return carry

    lax.fori_loop(0, blocks, prepare, 0)

    def attend(i, carry):
        dispatch(table[1:], i, 0, heads * blocks)
        head, block = i // blocks, i % blocks
        at = pl.ds(pl.multiple_of(block * BLOCK, BLOCK), BLOCK)
        scores = contract(query_ref[head, at, :], key_ref[head], 1, 1)
        highest = jnp.max(scores, 1, keepdims=True)
        exponent = jnp.exp2((scores - highest) * (scale * LOG2E))
        denominator = jnp.sum(exponent, 1, keepdims=True)
        result = jnp.dot(
            exponent.astype(jnp.bfloat16), value_ref[head], preferred_element_type=jnp.float32
        )
        held[head, at, :] = result / denominator
        logsum_ref[head, at, :] = jnp.broadcast_to(
            (highest * scale + jnp.log(denominator)) * LOG2E, (BLOCK, LANES)
        )
        return carry

    lax.fori_loop(0, heads * blocks, attend, 0)
    out_half = out_ref.shape[1] // XS

    def finish(i, carry):
        at = pl.ds(pl.multiple_of(i * BLOCK, BLOCK), BLOCK)
        padding = jnp.zeros((BLOCK, out_half - per * HEAD), jnp.float32)
        for half in range(2):
            pieces = [held[half * per + local, at, :][:, :HEAD] for local in range(per)]
            row = jnp.concatenate(pieces + [padding], 1)
            out_ref[at, half * out_half : (half + 1) * out_half] = row.astype(jnp.bfloat16)
        return carry

    lax.fori_loop(0, blocks, finish, 0)
    end()


def attend(projected, tables, shards, units, out_half, heads, scale, ident):
    slots = projected.shape[0]
    count = len(shards)
    rows = shards[0].shape[0]
    chunks = grouped(count - 1, rows, units) + two_hops(count - 1, rows)
    packed = jax.ShapeDtypeStruct((heads, slots, LANES), jnp.bfloat16)
    results = pl.pallas_call(
        partial(attend_kernel, heads, scale, chunks, count),
        out_shape=[
            jax.ShapeDtypeStruct((slots, XS * out_half), jnp.bfloat16),
            packed,
            packed,
            packed,
            jax.ShapeDtypeStruct((heads, slots, LANES), jnp.float32),
        ]
        + [whole_shape(shard) for shard in shards],
        in_specs=[VMEM] * (5 + count),
        out_specs=[VMEM] * 5 + [HBM] * count,
        scratch_shapes=[pltpu.VMEM((heads, slots, LANES), jnp.float32)]
        + gather_scratch(chunks, count),
        compiler_params=pltpu.CompilerParams(
            collective_id=ident, has_side_effects=True, vmem_limit_bytes=60 * 2**20
        ),
        name="attend",
    )(projected, *tables, *shards)
    return results[0], results[1:5], results[5:]


def attend_back_kernel(heads, scale, chunks, matrices, *refs):
    query_ref, key_ref, value_ref, logsum_ref = refs[:4]
    grads, (cos_ref, left_ref, right_ref) = refs[4], refs[5:8]
    pieces, refs = refs[8 : 8 + 4 * matrices], refs[8 + 4 * matrices :]
    out_ref, sums, refs = refs[0], refs[1 : 1 + matrices], refs[1 + matrices :]
    held, grad_q, grad_k, grad_v = refs[:4]
    buffers, semaphores = refs[4 : 4 + 4 * matrices], refs[4 + 4 * matrices :]
    slots, grad_half, out_half = cos_ref.shape[0], grads.shape[1] // XS, out_ref.shape[1] // XS
    per = heads // 2
    blocks = slots // BLOCK
    greet(line_peers())
    events, end = scatter_plan(chunks, SCATTER_SPACING, pieces, sums, buffers, *semaphores)
    table = table_of(events, SCATTER_WEIGHTS, heads * blocks + 1)
    for event in table[0]:
        event()

    def prepare(i, carry):
        at = pl.ds(pl.multiple_of(i * BLOCK, BLOCK), BLOCK)
        for head in range(heads):
            start = head // per * grad_half + head % per * HEAD
            piece = grads[at, start : start + HEAD]
            padding = jnp.zeros((BLOCK, LANES - HEAD), piece.dtype)
            held[head, at, :] = jnp.concatenate([piece, padding], 1)
        return carry

    lax.fori_loop(0, blocks, prepare, 0)

    def attend(i, carry):
        dispatch(table[1:], i, 0, heads * blocks)
        head, block = i // blocks, i % blocks
        at = pl.ds(pl.multiple_of(block * BLOCK, BLOCK), BLOCK)
        query, grad = query_ref[head, at, :], held[head, at, :]
        key = key_ref[head]
        scores = contract(query, key, 1, 1)
        soft = jnp.exp2(scores * (scale * LOG2E) - logsum_ref[head, at, :1])
        grad_soft = contract(grad, value_ref[head], 1, 1)
        value_part = contract(soft.astype(jnp.bfloat16), grad, 0, 0)
        product = soft * grad_soft
        inner = jnp.sum(product, 1, keepdims=True)
        grad_scores = ((product - soft * inner) * scale).astype(jnp.bfloat16)
        grad_q[head, at, :] = jnp.dot(grad_scores, key, preferred_element_type=jnp.float32)
        key_part = contract(grad_scores, query, 0, 0)

        @pl.when(block == 0)
        def _():
            grad_v[head] = value_part
            grad_k[head] = key_part

        @pl.when(block > 0)
        def _():
            grad_v[head] += value_part
            grad_k[head] += key_part

        return carry

    lax.fori_loop(0, heads * blocks, attend, 0)

    def finish(i, carry):
        at = pl.ds(pl.multiple_of(i * BLOCK, BLOCK), BLOCK)
        tables = cos_ref[at, :], left_ref[at, :], right_ref[at, :]
        padding = jnp.zeros((BLOCK, out_half - 3 * per * HEAD), jnp.float32)
        for half in range(2):
            row = []
            for part, source in enumerate((grad_q, grad_k, grad_v)):
                for local in range(per):
                    values = source[half * per + local, at, :]
                    if part < 2:
                        values = turn(values, tables, True)
                    row.append(values[:, :HEAD])
            row = jnp.concatenate(row + [padding], 1)
            out_ref[at, half * out_half : (half + 1) * out_half] = row.astype(jnp.bfloat16)
        return carry

    lax.fori_loop(0, blocks, finish, 0)
    end()


def attend_back(saved, grads, tables, pieces, units, out_half, heads, scale, ident):
    count = len(pieces)
    chunks = scatter_chunks(pieces, units)
    shapes = [sum_shape(piece) for piece in pieces]
    slots = grads.shape[0]
    wide = pltpu.VMEM((heads, slots, LANES), jnp.float32)
    results = pl.pallas_call(
        partial(attend_back_kernel, heads, scale, chunks, count),
        out_shape=[jax.ShapeDtypeStruct((slots, XS * out_half), jnp.bfloat16)]
        + [jax.ShapeDtypeStruct(shape, jnp.float32) for shape in shapes],
        in_specs=[VMEM] * (8 + 4 * count),
        out_specs=[VMEM] * (1 + count),
        scratch_shapes=[pltpu.VMEM((heads, slots, LANES), jnp.bfloat16), wide, wide, wide]
        + scatter_scratch(chunks, shapes),
        compiler_params=pltpu.CompilerParams(
            collective_id=ident, has_side_effects=True, vmem_limit_bytes=63 * 2**20
        ),
        name="attend_back",
    )(*saved, grads, *tables[:3], *[array for piece in pieces for array in piece])
    return results[0], results[1:]


def turn_tables(positions, visible):
    lane = jnp.arange(LANES)
    inside = lane < HEAD
    frequency = rope_base ** (-(lane % QUARTER).astype(jnp.float32) / QUARTER)
    by_row = positions[:, :1].astype(jnp.float32) * frequency
    by_column = positions[:, 1:].astype(jnp.float32) * frequency
    angles = jnp.where(lane < HEAD // 2, by_row, by_column)
    cosine = jnp.where(inside, jnp.cos(angles), 0.0)
    sine = jnp.where(inside, jnp.sin(angles), 0.0)
    leads = lane // QUARTER % 2 == 0
    hide = jnp.where((lane == HEAD) & ~visible[:, None], -1e30, 0.0)
    return cosine, jnp.where(leads, -sine, 0.0), jnp.where(leads, 0.0, sine), hide


def image_device(
    block_input,
    conditioning,
    patch_counts,
    positions,
    w_mod,
    b_mod,
    w_qkv,
    b_qkv,
    w_out,
    b_out,
    w_up,
    b_up,
    w_down,
    b_down,
    cotangent,
):
    own_rows, model_width = block_input.shape
    slot_count = own_rows * CORES
    shard_rows, _, feat = w_qkv.shape
    units = w_up.shape[1]
    heads = CORES * feat // HEAD
    scale = 1.0 / math.sqrt(HEAD)
    images = ZS * YS * XS
    z, y, x, core = place()
    data = z * YS + y
    bf16 = jnp.bfloat16

    def swap(values):
        return lax.ppermute(values, "tensor", CORE_SWAP)

    def both(values):
        return jnp.concatenate([values, swap(values)], 0)

    def own_sum(terms):
        return terms[:own_rows] + swap(terms[own_rows:].astype(bf16)).astype(jnp.float32)

    qkv_width = 3 * feat
    qkv_half, out_half = -(-qkv_width // LANES) * LANES, -(-feat // LANES) * LANES
    qkv_shard = jnp.pad(
        w_qkv.reshape(shard_rows, qkv_width).astype(bf16), ((0, 0), (0, qkv_half - qkv_width))
    )
    out_shard = jnp.pad(w_out.T.astype(bf16), ((0, 0), (0, out_half - feat)))
    shards = [out_shard, w_up.astype(bf16), w_down.T.astype(bf16)]

    depth, lines = -(-shard_rows // LANES) * LANES, 6 * out_half // LANES
    silu_cond = jax.nn.silu(conditioning).astype(bf16).astype(jnp.float32)
    silu_blocks = silu_cond.reshape(XS, ZS * YS, shard_rows).transpose(1, 0, 2)
    silu_blocks = jnp.pad(silu_blocks, ((0, 0), (0, 8 - XS), (0, depth - shard_rows)))
    mod_matrix = jnp.pad(
        w_mod.astype(bf16), ((0, depth - shard_rows), (0, 0), (0, out_half - feat))
    ).reshape(depth, -1)
    mod_bias = jnp.pad(jnp.where(data == 0, b_mod, 0.0), ((0, 0), (0, out_half - feat)))
    whole, silu_in, mod_parts = gather_first(
        qkv_shard, silu_blocks, mod_matrix, mod_bias.reshape(1, -1), 2
    )
    qkv_full = whole.reshape(model_width, -1)
    silu_rows = silu_in[:, :XS, :shard_rows].reshape(images, shard_rows).astype(bf16)
    mod_parts = mod_parts[:, :lines].reshape(XS * CORES, 6, out_half)[:, :, :feat]
    mod = mod_parts.transpose(1, 0, 2).reshape(6, model_width)
    shift_one, scale_one, gate_one, shift_two, scale_two, gate_two = (mod[i] for i in range(6))
    biases = jnp.concatenate([jnp.pad(b_qkv.reshape(-1), (0, qkv_half - qkv_width)), b_up])
    other_biases = lax.ppermute(biases, "tensor", X_SWAP)
    low_biases = jnp.where(x == 0, biases, other_biases)
    high_biases = jnp.where(x == 0, other_biases, biases)
    bias_qkv = jnp.concatenate([low_biases[:qkv_half], high_biases[:qkv_half]])
    bias_up = jnp.concatenate([low_biases[qkv_half:], high_biases[qkv_half:]])

    own_slots = core * own_rows + jnp.arange(own_rows)
    other_slots = (1 - core) * own_rows + jnp.arange(own_rows)
    slots = jnp.concatenate([own_slots, other_slots])
    visible = slots < lax.dynamic_index_in_dim(patch_counts, x, 0, False)
    image_start = x * slot_count
    places = jnp.concatenate(
        [
            lax.dynamic_slice_in_dim(positions, image_start + core * own_rows, own_rows, 0),
            lax.dynamic_slice_in_dim(positions, image_start + (1 - core) * own_rows, own_rows, 0),
        ]
    )
    tables = turn_tables(places, visible)

    normal_one, inverse_one = row_norm(block_input)
    normal_other = row_norm(swap(block_input))[0]
    hidden_one = jnp.concatenate(
        [
            (normal * (1.0 + scale_one) + shift_one).astype(bf16)
            for normal in (normal_one, normal_other)
        ]
    )
    projected = jnp.dot(hidden_one, qkv_full, preferred_element_type=jnp.float32) + bias_qkv
    attended, saved, wholes = attend(
        projected, tables, shards, [48, 16, 16], out_half, heads, scale, 3
    )
    out_full, up_full = (whole.reshape(model_width, -1) for whole in wholes[:2])
    split = y_rows(shard_rows)
    part_y = lax.dynamic_index_in_dim(wholes[2][:, :, :split], y, 1, False)
    low, high = wholes[2][:, :, split:, :units], wholes[2][:, :, split:, units:]
    part_x = jnp.where(x == 0, low, high)
    got_y = lax.ppermute(part_y, "dp", Y_SWAP)
    got_x = lax.ppermute(part_x, "tensor", X_SWAP)
    branch_one = own_sum(contract(attended, out_full, 1, 1)) + b_out
    middle = block_input + gate_one * branch_one
    normal_two, inverse_two = row_norm(middle)
    hidden_two = both((normal_two * (1.0 + scale_two) + shift_two).astype(bf16))
    up_pre = jnp.dot(hidden_two, up_full, preferred_element_type=jnp.float32) + bias_up
    activated = gelu_tanh(up_pre).astype(bf16)

    def norm_back(grad_hidden, normal, inverse, factor):
        grad_normal = grad_hidden * (1.0 + factor)
        mean_plain = jnp.mean(grad_normal, 1, keepdims=True)
        mean_cross = jnp.mean(grad_normal * normal, 1, keepdims=True)
        return inverse[:, None] * (grad_normal - mean_plain - normal * mean_cross)

    def column_sum(values):
        return jnp.sum(values.astype(jnp.float32), 0)

    grad_rows_two = both((cotangent * gate_two).astype(bf16))
    grad_bdown = column_sum(grad_rows_two)
    grad_down = contract(grad_rows_two, activated, 0, 0).astype(bf16)
    sent_down, (grad_rows_two, got_y, got_x) = send_off(
        grad_down, 0, (grad_rows_two, got_y, got_x)
    )
    rows_y = jnp.stack(
        [jnp.where(y == 0, part_y, got_y), jnp.where(y == 0, got_y, part_y)], 1
    )
    rows_x = jnp.concatenate(
        [jnp.where(x == 0, part_x, got_x), jnp.where(x == 0, got_x, part_x)], -1
    )
    down_full = jnp.concatenate([rows_y, rows_x], 2).reshape(model_width, -1)
    grad_activated = jnp.dot(grad_rows_two, down_full, preferred_element_type=jnp.float32)
    grad_up = jax.vjp(gelu_tanh, up_pre)[1](grad_activated)[0].astype(bf16)
    grad_bup = column_sum(grad_up)
    grad_wup = contract(hidden_two, grad_up, 0, 0).astype(bf16)
    sent_down, grad_up = arrive_before(sent_down, grad_up)
    sent_up, grad_up = send_off(grad_wup, 1, grad_up)
    hidden_terms = contract(grad_up, up_full, 1, 1)
    other_terms = swap(hidden_terms[own_rows:].astype(bf16))
    other_terms, activated = lax.optimization_barrier((other_terms, activated))
    grad_hidden_two = hidden_terms[:own_rows] + other_terms.astype(jnp.float32)
    branch_two = own_sum(contract(activated, down_full, 1, 1)) + b_down
    block_output = middle + gate_two * branch_two
    grad_gate_two = jnp.sum(cotangent * branch_two, 0)
    grad_shift_two = jnp.sum(grad_hidden_two, 0)
    grad_scale_two = jnp.sum(grad_hidden_two * normal_two, 0)
    grad_middle = cotangent + norm_back(grad_hidden_two, normal_two, inverse_two, scale_two)
    grad_gate_one = jnp.sum(grad_middle * branch_one, 0)
    grad_rows_one = both((grad_middle * gate_one).astype(bf16))
    grad_bout = column_sum(grad_rows_one)
    grad_out = contract(grad_rows_one, attended, 0, 0).astype(bf16)
    sent_out, grad_rows_one = send_off(grad_out, 1, grad_rows_one)
    grad_attended = jnp.dot(grad_rows_one, out_full, preferred_element_type=jnp.float32)
    grad_projected, (sum_down, sum_up) = attend_back(
        saved,
        grad_attended.astype(bf16),
        tables,
        [settle(sent_down), settle(sent_up)],
        [16, 16],
        qkv_half,
        heads,
        scale,
        6,
    )
    grad_qkv = contract(hidden_one, grad_projected, 0, 0).astype(bf16)
    sent_qkv, grad_projected = send_off(grad_qkv, 0, grad_projected)
    bias_terms = column_sum(grad_projected).reshape(2, qkv_half)
    grad_hidden_one = own_sum(contract(grad_projected, qkv_full, 1, 1))
    grad_shift_one = jnp.sum(grad_hidden_one, 0)
    grad_scale_one = jnp.sum(grad_hidden_one * normal_one, 0)
    grad_input = grad_middle + norm_back(grad_hidden_one, normal_one, inverse_one, scale_one)

    grad_mod = jnp.stack(
        [
            grad_shift_one,
            grad_scale_one,
            grad_gate_one,
            grad_shift_two,
            grad_scale_two,
            grad_gate_two,
        ]
    )
    grad_mod = (grad_mod + swap(grad_mod)).astype(bf16).astype(jnp.float32)
    grad_mod = grad_mod.reshape(6, XS, CORES, feat)
    grad_mod = lax.dynamic_index_in_dim(grad_mod, core, 2, False)
    grad_mod = jnp.pad(grad_mod, ((0, 0), (0, 0), (0, out_half - feat)))
    small = qkv_half + units + 2 * model_width
    rest = -(-(lines * LANES + small) // (8 * LANES)) * 8 * LANES - lines * LANES - small
    sends = []
    for half in range(2):
        flat = jnp.concatenate(
            [
                grad_mod[:, half].reshape(-1),
                bias_terms[half],
                grad_bup[half * units : (half + 1) * units],
                grad_bout,
                grad_bdown,
                jnp.zeros(rest, jnp.float32),
            ]
        )
        sends.append(flat.reshape(-1, LANES))
    (sum_out, sum_qkv), small_all, silu_sum = scatter_last(
        [settle(sent_out), settle(sent_qkv)], [48, 16], jnp.stack(sends), mod_matrix, lines, 7
    )
    grad_wqkv = sum_qkv[:, :qkv_width].reshape(shard_rows, 3, feat)
    grad_wout = sum_out[:, :feat].T
    grad_wdown = sum_down.T
    summed = jnp.sum(small_all, 0)
    grad_bmod = summed[:lines].reshape(6, out_half)[:, :feat]
    summed = summed[lines:].reshape(-1)
    grad_bqkv = summed[:qkv_width].reshape(3, feat)
    grad_bup = summed[qkv_half : qkv_half + units]
    offset = qkv_half + units
    grad_bout = summed[offset : offset + model_width]
    grad_bdown = summed[offset + model_width : offset + 2 * model_width]
    mod_all = small_all[:, :lines].reshape(images, 6, out_half)[:, :, :feat]
    mod_all = mod_all.reshape(images, 6 * feat).astype(bf16)
    grad_wmod = contract(silu_rows, mod_all, 0, 0).reshape(shard_rows, 6, feat)
    grad_silu = silu_sum[:, :XS, :shard_rows].transpose(1, 0, 2).reshape(XS, model_width)
    grad_cond = jax.vjp(jax.nn.silu, conditioning)[1](grad_silu)[0]
    return (
        block_output,
        grad_input,
        grad_cond,
        grad_wmod,
        grad_bmod,
        grad_wqkv,
        grad_bqkv,
        grad_wout,
        grad_bout,
        sum_up,
        grad_bup,
        grad_wdown,
        grad_bdown,
    )

def solution(mesh):
    body = image_device if image_per_chip(mesh) else per_device
    placed = (
        P(("dp", "tensor"), None),
        P("dp", None),
        P("dp"),
        P("dp", None),
        P("dp", None, "tensor"),
        P(None, "tensor"),
        P("dp", None, "tensor"),
        P(None, "tensor"),
        P("tensor", "dp"),
        P(),
        P("dp", "tensor"),
        P("tensor"),
        P("tensor", "dp"),
        P(),
        P(("dp", "tensor"), None),
    )
    return jax.shard_map(
        body,
        mesh=mesh,
        in_specs=placed,
        out_specs=(
            P(("dp", "tensor"), None),
            P(("dp", "tensor"), None),
            P("dp", None),
            P("dp", None, "tensor"),
            P(None, "tensor"),
            P("dp", None, "tensor"),
            P(None, "tensor"),
            P("tensor", "dp"),
            P(),
            P("dp", "tensor"),
            P("tensor"),
            P("tensor", "dp"),
            P(),
        ),
        check_vma=False,
    )
```
